8 devices in a mesh: cp: 8 (over z, y, x, core).
Axes of the slice: x: 2, y: 2, z: 1, core: 2. Of those that a mesh axis runs over, the one named last changes fastest.
Arguments:
- queries: bfloat16 [2048, 16, 192], P('cp')
- latent: bfloat16 [2048, 512], P('cp')
- key_rope: bfloat16 [2048, 64], P('cp')
- w_uk: bfloat16 [512, 16, 128], replicated
- w_uv: bfloat16 [512, 16, 128], replicated
- d_out: bfloat16 [2048, 16, 128], P('cp')
Outputs:
- output 1: bfloat16 [2048, 16, 128], P('cp')
- output 2: bfloat16 [2048, 16, 192], P('cp')
- output 3: bfloat16 [2048, 512], P('cp')
- output 4: bfloat16 [2048, 64], P('cp')
- output 5: float32 [512, 16, 128], replicated
- output 6: float32 [512, 16, 128], replicated
All inputs are finite; a program needn't handle non-finite values.
Results may differ from the reference program's by a relative error of at most 0.0141521.
Values are sent between devices in bfloat16 or wider.
A program may use at most 1 GiB of HBM per device.

```python
import math
import jax
import jax.numpy as jnp
from jax import lax

TOK_DEV = 256
N_DEV = 8
N_HEADS = 16
LATENT = 512
NOPE_DIM = 128
ROPE_DIM = 64
V_DIM = 128

SEQ_LEN = TOK_DEV * N_DEV
QK_DIM = NOPE_DIM + ROPE_DIM
SOFT_SCALE = 1.0 / math.sqrt(QK_DIM)
Q_SPREAD = math.sqrt(0.75 * math.log(SEQ_LEN))


def setup_inputs(seed: int = 0) -> dict:
    rng_keys = jax.random.split(jax.random.key(seed), 6)
    queries = jax.random.normal(rng_keys[0], (SEQ_LEN, N_HEADS, QK_DIM), jnp.float32) * Q_SPREAD
    latent = jax.random.normal(rng_keys[1], (SEQ_LEN, LATENT), jnp.float32)
    key_rope = jax.random.normal(rng_keys[2], (SEQ_LEN, ROPE_DIM), jnp.float32)
    w_uk = jax.random.normal(rng_keys[3], (LATENT, N_HEADS, NOPE_DIM), jnp.float32) * LATENT ** -0.5
    w_uv = jax.random.normal(rng_keys[4], (LATENT, N_HEADS, V_DIM), jnp.float32) * LATENT ** -0.5
    d_out = jax.random.normal(rng_keys[5], (SEQ_LEN, N_HEADS, V_DIM), jnp.float32)
    return {
        "queries": queries.astype(jnp.bfloat16),
        "latent": latent.astype(jnp.bfloat16),
        "key_rope": key_rope.astype(jnp.bfloat16),
        "w_uk": w_uk.astype(jnp.bfloat16),
        "w_uv": w_uv.astype(jnp.bfloat16),
        "d_out": d_out.astype(jnp.bfloat16),
    }


def decompress(latent, w_uk, w_uv):
    lat_f = latent.astype(jnp.float32)
    k_nope = jnp.einsum("tl,lhd->thd", lat_f, w_uk.astype(jnp.float32)).astype(jnp.bfloat16)
    values = jnp.einsum("tl,lhd->thd", lat_f, w_uv.astype(jnp.float32)).astype(jnp.bfloat16)
    return k_nope, values


def attend(queries, latent, key_rope, w_uk, w_uv):
    k_nope, values = decompress(latent, w_uk, w_uv)
    k_f = k_nope.astype(jnp.float32)
    v_f = values.astype(jnp.float32)
    r_f = key_rope.astype(jnp.float32)
    key_pos = jnp.arange(SEQ_LEN)

    def block_rows(blk_pair):
        q_blk, q_start = blk_pair
        q_f = q_blk.astype(jnp.float32)
        scores = (jnp.einsum("qhd,khd->hqk", q_f[:, :, :NOPE_DIM], k_f)
                  + jnp.einsum("qhd,kd->hqk", q_f[:, :, NOPE_DIM:], r_f)) * SOFT_SCALE
        q_pos = q_start + jnp.arange(TOK_DEV)
        visible = key_pos[None, :] <= q_pos[:, None]
        scores = jnp.where(visible[None], scores, -1e30)
        attn_prob = jax.nn.softmax(scores, axis=-1)
        return jnp.einsum("hqk,khd->qhd", attn_prob, v_f)

    q_blocks = queries.reshape(N_DEV, TOK_DEV, N_HEADS, QK_DIM)
    q_starts = jnp.arange(N_DEV) * TOK_DEV
    out_rows = lax.map(jax.checkpoint(block_rows), (q_blocks, q_starts))
    return out_rows.reshape(SEQ_LEN, N_HEADS, V_DIM).astype(jnp.bfloat16)


def reference(queries, latent, key_rope, w_uk, w_uv, d_out):
    attn_out, pull_back = jax.vjp(attend, queries, latent, key_rope, w_uk.astype(jnp.float32), w_uv.astype(jnp.float32))
    d_query, d_latent, d_key_rope, d_w_uk, d_w_uv = pull_back(d_out)
    return (attn_out, d_query.astype(jnp.bfloat16), d_latent.astype(jnp.bfloat16), d_key_rope.astype(jnp.bfloat16), d_w_uk, d_w_uv)
```

```python
import functools
import math
import jax
import jax.numpy as jnp
from jax import lax
from jax.experimental import pallas as pl
from jax.experimental.pallas import tpu as pltpu
from jax.sharding import PartitionSpec as P

F32 = jnp.float32
BF16 = jnp.bfloat16
TOK = 256
CH = 512
HPC = 8
NOPE = 128
ROPE = 64
LAT = 512
NCHIP = 4
PAIRS = [[2 * i, 2 * i + 1] for i in range(4)]
CHIPS = [[0, 2, 4, 6], [1, 3, 5, 7]]


def nt(a, b):
    return lax.dot_general(a, b, (((1,), (1,)), ((), ())), preferred_element_type=F32)


def nn(a, b):
    return lax.dot_general(a, b, (((1,), (0,)), ((), ())), preferred_element_type=F32)


def tn(a, b):
    return lax.dot_general(a, b, (((0,), (0,)), ((), ())), preferred_element_type=F32)


def attn_kernel(q_ref, do_ref, c_ref, r_ref, w_ref, o_ref, dq_ref, dw_ref, dc_ref, dr_ref,
                ct, kv, qt, dot_, s_buf, p_buf):
    scale = 1.0 / math.sqrt(NOPE + ROPE)
    c2 = scale * math.log2(math.e)
    chip = lax.axis_index("cp") // 2

    dc_ref[...] = jnp.zeros_like(dc_ref)
    dr_ref[...] = jnp.zeros_like(dr_ref)

    def tr_chunk(j, _):
        rows = pl.ds(pl.multiple_of(j * CH, CH), CH)
        ct[j] = c_ref[rows, :].T
        return 0
    lax.fori_loop(0, chip + 1, tr_chunk, 0)

    def step(s, _):
        dw_ref[s] = jnp.zeros((LAT, 4 * NOPE), F32)
        for a in range(2):
            h = 2 * s + a
            qt[a] = q_ref[h].T
            dot_[a] = do_ref[h].T

        def phase1(j, stats, masked):
            rows = pl.ds(pl.multiple_of(j * CH, CH), CH)
            kvv = nn(c_ref[rows, :], w_ref[s]).astype(BF16)
            kv[rows, :] = kvv
            rp = r_ref[rows, :]
            out = []
            for a in range(2):
                k_cat = jnp.concatenate([kvv[:, a * NOPE:(a + 1) * NOPE], rp], axis=1)
                s2 = nn(k_cat, qt[a]) * c2
                if masked:
                    ki = lax.broadcasted_iota(jnp.int32, (CH, CH), 0)
                    qi = lax.broadcasted_iota(jnp.int32, (CH, CH), 1)
                    s2 = jnp.where(ki <= qi, s2, -1e30)
                s_buf[a, rows, :] = s2
                cm = jnp.max(s2, axis=0, keepdims=True)
                if stats is None:
                    m = cm
                    l = jnp.sum(jnp.exp2(s2 - m), axis=0, keepdims=True)
                else:
                    m0, l0 = stats[a]
                    m = jnp.maximum(m0, cm)
                    l = l0 * jnp.exp2(m0 - m) + jnp.sum(jnp.exp2(s2 - m), axis=0, keepdims=True)
                out.append((m, l))
            return tuple(out)

        stats = phase1(chip, None, True)
        stats = lax.fori_loop(0, chip, lambda j, st: phase1(j, st, False), stats)
        lse = [m + jnp.log2(l) for m, l in stats]

        def phase2(j, acc):
            rows = pl.ds(pl.multiple_of(j * CH, CH), CH)
            out = []
            for a in range(2):
                pb = jnp.exp2(s_buf[a, rows, :] - lse[a]).astype(BF16)
                p_buf[a, rows, :] = pb
                v = kv[rows, (2 + a) * NOPE:(3 + a) * NOPE]
                out.append(acc[a] + tn(v, pb))
            return tuple(out)

        ot = lax.fori_loop(0, chip + 1, phase2, tuple(jnp.zeros((NOPE, CH), F32) for _ in range(2)))
        delta = []
        for a in range(2):
            h = 2 * s + a
            delta.append(jnp.sum(ot[a] * dot_[a].astype(F32), axis=0, keepdims=True))
            o_ref[h] = ot[a].T.astype(BF16)

        def phase3(j, acc):
            rows = pl.ds(pl.multiple_of(j * CH, CH), CH)
            dks, dvs, out = [], [], []
            rp = r_ref[rows, :]
            dr = jnp.zeros((CH, NOPE), F32)
            for a in range(2):
                h = 2 * s + a
                k = kv[rows, a * NOPE:(a + 1) * NOPE]
                v = kv[rows, (2 + a) * NOPE:(3 + a) * NOPE]
                pb = p_buf[a, rows, :]
                dp = nn(v, dot_[a])
                ds = (pb.astype(F32) * (dp - delta[a])).astype(BF16)
                k_cat = jnp.concatenate([k, rp], axis=1)
                out.append(acc[a] + tn(k_cat, ds))
                dkr = nn(ds, q_ref[h]) * scale
                dks.append(dkr[:, :NOPE].astype(BF16))
                dr = dr + dkr[:, NOPE:]
                dvs.append(nn(pb, do_ref[h]).astype(BF16))
            dkv = jnp.concatenate(dks + dvs, axis=1)
            dr_ref[rows, :] += dr
            dc_ref[rows, :] += nt(dkv, w_ref[s])
            dw_ref[s] += nn(ct[j], dkv)
            return tuple(out)

        dqt = lax.fori_loop(0, chip + 1, phase3, tuple(jnp.zeros((2 * NOPE, CH), F32) for _ in range(2)))
        for a in range(2):
            dq_ref[2 * s + a] = (dqt[a].T * scale).astype(BF16)
        return 0

    lax.fori_loop(0, HPC // 2, step, 0)


def solution(mesh):
    seq_spec = P("cp")

    def local_step(queries, latent, key_rope, w_uk, w_uv, d_out):
        me = lax.axis_index("cp")
        core = me % 2
        swap = [(i, i ^ 1) for i in range(8)]

        def heads_of_core(x):
            xt = jnp.transpose(x, (1, 0, 2))
            mine = lax.dynamic_slice_in_dim(xt, core * HPC, HPC, axis=0)
            other = lax.dynamic_slice_in_dim(xt, (1 - core) * HPC, HPC, axis=0)
            got = lax.ppermute(other, "cp", swap)
            first = jnp.where(core == 0, mine, got)
            second = jnp.where(core == 0, got, mine)
            return jnp.concatenate([first, second], axis=1)

        def tokens_of_core(x):
            mine = lax.dynamic_slice_in_dim(x, core * TOK, TOK, axis=1)
            other = lax.dynamic_slice_in_dim(x, (1 - core) * TOK, TOK, axis=1)
            got = lax.ppermute(other, "cp", swap)
            lo = jnp.where(core == 0, mine, got)
            hi = jnp.where(core == 0, got, mine)
            return jnp.transpose(jnp.concatenate([lo, hi], axis=0), (1, 0, 2))

        q2 = heads_of_core(jnp.pad(queries, ((0, 0), (0, 0), (0, 64))))
        do2 = heads_of_core(d_out)
        cr = jnp.concatenate([latent, key_rope, jnp.zeros((TOK, 64), BF16)], axis=1)
        cr_all = lax.all_gather(cr, "cp", tiled=True)
        c_all, r_all = cr_all[:, :LAT], cr_all[:, LAT:]

        def w_half(w):
            w = lax.dynamic_slice_in_dim(w, core * HPC, HPC, axis=1)
            return jnp.transpose(w.reshape(LAT, 4, 2 * NOPE), (1, 0, 2))
        wcat = jnp.concatenate([w_half(w_uk), w_half(w_uv)], axis=2)

        n = CH * NCHIP
        o2, dq2, dw, dc, dr = pl.pallas_call(
            attn_kernel,
            out_shape=(jax.ShapeDtypeStruct((HPC, CH, NOPE), BF16),
                       jax.ShapeDtypeStruct((HPC, CH, 2 * NOPE), BF16),
                       jax.ShapeDtypeStruct((4, LAT, 4 * NOPE), F32),
                       jax.ShapeDtypeStruct((n, LAT), F32),
                       jax.ShapeDtypeStruct((n, NOPE), F32)),
            in_specs=[pl.BlockSpec(memory_space=pltpu.VMEM)] * 5,
            out_specs=[pl.BlockSpec(memory_space=pltpu.VMEM)] * 5,
            scratch_shapes=[pltpu.VMEM((NCHIP, LAT, CH), BF16),
                            pltpu.VMEM((n, 4 * NOPE), BF16),
                            pltpu.VMEM((2, 2 * NOPE, CH), BF16),
                            pltpu.VMEM((2, NOPE, CH), BF16),
                            pltpu.VMEM((2, n, CH), F32),
                            pltpu.VMEM((2, n, CH), BF16)],
            compiler_params=pltpu.CompilerParams(vmem_limit_bytes=62 << 20),
            cost_estimate=pl.CostEstimate(flops=30 * 10**9, bytes_accessed=20 << 20, transcendentals=10**7),
        )(q2, do2, c_all, r_all, wcat)

        attn_out = tokens_of_core(o2)
        d_query = tokens_of_core(dq2)[:, :, :NOPE + ROPE]
        d_latent = lax.psum_scatter(dc, "cp", scatter_dimension=0, tiled=True).astype(BF16)
        d_key_rope = lax.psum_scatter(dr[:, :ROPE], "cp", scatter_dimension=0, tiled=True).astype(BF16)

        dw = lax.psum(dw, "cp", axis_index_groups=CHIPS)
        dw = lax.all_gather(dw, "cp", axis_index_groups=PAIRS)
        dw = dw.reshape(2, 4, LAT, 2, 2, NOPE)
        dw = jnp.transpose(dw, (3, 2, 0, 1, 4, 5)).reshape(2, LAT, 16, NOPE)
        return attn_out, d_query, d_latent, d_key_rope, dw[0], dw[1]

    return jax.shard_map(local_step, mesh=mesh,
                         in_specs=(seq_spec, seq_spec, seq_spec, P(), P(), seq_spec),
                         out_specs=(seq_spec, seq_spec, seq_spec, seq_spec, P(), P()),
                         check_vma=False)
```

```python
import math
import jax
import jax.numpy as jnp
from jax import lax
from jax.experimental import pallas as pl
from jax.experimental.pallas import tpu as pltpu
from jax.sharding import PartitionSpec as P

F32 = jnp.float32
BF16 = jnp.bfloat16
TOK = 256
CH = 512
HPC = 8
NS = HPC // 2
NOPE = 128
ROPE = 64
LAT = 512
CRW = LAT + NOPE
NCHIP = 4
SEQ = CH * NCHIP
MESH = pl.DeviceIdType.MESH
A_COLS = pl.ds(0, 256)
B_COLS = pl.ds(256, 256)


def nt(a, b):
    return lax.dot_general(a, b, (((1,), (1,)), ((), ())), preferred_element_type=F32)


def nn(a, b):
    return lax.dot_general(a, b, (((1,), (0,)), ((), ())), preferred_element_type=F32)


def tn(a, b):
    return lax.dot_general(a, b, (((0,), (0,)), ((), ())), preferred_element_type=F32)


def mul(i, n):
    return pl.multiple_of(i * n, n)


def attn_kernel(q_in, do_in, cr_in, wk_in, wv_in,
                o_out, dq_out, dw_out, dlat_out, dr_out,
                q_ref, do_ref, cr_ref, wk, wv, o_ref, dq_ref, dw_ref, dwo, dcr,
                ct, kv, qt, dot_, s_buf, p_buf, rb1, rb2, rbd, rbe,
                lsem, xs, xr, cs, crs, ws, wr, fs, fr, fl, ds_, dr_s):
    scale = 1.0 / math.sqrt(NOPE + ROPE)
    c2 = scale * math.log2(math.e)
    me = lax.axis_index("cp")
    core = lax.rem(me, 2)
    chip = lax.div(me, 2)
    x = lax.rem(chip, 2)
    y = lax.div(chip, 2)
    partner = me + 1 - 2 * core
    xn = me + 2 - 4 * x
    yn = me + 4 - 8 * y
    dn = xn + 4 - 8 * y
    chip_x = chip + 1 - 2 * x
    chip_y = chip + 2 - 4 * y
    chip_d = chip_x + 2 - 4 * y

    def rcopy(src, dst, ss, rs, dev):
        return pltpu.make_async_remote_copy(src_ref=src, dst_ref=dst, send_sem=ss, recv_sem=rs,
                                            device_id=(dev,), device_id_type=MESH)

    bar = pltpu.get_barrier_semaphore()
    for peer in (partner, xn, yn, dn):
        pl.semaphore_signal(bar, inc=1, device_id=(peer,), device_id_type=MESH)
    pl.semaphore_wait(bar, 4)

    my_rows = pl.ds(mul(me, TOK), TOK)
    own_rows = pl.ds(mul(core, TOK), TOK)
    oth_rows = pl.ds(mul(1 - core, TOK), TOK)
    mine = pl.ds(mul(core, HPC), HPC)
    other = pl.ds(mul(1 - core, HPC), HPC)
    c_direct = [rcopy(cr_in, cr_ref.at[my_rows], cs.at[i], crs.at[i], dev)
                for i, dev in enumerate((partner, dn, xn, yn))]
    for cp in c_direct:
        cp.start()
    local = [pltpu.make_async_copy(cr_in, cr_ref.at[my_rows], lsem.at[0]),
             pltpu.make_async_copy(q_in.at[mine], q_ref.at[:, own_rows], lsem.at[1]),
             pltpu.make_async_copy(do_in.at[mine], do_ref.at[:, own_rows], lsem.at[2]),
             pltpu.make_async_copy(wk_in, wk, lsem.at[3]),
             pltpu.make_async_copy(wv_in, wv, lsem.at[4])]
    heads = [rcopy(q_in.at[other], q_ref.at[:, own_rows], xs.at[0], xr.at[0], partner),
             rcopy(do_in.at[other], do_ref.at[:, own_rows], xs.at[1], xr.at[1], partner)]
    for cp in heads + local:
        cp.start()
    dcr[...] = jnp.zeros_like(dcr)
    for cp in heads + local:
        cp.wait()
    c_direct[0].wait()

    c_fwd = []
    for i, src in ((1, dn), (2, xn), (3, yn)):
        rows = pl.ds(mul(src, TOK), TOK)
        c_fwd.append(rcopy(cr_ref.at[rows], cr_ref.at[rows], cs.at[3 + i], crs.at[3 + i], partner))

    def wait_latents():
        for i in (2, 3, 1):
            c_direct[i].wait()
            c_fwd[i - 1].start()
        for cp in c_fwd:
            cp.wait()

        def tr_chunk(j, _):
            ct[j] = cr_ref[pl.ds(mul(j, CH), CH), :LAT].T
            return 0
        lax.fori_loop(0, chip + 1, tr_chunk, 0)

    hx = pl.ds(mul(x, 256), 256)
    hx1 = pl.ds(mul(1 - x, 256), 256)
    hy = pl.ds(mul(y, 256), 256)
    hy1 = pl.ds(mul(1 - y, 256), 256)
    qa = pl.ds(pl.multiple_of(x * 256 + y * 128, 128), 128)
    qa1 = pl.ds(pl.multiple_of(x * 256 + (1 - y) * 128, 128), 128)
    qb = pl.ds(pl.multiple_of(y * 256 + x * 128, 128), 128)
    qb1 = pl.ds(pl.multiple_of(y * 256 + (1 - x) * 128, 128), 128)

    def w_copy(phase, s):
        if phase == 1:
            pair = ((dw_ref.at[s, hx1, A_COLS], rb1.at[0], xn), (dw_ref.at[s, hy1, B_COLS], rb1.at[1], yn))
        elif phase == 2:
            pair = ((dw_ref.at[s, qa1, A_COLS], rb2.at[0], yn), (dw_ref.at[s, qb1, B_COLS], rb2.at[1], xn))
        elif phase == 3:
            pair = ((dwo.at[s, qa, A_COLS], dwo.at[s, qa, A_COLS], yn),
                    (dwo.at[s, qb, B_COLS], dwo.at[s, qb, B_COLS], xn))
        else:
            pair = ((dwo.at[s, hx, A_COLS], dwo.at[s, hx, A_COLS], xn),
                    (dwo.at[s, hy, B_COLS], dwo.at[s, hy, B_COLS], yn))
        return [rcopy(a, b, ws.at[phase - 1, i], wr.at[phase - 1, i], d) for i, (a, b, d) in enumerate(pair)]

    def w_start(phase, s):
        for cp in w_copy(phase, s):
            cp.start()

    def w_wait(phase, s):
        for cp in w_copy(phase, s):
            cp.wait()

    def finish1(s):
        w_wait(1, s)
        dw_ref[s, hx, A_COLS] += rb1[0]
        dw_ref[s, hy, B_COLS] += rb1[1]
        w_start(2, s)

    def finish2(s):
        w_wait(2, s)
        dwo[s, qa, A_COLS] = dw_ref[s, qa, A_COLS] + rb2[0]
        dwo[s, qb, B_COLS] = dw_ref[s, qb, B_COLS] + rb2[1]
        w_start(3, s)

    def finish3(s):
        w_wait(3, s)
        w_start(4, s)

    def w_final(s):
        slot = core * NS + s
        return (pltpu.make_async_copy(dwo.at[s], dw_out.at[slot], fl.at[s]),
                rcopy(dwo.at[s], dw_out.at[slot], fs.at[s], fr.at[s], partner))

    def finish4(s):
        w_wait(4, s)
        for cp in w_final(s):
            cp.start()

    def step(s, _):
        dw_ref[s] = jnp.zeros((LAT, 4 * NOPE), F32)
        for a in range(2):
            h = 2 * s + a
            qt[a] = q_ref[h].T
            dot_[a] = do_ref[h].T
        w_s = jnp.concatenate([wk[2 * s], wk[2 * s + 1], wv[2 * s], wv[2 * s + 1]], axis=1)

        def phase1(j, stats, masked):
            rows = pl.ds(mul(j, CH), CH)
            kvv = nn(cr_ref[rows, :LAT], w_s).astype(BF16)
            kv[rows, :] = kvv
            rp = cr_ref[rows, LAT:]
            out = []
            for a in range(2):
                k_cat = jnp.concatenate([kvv[:, a * NOPE:(a + 1) * NOPE], rp], axis=1)
                s2 = nn(k_cat, qt[a]) * c2
                if masked:
                    ki = lax.broadcasted_iota(jnp.int32, (CH, CH), 0)
                    qi = lax.broadcasted_iota(jnp.int32, (CH, CH), 1)
                    s2 = jnp.where(ki <= qi, s2, -1e30)
                s_buf[a, rows, :] = s2
                cm = jnp.max(s2, axis=0, keepdims=True)
                if stats is None:
                    m = cm
                    l = jnp.sum(jnp.exp2(s2 - m), axis=0, keepdims=True)
                else:
                    m0, l0 = stats[a]
                    m = jnp.maximum(m0, cm)
                    l = l0 * jnp.exp2(m0 - m) + jnp.sum(jnp.exp2(s2 - m), axis=0, keepdims=True)
                out.append((m, l))
            return tuple(out)

        stats = phase1(chip, None, True)

        @pl.when(s == 0)
        def _():
            wait_latents()

        stats = lax.fori_loop(0, chip, lambda j, st: phase1(j, st, False), stats)
        lse = [m + jnp.log2(l) for m, l in stats]

        @pl.when(s > 1)
        def _():
            finish4(s - 2)

        @pl.when(s > 0)
        def _():
            finish1(s - 1)

        def phase2(j, acc):
            rows = pl.ds(mul(j, CH), CH)
            out = []
            for a in range(2):
                pb = jnp.exp2(s_buf[a, rows, :] - lse[a]).astype(BF16)
                p_buf[a, rows, :] = pb
                v = kv[rows, (2 + a) * NOPE:(3 + a) * NOPE]
                out.append(acc[a] + tn(v, pb))
            return tuple(out)

        ot = lax.fori_loop(0, chip + 1, phase2, tuple(jnp.zeros((NOPE, CH), F32) for _ in range(2)))
        delta = []
        for a in range(2):
            h = 2 * s + a
            delta.append(jnp.sum(ot[a] * dot_[a].astype(F32), axis=0, keepdims=True))
            o_ref[h] = ot[a].T.astype(BF16)

        @pl.when(s > 0)
        def _():
            finish2(s - 1)

        def phase3(j, acc):
            rows = pl.ds(mul(j, CH), CH)
            dks, dvs, out = [], [], []
            rp = cr_ref[rows, LAT:]
            dr = jnp.zeros((CH, NOPE), F32)
            for a in range(2):
                h = 2 * s + a
                k = kv[rows, a * NOPE:(a + 1) * NOPE]
                v = kv[rows, (2 + a) * NOPE:(3 + a) * NOPE]
                pb = p_buf[a, rows, :]
                dp = nn(v, dot_[a])
                ds = (pb.astype(F32) * (dp - delta[a])).astype(BF16)
                k_cat = jnp.concatenate([k, rp], axis=1)
                out.append(acc[a] + tn(k_cat, ds))
                dkr = nn(ds, q_ref[h]) * scale
                dks.append(dkr[:, :NOPE].astype(BF16))
                dr = dr + dkr[:, NOPE:]
                dvs.append(nn(pb, do_ref[h]).astype(BF16))
            dkv = jnp.concatenate(dks + dvs, axis=1)
            dcr[j, :, LAT:] += dr
            dcr[j, :, :LAT] += nt(dkv, w_s)
            dw_ref[s] += nn(ct[j], dkv)
            return tuple(out)

        dqt = lax.fori_loop(0, chip + 1, phase3, tuple(jnp.zeros((2 * NOPE, CH), F32) for _ in range(2)))
        for a in range(2):
            dq_ref[2 * s + a] = (dqt[a].T * scale).astype(BF16)

        @pl.when(s > 0)
        def _():
            finish3(s - 1)

        w_start(1, s)
        return 0

    lax.fori_loop(0, NS, step, 0)

    d1 = rcopy(dcr.at[:, oth_rows], rbd, ds_.at[0], dr_s.at[0], partner)
    d1.start()
    outs = [pltpu.make_async_copy(o_ref.at[:, own_rows], o_out.at[mine], lsem.at[5]),
            pltpu.make_async_copy(dq_ref.at[:, own_rows], dq_out.at[mine], lsem.at[6]),
            rcopy(o_ref.at[:, oth_rows], o_out.at[mine], xs.at[2], xr.at[2], partner),
            rcopy(dq_ref.at[:, oth_rows], dq_out.at[mine], xs.at[3], xr.at[3], partner)]
    for cp in outs:
        cp.start()
    d1.wait()
    dcr[:, own_rows, :] += rbd[...]

    kinds = ((chip_d, dn), (chip_x, xn), (chip_y, yn))
    d2 = [rcopy(dcr.at[ch, own_rows], rbe.at[i], ds_.at[1 + i], dr_s.at[1 + i], dev)
          for i, (ch, dev) in enumerate(kinds)]
    finish4(NS - 2)
    finish1(NS - 1)
    for i, (ch, dev) in enumerate(kinds):
        @pl.when(ch < chip)
        def _(i=i):
            d2[i].start()
    finish2(NS - 1)
    finish3(NS - 1)
    for i, (ch, dev) in enumerate(kinds):
        @pl.when(ch > chip)
        def _(i=i):
            d2[i].wait_recv()
            dcr[chip, own_rows, :] += rbe[i]

        @pl.when(ch < chip)
        def _(i=i):
            d2[i].wait_send()
    dlat_out[...] = dcr[chip, own_rows, :LAT].astype(BF16)
    dr_out[...] = dcr[chip, own_rows, LAT:LAT + ROPE].astype(BF16)
    finish4(NS - 1)
    for cp in outs:
        cp.wait()
    for s in range(NS):
        for cp in w_final(s):
            cp.wait()


def solution(mesh):
    seq_spec = P("cp")

    def local_step(queries, latent, key_rope, w_uk, w_uv, d_out):
        core = lax.rem(lax.axis_index("cp"), 2)

        q_t = jnp.transpose(jnp.pad(queries, ((0, 0), (0, 0), (0, 64))), (1, 0, 2))
        do_t = jnp.transpose(d_out, (1, 0, 2))
        cr = jnp.concatenate([latent, key_rope, jnp.zeros((TOK, 64), BF16)], axis=1)

        def w_half(w):
            return jnp.transpose(lax.dynamic_slice_in_dim(w, core * HPC, HPC, axis=1), (1, 0, 2))

        any_spec = pl.BlockSpec(memory_space=pl.ANY)
        vm_spec = pl.BlockSpec(memory_space=pltpu.VMEM)
        dma = pltpu.SemaphoreType.DMA
        o_t, dq_t, dw, d_latent, d_key_rope = pl.pallas_call(
            attn_kernel,
            out_shape=(jax.ShapeDtypeStruct((2 * HPC, TOK, NOPE), BF16),
                       jax.ShapeDtypeStruct((2 * HPC, TOK, 2 * NOPE), BF16),
                       jax.ShapeDtypeStruct((2 * NS, LAT, 4 * NOPE), F32),
                       jax.ShapeDtypeStruct((TOK, LAT), BF16),
                       jax.ShapeDtypeStruct((TOK, ROPE), BF16)),
            in_specs=[any_spec] * 5,
            out_specs=[any_spec] * 3 + [vm_spec] * 2,
            scratch_shapes=[pltpu.VMEM((HPC, CH, 2 * NOPE), BF16),
                            pltpu.VMEM((HPC, CH, NOPE), BF16),
                            pltpu.VMEM((SEQ, CRW), BF16),
                            pltpu.VMEM((HPC, LAT, NOPE), BF16),
                            pltpu.VMEM((HPC, LAT, NOPE), BF16),
                            pltpu.VMEM((HPC, CH, NOPE), BF16),
                            pltpu.VMEM((HPC, CH, 2 * NOPE), BF16),
                            pltpu.VMEM((NS, LAT, 4 * NOPE), F32),
                            pltpu.VMEM((NS, LAT, 4 * NOPE), F32),
                            pltpu.VMEM((NCHIP, CH, CRW), F32),
                            pltpu.VMEM((NCHIP, LAT, CH), BF16),
                            pltpu.VMEM((SEQ, 4 * NOPE), BF16),
                            pltpu.VMEM((2, 2 * NOPE, CH), BF16),
                            pltpu.VMEM((2, NOPE, CH), BF16),
                            pltpu.VMEM((2, SEQ, CH), F32),
                            pltpu.VMEM((2, SEQ, CH), BF16),
                            pltpu.VMEM((2, 256, 256), F32),
                            pltpu.VMEM((2, 128, 256), F32),
                            pltpu.VMEM((NCHIP, TOK, CRW), F32),
                            pltpu.VMEM((3, TOK, CRW), F32),
                            dma((7,)), dma((4,)), dma((4,)), dma((7,)), dma((7,)),
                            dma((4, 2)), dma((4, 2)), dma((NS,)), dma((NS,)), dma((NS,)),
                            dma((4,)), dma((4,))],
            compiler_params=pltpu.CompilerParams(vmem_limit_bytes=62 << 20, collective_id=0, has_side_effects=True),
            cost_estimate=pl.CostEstimate(flops=30 * 10**9, bytes_accessed=20 << 20, transcendentals=10**7),
        )(q_t, do_t, cr, w_half(w_uk), w_half(w_uv))

        attn_out = jnp.transpose(o_t, (1, 0, 2))
        d_query = jnp.transpose(dq_t, (1, 0, 2))[:, :, :NOPE + ROPE]
        dw = dw.reshape(2 * NS, LAT, 2, 2, NOPE)
        dw = jnp.transpose(dw, (2, 1, 0, 3, 4)).reshape(2, LAT, 16, NOPE)
        return attn_out, d_query, d_latent, d_key_rope, dw[0], dw[1]

    return jax.shard_map(local_step, mesh=mesh,
                         in_specs=(seq_spec, seq_spec, seq_spec, P(), P(), seq_spec),
                         out_specs=(seq_spec, seq_spec, seq_spec, seq_spec, P(), P()),
                         check_vma=False)
```

```python
import math
import jax
import jax.numpy as jnp
from jax import lax
from jax.experimental import pallas as pl
from jax.experimental.pallas import tpu as pltpu
from jax.sharding import PartitionSpec as P

F32 = jnp.float32
BF16 = jnp.bfloat16
TOK = 256
CH = 512
HEADS = 16
HPC = 8
G = 2
NS = HPC // G
NOPE = 128
ROPE = 64
QK = NOPE + ROPE
LAT = 512
GW = G * NOPE
MSG = TOK + ROPE // 2
NCHIP = 4
SEQ = CH * NCHIP
MESH = pl.DeviceIdType.MESH
A_COLS = pl.ds(0, GW)
B_COLS = pl.ds(GW, GW)


def nt(a, b):
    return lax.dot_general(a, b, (((1,), (1,)), ((), ())), preferred_element_type=F32)


def nn(a, b):
    return lax.dot_general(a, b, (((1,), (0,)), ((), ())), preferred_element_type=F32)


def tn(a, b):
    return lax.dot_general(a, b, (((0,), (0,)), ((), ())), preferred_element_type=F32)


def mul(i, n):
    return pl.multiple_of(i * n, n)


def attn_kernel(q_in, do_in, c_in, r_in, wk_in, wv_in,
                o_out, dq_out, dw_out, dlat_out, dr_out,
                do_raw, wk_raw, wv_raw, stage, do_snd,
                qt, do_ref, c_ref, rt, rn, wk, wv, o_ref, dq_ref, dw_ref, dwo, dcr, drr, msg,
                ct, kv, qn, dot_, s_buf, p_buf, rb1, rb2, rbd, rbr, rbe, rly,
                lsem, xs, xr, cs, crs, ws, wr, fs, fr, fl, d1s, d1r, d2s, d2r):
    scale = 1.0 / math.sqrt(QK)
    c2 = scale * math.log2(math.e)
    me = lax.axis_index("cp")
    core = lax.rem(me, 2)
    chip = lax.div(me, 2)
    x = lax.rem(chip, 2)
    y = lax.div(chip, 2)
    partner = me + 1 - 2 * core
    xn = me + 2 - 4 * x
    yn = me + 4 - 8 * y
    dn = xn + 4 - 8 * y
    chip_x = chip + 1 - 2 * x
    chip_y = chip + 2 - 4 * y
    chip_d = chip_x + 2 - 4 * y

    def rcopy(src, dst, ss, rs, dev):
        return pltpu.make_async_remote_copy(src_ref=src, dst_ref=dst, send_sem=ss, recv_sem=rs,
                                            device_id=(dev,), device_id_type=MESH)

    my_rows = pl.ds(mul(me, TOK), TOK)
    own_rows = pl.ds(mul(core, TOK), TOK)
    oth_rows = pl.ds(mul(1 - core, TOK), TOK)
    mine = pl.ds(mul(core, HPC), HPC)

    other = pl.ds(mul(1 - core, HPC), HPC)

    local = [pltpu.make_async_copy(c_in, c_ref.at[my_rows], lsem.at[0]),
             pltpu.make_async_copy(r_in, rt.at[:, my_rows], lsem.at[1]),
             pltpu.make_async_copy(q_in.at[mine], qt.at[:, :, own_rows], lsem.at[2]),
             pltpu.make_async_copy(do_in, do_raw, lsem.at[3]),
             pltpu.make_async_copy(wk_in.at[:, mine], wk_raw, lsem.at[4]),
             pltpu.make_async_copy(wv_in.at[:, mine], wv_raw, lsem.at[5])]
    for cp in local:
        cp.start()

    bar = pltpu.get_barrier_semaphore()
    for peer in (partner, xn, yn, dn):
        pl.semaphore_signal(bar, inc=1, device_id=(peer,), device_id_type=MESH)
    pl.semaphore_wait(bar, 4)

    local[0].wait()
    local[1].wait()

    def latent_copies(i, src, dev):
        rows = pl.ds(mul(src, TOK), TOK)
        return (rcopy(c_ref.at[rows], c_ref.at[rows], cs.at[0, i], crs.at[0, i], dev),
                rcopy(rt.at[:, rows], rt.at[:, rows], cs.at[1, i], crs.at[1, i], dev))

    c_direct = [latent_copies(i, me, dev) for i, dev in enumerate((partner, dn, xn, yn))]
    for pair in c_direct:
        for cp in pair:
            cp.start()

    heads = [rcopy(q_in.at[other], qt.at[:, :, own_rows], xs.at[0], xr.at[0], partner),
             rcopy(do_snd, do_ref.at[:, own_rows], xs.at[1], xr.at[1], partner)]
    heads[0].start()
    local[3].wait()

    def pick(h, rows, stride):
        return stage[pl.ds(h, rows, stride=stride), :].astype(BF16)

    def widen(i, _):
        rows = pl.ds(mul(i, 256), 256)
        stage[rows, :] = do_raw[rows, :].astype(F32)
        return 0
    lax.fori_loop(0, TOK * HEADS // 256, widen, 0)
    is0 = core == 0
    for i in range(HPC):
        lo = pick(i, TOK, HEADS)
        hi = pick(i + HPC, TOK, HEADS)
        do_ref[i, own_rows, :] = jnp.where(is0, lo, hi)
        do_snd[i] = jnp.where(is0, hi, lo)
    heads[1].start()
    for t, (raw, out) in enumerate(((wk_raw, wk), (wv_raw, wv))):
        local[4 + t].wait()

        def body(i, _, raw=raw):
            ls = pl.ds(mul(i, 32), 32)
            stage[pl.ds(mul(i, 256), 256), :] = raw[ls].astype(F32).reshape(256, NOPE)
            return 0
        lax.fori_loop(0, LAT // 32, body, 0)
        for i in range(HPC):
            out[i] = pick(i, LAT, HPC)

    def zero_dc(j, _):
        dcr[j] = jnp.zeros((CH, LAT), F32)
        drr[j] = jnp.zeros((CH, ROPE), F32)
        return 0
    lax.fori_loop(0, chip + 1, zero_dc, 0)
    local[2].wait()
    for cp in heads:
        cp.wait()
    for cp in c_direct[0]:
        cp.wait()

    def turn(j, _):
        rows = pl.ds(mul(j, CH), CH)
        ct[j] = c_ref[rows, :].T
        rn[rows, :] = rt[:, rows].T
        return 0
    turn(chip, 0)

    c_fwd = [latent_copies(3 + i, src, partner) for i, src in ((1, dn), (2, xn), (3, yn))]

    def wait_latents():
        for i in (2, 3, 1):
            for cp in c_direct[i]:
                cp.wait()
            for cp in c_fwd[i - 1]:
                cp.start()
        for pair in c_fwd:
            for cp in pair:
                cp.wait()
        lax.fori_loop(0, chip, turn, 0)

    hx = pl.ds(mul(x, 256), 256)
    hx1 = pl.ds(mul(1 - x, 256), 256)
    hy = pl.ds(mul(y, 256), 256)
    hy1 = pl.ds(mul(1 - y, 256), 256)
    qa = pl.ds(pl.multiple_of(x * 256 + y * 128, 128), 128)
    qa1 = pl.ds(pl.multiple_of(x * 256 + (1 - y) * 128, 128), 128)
    qb = pl.ds(pl.multiple_of(y * 256 + x * 128, 128), 128)
    qb1 = pl.ds(pl.multiple_of(y * 256 + (1 - x) * 128, 128), 128)

    def w_copy(phase, s):
        if phase == 1:
            pair = ((dw_ref.at[s, hx1, A_COLS], rb1.at[0], xn), (dw_ref.at[s, hy1, B_COLS], rb1.at[1], yn))
        elif phase == 2:
            pair = ((dw_ref.at[s, qa1, A_COLS], rb2.at[0], yn), (dw_ref.at[s, qb1, B_COLS], rb2.at[1], xn))
        elif phase == 3:
            pair = ((dwo.at[s, qa, A_COLS], dwo.at[s, qa, A_COLS], yn),
                    (dwo.at[s, qb, B_COLS], dwo.at[s, qb, B_COLS], xn))
        else:
            pair = ((dwo.at[s, hx, A_COLS], dwo.at[s, hx, A_COLS], xn),
                    (dwo.at[s, hy, B_COLS], dwo.at[s, hy, B_COLS], yn))
        return [rcopy(a, b, ws.at[phase - 1, i], wr.at[phase - 1, i], d) for i, (a, b, d) in enumerate(pair)]

    def w_start(phase, s):
        for cp in w_copy(phase, s):
            cp.start()

    def w_wait(phase, s):
        for cp in w_copy(phase, s):
            cp.wait()

    def add1(s):
        w_wait(1, s)
        dw_ref[s, hx, A_COLS] += rb1[0]
        dw_ref[s, hy, B_COLS] += rb1[1]

    def add2(s):
        w_wait(2, s)
        dwo[s, qa, A_COLS] = dw_ref[s, qa, A_COLS] + rb2[0]
        dwo[s, qb, B_COLS] = dw_ref[s, qb, B_COLS] + rb2[1]

    def w_final(s):
        slot = core * NS + s
        return (pltpu.make_async_copy(dwo.at[s], dw_out.at[slot], fl.at[s]),
                rcopy(dwo.at[s], dw_out.at[slot], fs.at[s], fr.at[s], partner))

    def deliver(s):
        w_wait(4, s)
        for cp in w_final(s):
            cp.start()

    def d1_copies(j):
        return (rcopy(dcr.at[j, oth_rows], rbd.at[j], d1s.at[0, j], d1r.at[0, j], partner),
                rcopy(drr.at[j, oth_rows], rbr.at[j], d1s.at[1, j], d1r.at[1, j], partner))

    def step(s, _):
        dw_ref[s] = jnp.zeros((LAT, 2 * GW), F32)
        for a in range(G):
            h = G * s + a
            qn[a] = qt[h].T
            dot_[a] = do_ref[h].T
        w_s = jnp.concatenate([wk[G * s + a] for a in range(G)] + [wv[G * s + a] for a in range(G)], axis=1)

        def phase1(j, stats, masked):
            rows = pl.ds(mul(j, CH), CH)
            kvv = nn(c_ref[rows, :], w_s).astype(BF16)
            kv[rows, :] = kvv
            rp = rn[rows, :]
            out = []
            for a in range(G):
                k_cat = jnp.concatenate([kvv[:, a * NOPE:(a + 1) * NOPE], rp], axis=1)
                s2 = nn(k_cat, qt[G * s + a]) * c2
                if masked:
                    ki = lax.broadcasted_iota(jnp.int32, (CH, CH), 0)
                    qi = lax.broadcasted_iota(jnp.int32, (CH, CH), 1)
                    s2 = jnp.where(ki <= qi, s2, -1e30)
                s_buf[a, rows, :] = s2
                cm = jnp.max(s2, axis=0, keepdims=True)
                if stats is None:
                    m = cm
                    l = jnp.sum(jnp.exp2(s2 - m), axis=0, keepdims=True)
                else:
                    m0, l0 = stats[a]
                    m = jnp.maximum(m0, cm)
                    l = l0 * jnp.exp2(m0 - m) + jnp.sum(jnp.exp2(s2 - m), axis=0, keepdims=True)
                out.append((m, l))
            return tuple(out)

        stats = phase1(chip, None, True)

        @pl.when(s == 0)
        def _():
            wait_latents()

        stats = lax.fori_loop(0, chip, lambda j, st: phase1(j, st, False), stats)
        lse = [m + jnp.log2(l) for m, l in stats]

        @pl.when(s > 1)
        def _():
            w_wait(3, s - 2)
            w_start(4, s - 2)

        def phase2(j, acc):
            rows = pl.ds(mul(j, CH), CH)
            out = []
            for a in range(G):
                pb = jnp.exp2(s_buf[a, rows, :] - lse[a]).astype(BF16)
                p_buf[a, rows, :] = pb
                v = kv[rows, GW + a * NOPE:GW + (a + 1) * NOPE]
                out.append(acc[a] + tn(v, pb))
            return tuple(out)

        ot = lax.fori_loop(0, chip + 1, phase2, tuple(jnp.zeros((NOPE, CH), F32) for _ in range(G)))
        delta = []
        for a in range(G):
            h = G * s + a
            delta.append(jnp.sum(ot[a] * dot_[a].astype(F32), axis=0, keepdims=True))
            o_ref[h] = ot[a].T.astype(BF16)

        @pl.when(s > 0)
        def _():
            add1(s - 1)
            w_start(2, s - 1)

        def phase3(j, acc):
            rows = pl.ds(mul(j, CH), CH)
            dks, dvs, out = [], [], []
            dr = jnp.zeros((CH, ROPE), F32)
            for a in range(G):
                h = G * s + a
                k = kv[rows, a * NOPE:(a + 1) * NOPE]
                v = kv[rows, GW + a * NOPE:GW + (a + 1) * NOPE]
                pb = p_buf[a, rows, :]
                dp = nn(v, dot_[a])
                ds = (pb.astype(F32) * (dp - delta[a])).astype(BF16)
                out.append((acc[a][0] + tn(k, ds), acc[a][1] + nn(rt[:, rows], ds)))
                dkr = nn(ds, qn[a]) * scale
                dks.append(dkr[:, :NOPE].astype(BF16))
                dr = dr + dkr[:, NOPE:]
                dvs.append(nn(pb, do_ref[h]).astype(BF16))
            dkv = jnp.concatenate(dks + dvs, axis=1)
            drr[j] += dr
            dcr[j] += nt(dkv, w_s)
            dw_ref[s] += nn(ct[j], dkv)

            @pl.when(s == NS - 1)
            def _():
                for cp in d1_copies(j):
                    cp.start()
            return tuple(out)

        dqt = lax.fori_loop(0, chip + 1, phase3, tuple((jnp.zeros((NOPE, CH), F32), jnp.zeros((ROPE, CH), F32)) for _ in range(G)))
        for a in range(G):
            dq_ref[G * s + a, :NOPE] = (dqt[a][0] * scale).astype(BF16)
            dq_ref[G * s + a, NOPE:] = (dqt[a][1] * scale).astype(BF16)

        @pl.when(s > 0)
        def _():
            add2(s - 1)

        @pl.when(s > 1)
        def _():
            deliver(s - 2)

        @pl.when(s > 0)
        def _():
            w_start(3, s - 1)

        w_start(1, s)
        return 0

    lax.fori_loop(0, NS, step, 0)

    outs = [pltpu.make_async_copy(o_ref.at[:, own_rows], o_out.at[mine], lsem.at[6]),
            pltpu.make_async_copy(dq_ref.at[:, :, own_rows], dq_out.at[mine], lsem.at[7]),
            rcopy(o_ref.at[:, oth_rows], o_out.at[mine], xs.at[2], xr.at[2], partner),
            rcopy(dq_ref.at[:, :, oth_rows], dq_out.at[mine], xs.at[3], xr.at[3], partner)]
    for cp in outs:
        cp.start()

    def join(j, _):
        for cp in d1_copies(j):
            cp.wait()
        msg[j, :TOK] = dcr[j, own_rows, :] + rbd[j]
        drt = (drr[j, own_rows, :] + rbr[j]).T
        msg[j, TOK:] = jnp.concatenate([drt[:ROPE // 2], drt[ROPE // 2:]], axis=1)
        return 0
    lax.fori_loop(0, chip + 1, join, 0)

    first, second = pl.ds(0, MSG // 2), pl.ds(MSG // 2, MSG // 2)
    sends = ((chip_x, rcopy(msg.at[chip_x], rbe.at[0], d2s.at[0], d2r.at[0], xn)),
             (chip_y, rcopy(msg.at[chip_y], rbe.at[1], d2s.at[1], d2r.at[1], yn)),
             (chip_d, rcopy(msg.at[chip_d, first], rbe.at[2, first], d2s.at[2], d2r.at[2], dn)),
             (chip_d, rcopy(msg.at[chip_d, second], rly, d2s.at[3], d2r.at[3], yn)))
    relay = rcopy(rly, rbe.at[2, second], d2s.at[4], d2r.at[4], xn)
    low = y == 0

    w_wait(3, NS - 2)
    w_start(4, NS - 2)
    for i in (3, 2):
        @pl.when(sends[i][0] < chip)
        def _(i=i):
            sends[i][1].start()
    add1(NS - 1)
    w_start(2, NS - 1)
    for i in (0, 1):
        @pl.when(sends[i][0] < chip)
        def _(i=i):
            sends[i][1].start()

    @pl.when(low)
    def _():
        sends[3][1].wait_recv()
        relay.start()
    add2(NS - 1)
    deliver(NS - 2)
    w_start(3, NS - 1)
    w_wait(3, NS - 1)
    w_start(4, NS - 1)
    for i in (0, 1):
        @pl.when(sends[i][0] > chip)
        def _(i=i):
            sends[i][1].wait_recv()
            msg[chip] += rbe[i]

    @pl.when(low)
    def _():
        sends[2][1].wait_recv()
        relay.wait_recv()
        msg[chip] += rbe[2]
        relay.wait_send()
    for ch, cp in sends:
        @pl.when(ch < chip)
        def _(cp=cp):
            cp.wait_send()
    dlat_out[...] = msg[chip, :TOK].astype(BF16)
    dr_out[:ROPE // 2] = msg[chip, TOK:, :TOK].astype(BF16)
    dr_out[ROPE // 2:] = msg[chip, TOK:, TOK:].astype(BF16)
    deliver(NS - 1)
    for cp in outs:
        cp.wait()

    def drain(s, _):
        for cp in w_final(s):
            cp.wait()
        return 0
    lax.fori_loop(0, NS, drain, 0)


PARTS = 4


def layout_kernel(o_t, dw, o_ref, dk_ref, dv_ref, stage):
    tok, lat = TOK // PARTS, LAT // PARTS
    for h in range(HEADS):
        stage[pl.ds(h, tok, stride=HEADS), :] = o_t[h].astype(F32)
    o_ref[...] = stage[...].astype(BF16)
    for i in range(2 * NS):
        for a in range(G):
            rows = pl.ds(G * i + a, lat, stride=HEADS)
            dk_ref[rows, :] = dw[i, :, a * NOPE:(a + 1) * NOPE]
            dv_ref[rows, :] = dw[i, :, GW + a * NOPE:GW + (a + 1) * NOPE]


def to_output_layout(o_t, dw):
    tok, lat = TOK // PARTS, LAT // PARTS
    return pl.pallas_call(
        layout_kernel,
        grid=(PARTS,),
        out_shape=(jax.ShapeDtypeStruct((TOK * HEADS, NOPE), BF16),
                   jax.ShapeDtypeStruct((LAT * HEADS, NOPE), F32),
                   jax.ShapeDtypeStruct((LAT * HEADS, NOPE), F32)),
        in_specs=[pl.BlockSpec((HEADS, tok, NOPE), lambda i: (0, i, 0)),
                  pl.BlockSpec((2 * NS, lat, 2 * GW), lambda i: (0, i, 0))],
        out_specs=[pl.BlockSpec((tok * HEADS, NOPE), lambda i: (i, 0)),
                   pl.BlockSpec((lat * HEADS, NOPE), lambda i: (i, 0)),
                   pl.BlockSpec((lat * HEADS, NOPE), lambda i: (i, 0))],
        scratch_shapes=[pltpu.VMEM((tok * HEADS, NOPE), F32)],
        compiler_params=pltpu.CompilerParams(vmem_limit_bytes=60 << 20),
    )(o_t, dw)


def solution(mesh):
    seq_spec = P("cp")

    def local_step(queries, latent, key_rope, w_uk, w_uv, d_out):
        any_spec = pl.BlockSpec(memory_space=pl.ANY)
        vm_spec = pl.BlockSpec(memory_space=pltpu.VMEM)
        dma = pltpu.SemaphoreType.DMA
        vm = pltpu.VMEM
        o_t, dq_t, dw, d_latent, d_key_rope = pl.pallas_call(
            attn_kernel,
            out_shape=(jax.ShapeDtypeStruct((HEADS, TOK, NOPE), BF16),
                       jax.ShapeDtypeStruct((HEADS, QK, TOK), BF16),
                       jax.ShapeDtypeStruct((2 * NS, LAT, 2 * GW), F32),
                       jax.ShapeDtypeStruct((TOK, LAT), BF16),
                       jax.ShapeDtypeStruct((ROPE, TOK), BF16)),
            in_specs=[any_spec] * 6,
            out_specs=[any_spec] * 3 + [vm_spec] * 2,
            scratch_shapes=[vm((TOK * HEADS, NOPE), BF16),
                            vm((LAT, HPC, NOPE), BF16), vm((LAT, HPC, NOPE), BF16),
                            vm((TOK * HEADS, NOPE), F32), vm((HPC, TOK, NOPE), BF16),
                            vm((HPC, QK, CH), BF16), vm((HPC, CH, NOPE), BF16),
                            vm((SEQ, LAT), BF16), vm((ROPE, SEQ), BF16), vm((SEQ, ROPE), BF16),
                            vm((HPC, LAT, NOPE), BF16), vm((HPC, LAT, NOPE), BF16),
                            vm((HPC, CH, NOPE), BF16), vm((HPC, QK, CH), BF16),
                            vm((NS, LAT, 2 * GW), F32), vm((NS, LAT, 2 * GW), F32),
                            vm((NCHIP, CH, LAT), F32), vm((NCHIP, CH, ROPE), F32), vm((NCHIP, MSG, LAT), F32),
                            vm((NCHIP, LAT, CH), BF16), vm((SEQ, 2 * GW), BF16),
                            vm((G, CH, QK), BF16), vm((G, NOPE, CH), BF16),
                            vm((G, SEQ, CH), F32), vm((G, SEQ, CH), BF16),
                            vm((2, 256, GW), F32), vm((2, 128, GW), F32),
                            vm((NCHIP, TOK, LAT), F32), vm((NCHIP, TOK, ROPE), F32),
                            vm((3, MSG, LAT), F32), vm((MSG // 2, LAT), F32),
                            dma((8,)), dma((4,)), dma((4,)), dma((2, 7)), dma((2, 7)),
                            dma((4, 2)), dma((4, 2)), dma((NS,)), dma((NS,)), dma((NS,)),
                            dma((2, NCHIP)), dma((2, NCHIP)), dma((5,)), dma((5,))],
            compiler_params=pltpu.CompilerParams(vmem_limit_bytes=63 << 20, collective_id=0, has_side_effects=True),
            cost_estimate=pl.CostEstimate(flops=30 * 10**9, bytes_accessed=20 << 20, transcendentals=10**7),
        )(jnp.transpose(queries, (1, 2, 0)), d_out.reshape(TOK * HEADS, NOPE), latent, key_rope.T, w_uk, w_uv)

        o, dk, dv = to_output_layout(o_t, dw)
        return (o.reshape(TOK, HEADS, NOPE), jnp.transpose(dq_t, (2, 0, 1)), d_latent, d_key_rope.T,
                dk.reshape(LAT, HEADS, NOPE), dv.reshape(LAT, HEADS, NOPE))

    return jax.shard_map(local_step, mesh=mesh,
                         in_specs=(seq_spec, seq_spec, seq_spec, P(), P(), seq_spec),
                         out_specs=(seq_spec, seq_spec, seq_spec, seq_spec, P(), P()),
                         check_vma=False)
```

```python
import math
import jax
import jax.numpy as jnp
from jax import lax
from jax.experimental import pallas as pl
from jax.experimental.pallas import tpu as pltpu
from jax.sharding import PartitionSpec as P

F32 = jnp.float32
BF16 = jnp.bfloat16
TOK = 256
CH = 512
KC = 1024
HEADS = 16
HPC = 8
NS = HPC
NOPE = 128
ROPE = 64
QK = NOPE + ROPE
LAT = 512
MSG = TOK + ROPE // 2
NCHIP = 4
SEQ = CH * NCHIP
MESH = pl.DeviceIdType.MESH
A_COLS = pl.ds(0, NOPE)
B_COLS = pl.ds(NOPE, NOPE)


def nt(a, b):
    return lax.dot_general(a, b, (((1,), (1,)), ((), ())), preferred_element_type=F32)


def nn(a, b):
    return lax.dot_general(a, b, (((1,), (0,)), ((), ())), preferred_element_type=F32)


def tn(a, b):
    return lax.dot_general(a, b, (((0,), (0,)), ((), ())), preferred_element_type=F32)


def mul(i, n):
    return pl.multiple_of(i * n, n)


def attn_kernel(q_in, do_in, c_in, r_in, wk_in, wv_in,
                o_out, dq_out, dw_out, dlat_out, dr_out,
                do_raw, wk_raw, wv_raw, stage, do_snd,
                qt, do_ref, c_ref, rt, rn, wk, wv, o_ref, dq_ref, dw_ref, dwo, dcr, drr, msg,
                ct, kv, qn, dot_, s_buf, p_buf, rb1, rb2, rbd, rbr, rbx, rby, rbh,
                lsem, xs, xr, cs, crs, ws, wr, fs, fr, fl, d1s, d1r, d2s, d2r):
    scale = 1.0 / math.sqrt(QK)
    c2 = scale * math.log2(math.e)
    me = lax.axis_index("cp")
    core = lax.rem(me, 2)
    chip = lax.div(me, 2)
    x = lax.rem(chip, 2)
    y = lax.div(chip, 2)
    partner = me + 1 - 2 * core
    xn = me + 2 - 4 * x
    yn = me + 4 - 8 * y
    dn = xn + 4 - 8 * y

    def rcopy(src, dst, ss, rs, dev):
        return pltpu.make_async_remote_copy(src_ref=src, dst_ref=dst, send_sem=ss, recv_sem=rs,
                                            device_id=(dev,), device_id_type=MESH)

    my_rows = pl.ds(mul(me, TOK), TOK)
    own_rows = pl.ds(mul(core, TOK), TOK)
    oth_rows = pl.ds(mul(1 - core, TOK), TOK)
    mine = pl.ds(mul(core, HPC), HPC)

    other = pl.ds(mul(1 - core, HPC), HPC)

    local = [pltpu.make_async_copy(c_in, c_ref.at[my_rows], lsem.at[0]),
             pltpu.make_async_copy(r_in, rt.at[:, my_rows], lsem.at[1]),
             pltpu.make_async_copy(q_in.at[mine], qt.at[:, :, own_rows], lsem.at[2]),
             pltpu.make_async_copy(do_in, do_raw, lsem.at[3]),
             pltpu.make_async_copy(wk_in.at[:, mine], wk_raw, lsem.at[4]),
             pltpu.make_async_copy(wv_in.at[:, mine], wv_raw, lsem.at[5])]
    for cp in local:
        cp.start()

    bar = pltpu.get_barrier_semaphore()
    for peer in (partner, xn, yn, dn):
        pl.semaphore_signal(bar, inc=1, device_id=(peer,), device_id_type=MESH)
    pl.semaphore_wait(bar, 4)

    local[0].wait()
    local[1].wait()

    def latent_copies(i, src, dev):
        rows = pl.ds(mul(src, TOK), TOK)
        return (rcopy(c_ref.at[rows], c_ref.at[rows], cs.at[0, i], crs.at[0, i], dev),
                rcopy(rt.at[:, rows], rt.at[:, rows], cs.at[1, i], crs.at[1, i], dev))

    c_direct = [latent_copies(i, me, dev) for i, dev in enumerate((partner, xn, yn, dn))]
    for pair in c_direct:
        for cp in pair:
            cp.start()

    heads = [rcopy(q_in.at[other], qt.at[:, :, own_rows], xs.at[0], xr.at[0], partner),
             rcopy(do_snd, do_ref.at[:, own_rows], xs.at[1], xr.at[1], partner)]
    heads[0].start()
    local[3].wait()

    def pick(h, rows, stride):
        return stage[pl.ds(h, rows, stride=stride), :].astype(BF16)

    def widen(i, _):
        rows = pl.ds(mul(i, 256), 256)
        stage[rows, :] = do_raw[rows, :].astype(F32)
        return 0
    lax.fori_loop(0, TOK * HEADS // 256, widen, 0)
    is0 = core == 0
    for i in range(HPC):
        lo = pick(i, TOK, HEADS)
        hi = pick(i + HPC, TOK, HEADS)
        do_ref[i, own_rows, :] = jnp.where(is0, lo, hi)
        do_snd[i] = jnp.where(is0, hi, lo)
    heads[1].start()
    for t, (raw, out) in enumerate(((wk_raw, wk), (wv_raw, wv))):
        local[4 + t].wait()

        def body(i, _, raw=raw):
            ls = pl.ds(mul(i, 32), 32)
            stage[pl.ds(mul(i, 256), 256), :] = raw[ls].astype(F32).reshape(256, NOPE)
            return 0
        lax.fori_loop(0, LAT // 32, body, 0)
        for i in range(HPC):
            out[i] = pick(i, LAT, HPC)

    def zero_dc(j, _):
        rows = pl.ds(mul(j, KC), KC)
        dcr[rows, :] = jnp.zeros((KC, LAT), F32)
        drr[rows, :] = jnp.zeros((KC, ROPE), F32)
        return 0
    lax.fori_loop(0, y + 1, zero_dc, 0)
    local[2].wait()
    for cp in heads:
        cp.wait()
    for cp in c_direct[0]:
        cp.wait()

    def turn(j):
        rows = pl.ds(mul(j, KC), KC)
        ct[j] = c_ref[rows, :].T
        rn[rows, :] = rt[:, rows].T

    c_fwd = [None] + [latent_copies(3 + i, src, partner) for i, src in ((1, xn), (2, yn), (3, dn))]

    def wait_latents(which):
        for i in which:
            for cp in c_direct[i]:
                cp.wait()
            for cp in c_fwd[i]:
                cp.start()
        for i in which:
            for cp in c_fwd[i]:
                cp.wait()

    wait_latents((1,))
    turn(y)

    hx = pl.ds(mul(x, 256), 256)
    hx1 = pl.ds(mul(1 - x, 256), 256)
    hy = pl.ds(mul(y, 256), 256)
    hy1 = pl.ds(mul(1 - y, 256), 256)
    qa = pl.ds(pl.multiple_of(x * 256 + y * 128, 128), 128)
    qa1 = pl.ds(pl.multiple_of(x * 256 + (1 - y) * 128, 128), 128)
    qb = pl.ds(pl.multiple_of(y * 256 + x * 128, 128), 128)
    qb1 = pl.ds(pl.multiple_of(y * 256 + (1 - x) * 128, 128), 128)

    def w_copy(phase, s):
        par = lax.rem(s, 2)
        if phase == 1:
            pair = ((dw_ref.at[s, hx1, A_COLS], rb1.at[par, 0], xn), (dw_ref.at[s, hy1, B_COLS], rb1.at[par, 1], yn))
        elif phase == 2:
            pair = ((dw_ref.at[s, qa1, A_COLS], rb2.at[par, 0], yn), (dw_ref.at[s, qb1, B_COLS], rb2.at[par, 1], xn))
        elif phase == 3:
            pair = ((dwo.at[s, qa, A_COLS], dwo.at[s, qa, A_COLS], yn),
                    (dwo.at[s, qb, B_COLS], dwo.at[s, qb, B_COLS], xn))
        else:
            pair = ((dwo.at[s, hx, A_COLS], dwo.at[s, hx, A_COLS], xn),
                    (dwo.at[s, hy, B_COLS], dwo.at[s, hy, B_COLS], yn))
        return [rcopy(a, b, ws.at[phase - 1, par, i], wr.at[phase - 1, par, i], d)
                for i, (a, b, d) in enumerate(pair)]

    def w_start(phase, s):
        for cp in w_copy(phase, s):
            cp.start()

    def w_wait(phase, s):
        for cp in w_copy(phase, s):
            cp.wait()

    def w_final(s, late):
        slot = core * NS + s
        parts = ((hx1, A_COLS), (hy1, B_COLS)) if late else ((hx, A_COLS), (hy, B_COLS))
        return [rcopy(dwo.at[s, r, c], dw_out.at[slot, r, c], fs.at[s, 2 * late + i], fr.at[s, 2 * late + i], partner)
                for i, (r, c) in enumerate(parts)]

    def w_local(s):
        return pltpu.make_async_copy(dwo.at[s], dw_out.at[core * NS + s], fl.at[s])

    def stage2(s):
        par = lax.rem(s, 2)
        w_wait(1, s)
        dw_ref[s, hx, A_COLS] += rb1[par, 0]
        dw_ref[s, hy, B_COLS] += rb1[par, 1]
        w_start(2, s)

    def stage3(s):
        par = lax.rem(s, 2)
        w_wait(2, s)
        dwo[s, qa, A_COLS] = dw_ref[s, qa, A_COLS] + rb2[par, 0]
        dwo[s, qb, B_COLS] = dw_ref[s, qb, B_COLS] + rb2[par, 1]
        w_start(3, s)

    def stage4(s):
        w_wait(3, s)
        w_start(4, s)
        for cp in w_final(s, 0):
            cp.start()

    def stage5(s):
        w_wait(4, s)
        for cp in w_final(s, 1):
            cp.start()
        w_local(s).start()

    def d1_copies(j):
        rows = pl.ds(pl.multiple_of(j * CH + (1 - core) * TOK, TOK), TOK)
        return (rcopy(dcr.at[rows], rbd.at[j], d1s.at[0, j], d1r.at[0, j], partner),
                rcopy(drr.at[rows], rbr.at[j], d1s.at[1, j], d1r.at[1, j], partner))

    def step(s, _):
        dw_ref[s] = jnp.zeros((LAT, 2 * NOPE), F32)
        qn[...] = qt[s].T
        dot_[...] = do_ref[s].T
        w_s = jnp.concatenate([wk[s], wv[s]], axis=1)

        def phase1(j, masked):
            rows = pl.ds(mul(j, KC), KC)
            kvv = nn(c_ref[rows, :], w_s).astype(BF16)
            kv[rows, :] = kvv
            k_cat = jnp.concatenate([kvv[:, :NOPE], rn[rows, :]], axis=1)
            s2 = nn(k_cat, qt[s]) * c2
            if masked:
                ki = lax.broadcasted_iota(jnp.int32, (KC, CH), 0)
                qi = lax.broadcasted_iota(jnp.int32, (KC, CH), 1)
                s2 = jnp.where(ki - qi <= x * CH, s2, -1e30)
            s_buf[rows, :] = s2
            m = jnp.max(s2, axis=0, keepdims=True)
            return m, jnp.sum(jnp.exp2(s2 - m), axis=0, keepdims=True)

        stats = phase1(y, True)

        @pl.when(s == 0)
        def _():
            @pl.when(y == 1)
            def _():
                wait_latents((2, 3))
                turn(0)

        def more(j, st):
            m0, l0 = st
            m1, l1 = phase1(j, False)
            m = jnp.maximum(m0, m1)
            return m, l0 * jnp.exp2(m0 - m) + l1 * jnp.exp2(m1 - m)

        m, l = lax.fori_loop(0, y, more, stats)
        lse = m + jnp.log2(l)

        def phase2(j, acc):
            rows = pl.ds(mul(j, KC), KC)
            pb = jnp.exp2(s_buf[rows, :] - lse).astype(BF16)
            p_buf[rows, :] = pb
            return acc + tn(kv[rows, NOPE:], pb)

        ot = lax.fori_loop(0, y + 1, phase2, jnp.zeros((NOPE, CH), F32))
        delta = jnp.sum(ot * dot_[...].astype(F32), axis=0, keepdims=True)
        o_ref[s] = ot.T.astype(BF16)

        @pl.when(s > 1)
        def _():
            stage3(s - 2)

        def phase3(j, acc):
            rows = pl.ds(mul(j, KC), KC)
            k = kv[rows, :NOPE]
            v = kv[rows, NOPE:]
            pb = p_buf[rows, :]
            dp = nn(v, dot_[...])
            ds = (pb.astype(F32) * (dp - delta)).astype(BF16)
            dkr = nn(ds, qn[...]) * scale
            dv = nn(pb, do_ref[s])
            dkv = jnp.concatenate([dkr[:, :NOPE].astype(BF16), dv.astype(BF16)], axis=1)
            drr[rows, :] += dkr[:, NOPE:]
            dcr[rows, :] += nt(dkv, w_s)
            dw_ref[s] += nn(ct[j], dkv)
            out = (acc[0] + tn(k, ds), acc[1] + nn(rt[:, rows], ds))

            @pl.when(s == NS - 1)
            def _():
                for t in range(2):
                    for cp in d1_copies(2 * j + t):
                        cp.start()

            @pl.when(j == 0)
            def _():
                @pl.when(s > 0)
                def _():
                    stage2(s - 1)
            return out

        dqn, dqr = lax.fori_loop(0, y + 1, phase3, (jnp.zeros((NOPE, CH), F32), jnp.zeros((ROPE, CH), F32)))
        w_start(1, s)
        dq_ref[s, :NOPE] = (dqn * scale).astype(BF16)
        dq_ref[s, NOPE:] = (dqr * scale).astype(BF16)

        @pl.when(s > 1)
        def _():
            stage4(s - 2)

        @pl.when(s > 2)
        def _():
            stage5(s - 3)
        return 0

    lax.fori_loop(0, NS, step, 0)

    @pl.when(y == 0)
    def _():
        wait_latents((2, 3))

    outs = [pltpu.make_async_copy(o_ref.at[:, own_rows], o_out.at[mine], lsem.at[6]),
            pltpu.make_async_copy(dq_ref.at[:, :, own_rows], dq_out.at[mine], lsem.at[7]),
            rcopy(o_ref.at[:, oth_rows], o_out.at[mine], xs.at[2], xr.at[2], partner),
            rcopy(dq_ref.at[:, :, oth_rows], dq_out.at[mine], xs.at[3], xr.at[3], partner)]
    for cp in outs:
        cp.start()

    def join(j):
        for cp in d1_copies(j):
            cp.wait()
        rows = pl.ds(pl.multiple_of(j * CH + core * TOK, TOK), TOK)
        msg[j, :TOK] = dcr[rows, :] + rbd[j]
        drt = (drr[rows, :] + rbr[j]).T
        msg[j, TOK:] = jnp.concatenate([drt[:ROPE // 2], drt[ROPE // 2:]], axis=1)


    halves = (pl.ds(0, MSG // 2), pl.ds(MSG // 2, MSG // 2))

    def to_x(j):
        return [rcopy(msg.at[j, h], rbx.at[h], d2s.at[0, i], d2r.at[0, i], xn) for i, h in enumerate(halves)]

    def to_y(j):
        return [rcopy(msg.at[j, h], rby.at[h], d2s.at[1, i], d2r.at[1, i], yn) for i, h in enumerate(halves)]

    half_x = rcopy(msg.at[0, halves[0]], rbh, d2s.at[2, 0], d2r.at[2, 0], xn)
    half_y = rcopy(msg.at[0, halves[1]], rbh, d2s.at[2, 1], d2r.at[2, 0], yn)

    stage3(NS - 2)
    join(0)
    stage2(NS - 1)

    @pl.when(chip == 3)
    def _():
        half_x.start()
        half_y.start()
    join(1)

    @pl.when(chip == 2)
    def _():
        for cp in to_x(1):
            cp.start()
    stage5(NS - 3)

    @pl.when(y == 1)
    def _():
        join(2)
    stage4(NS - 2)
    stage3(NS - 1)

    @pl.when(chip == 2)
    def _():
        half_x.wait_recv()
        msg[0, halves[0]] += rbh[...]

    @pl.when(chip == 1)
    def _():
        half_y.wait_recv()
        msg[0, halves[1]] += rbh[...]
    stage4(NS - 1)

    @pl.when(chip == 1)
    def _():
        for cp in to_x(0):
            cp.start()

    @pl.when(chip == 2)
    def _():
        for cp in to_y(0):
            cp.start()

    @pl.when(chip == 3)
    def _():
        for cp in to_x(2):
            cp.start()
        for i, h in enumerate(halves):
            to_x(1)[i].wait_recv()
            msg[1, h] += rbx[h]
            to_y(1)[i].start()

    @pl.when(y == 1)
    def _():
        join(3)
    stage5(NS - 2)
    stage5(NS - 1)

    def all_of(copies, recv):
        for cp in copies:
            if recv:
                cp.wait_recv()
            else:
                cp.wait_send()

    @pl.when(chip != 3)
    def _():
        @pl.when(chip != 1)
        def _():
            all_of(to_x(0), True)
            msg[chip] += rbx[...]

        @pl.when(chip != 2)
        def _():
            all_of(to_y(0), True)
            msg[chip] += rby[...]

    dlat_out[...] = msg[chip, :TOK].astype(BF16)
    dr_out[:ROPE // 2] = msg[chip, TOK:, :TOK].astype(BF16)
    dr_out[ROPE // 2:] = msg[chip, TOK:, TOK:].astype(BF16)

    @pl.when(chip != 0)
    def _():
        all_of(to_x(0), False)

        @pl.when(chip != 1)
        def _():
            all_of(to_y(0), False)

    @pl.when(chip == 3)
    def _():
        all_of((half_x, half_y), False)
    for cp in outs:
        cp.wait()

    def drain(s, _):
        for cp in w_final(s, 0) + w_final(s, 1):
            cp.wait()
        w_local(s).wait()
        return 0
    lax.fori_loop(0, NS, drain, 0)


PARTS = 2


def layout_kernel(o_t, dw, dq_t, dc, dr, o_ref, dk_ref, dv_ref, dq_ref, dc_ref, dr_ref):
    def by_row(v):
        return jnp.swapaxes(v, 0, 1).reshape(v.shape[0] * v.shape[1], NOPE)

    dk_ref[...] = by_row(dw[:, :, :NOPE])
    dv_ref[...] = by_row(dw[:, :, NOPE:])
    o_ref[...] = by_row(o_t[...].astype(F32)).astype(BF16)
    dq_ref[...] = dq_t[...]
    dc_ref[...] = dc[...]
    dr_ref[...] = dr[...]


def to_output_layout(o_t, dw, dq_t, dc, dr):
    tok, lat = TOK // PARTS, LAT // PARTS
    passed = [pl.BlockSpec((HEADS // PARTS, QK, TOK), lambda i: (i, 0, 0)),
              pl.BlockSpec((tok, LAT), lambda i: (i, 0)),
              pl.BlockSpec((ROPE // PARTS, TOK), lambda i: (i, 0))]
    return pl.pallas_call(
        layout_kernel,
        grid=(PARTS,),
        out_shape=(jax.ShapeDtypeStruct((TOK * HEADS, NOPE), BF16),
                   jax.ShapeDtypeStruct((LAT * HEADS, NOPE), F32),
                   jax.ShapeDtypeStruct((LAT * HEADS, NOPE), F32),
                   jax.ShapeDtypeStruct(dq_t.shape, BF16),
                   jax.ShapeDtypeStruct(dc.shape, BF16),
                   jax.ShapeDtypeStruct(dr.shape, BF16)),
        in_specs=[pl.BlockSpec((HEADS, tok, NOPE), lambda i: (0, i, 0)),
                  pl.BlockSpec((HEADS, lat, 2 * NOPE), lambda i: (0, i, 0))] + passed,
        out_specs=[pl.BlockSpec((tok * HEADS, NOPE), lambda i: (i, 0)),
                   pl.BlockSpec((lat * HEADS, NOPE), lambda i: (i, 0)),
                   pl.BlockSpec((lat * HEADS, NOPE), lambda i: (i, 0))] + passed,
        compiler_params=pltpu.CompilerParams(vmem_limit_bytes=60 << 20),
    )(o_t, dw, dq_t, dc, dr)


def solution(mesh):
    seq_spec = P("cp")

    def local_step(queries, latent, key_rope, w_uk, w_uv, d_out):
        any_spec = pl.BlockSpec(memory_space=pl.ANY)
        vm_spec = pl.BlockSpec(memory_space=pltpu.VMEM)
        dma = pltpu.SemaphoreType.DMA
        vm = pltpu.VMEM
        o_t, dq_t, dw, d_latent, d_key_rope = pl.pallas_call(
            attn_kernel,
            out_shape=(jax.ShapeDtypeStruct((HEADS, TOK, NOPE), BF16),
                       jax.ShapeDtypeStruct((HEADS, QK, TOK), BF16),
                       jax.ShapeDtypeStruct((HEADS, LAT, 2 * NOPE), F32),
                       jax.ShapeDtypeStruct((TOK, LAT), BF16),
                       jax.ShapeDtypeStruct((ROPE, TOK), BF16)),
            in_specs=[any_spec] * 6,
            out_specs=[any_spec] * 3 + [vm_spec] * 2,
            scratch_shapes=[vm((TOK * HEADS, NOPE), BF16),
                            vm((LAT, HPC, NOPE), BF16), vm((LAT, HPC, NOPE), BF16),
                            vm((TOK * HEADS, NOPE), F32), vm((HPC, TOK, NOPE), BF16),
                            vm((HPC, QK, CH), BF16), vm((HPC, CH, NOPE), BF16),
                            vm((SEQ, LAT), BF16), vm((ROPE, SEQ), BF16), vm((SEQ, ROPE), BF16),
                            vm((HPC, LAT, NOPE), BF16), vm((HPC, LAT, NOPE), BF16),
                            vm((HPC, CH, NOPE), BF16), vm((HPC, QK, CH), BF16),
                            vm((NS, LAT, 2 * NOPE), F32), vm((NS, LAT, 2 * NOPE), F32),
                            vm((SEQ, LAT), F32), vm((SEQ, ROPE), F32), vm((NCHIP, MSG, LAT), F32),
                            vm((SEQ // KC, LAT, KC), BF16), vm((SEQ, 2 * NOPE), BF16),
                            vm((CH, QK), BF16), vm((NOPE, CH), BF16),
                            vm((SEQ, CH), F32), vm((SEQ, CH), BF16),
                            vm((2, 2, 256, NOPE), F32), vm((2, 2, 128, NOPE), F32),
                            vm((NCHIP, TOK, LAT), F32), vm((NCHIP, TOK, ROPE), F32),
                            vm((MSG, LAT), F32), vm((MSG, LAT), F32), vm((MSG // 2, LAT), F32),
                            dma((8,)), dma((4,)), dma((4,)), dma((2, 7)), dma((2, 7)),
                            dma((4, 2, 2)), dma((4, 2, 2)), dma((NS, 4)), dma((NS, 4)), dma((NS,)),
                            dma((2, NCHIP)), dma((2, NCHIP)), dma((3, 2)), dma((3, 2))],
            compiler_params=pltpu.CompilerParams(vmem_limit_bytes=63 << 20, collective_id=0, has_side_effects=True),
            cost_estimate=pl.CostEstimate(flops=30 * 10**9, bytes_accessed=20 << 20, transcendentals=10**7),
        )(jnp.transpose(queries, (1, 2, 0)), d_out.reshape(TOK * HEADS, NOPE), latent, key_rope.T, w_uk, w_uv)

        o, dk, dv, dq_t, d_latent, d_key_rope = to_output_layout(o_t, dw, dq_t, d_latent, d_key_rope)
        return (o.reshape(TOK, HEADS, NOPE), jnp.transpose(dq_t, (2, 0, 1)), d_latent, d_key_rope.T,
                dk.reshape(LAT, HEADS, NOPE), dv.reshape(LAT, HEADS, NOPE))

    return jax.shard_map(local_step, mesh=mesh,
                         in_specs=(seq_spec, seq_spec, seq_spec, P(), P(), seq_spec),
                         out_specs=(seq_spec, seq_spec, seq_spec, seq_spec, P(), P()),
                         check_vma=False)
```

```python
import math
import jax
import jax.numpy as jnp
from jax import lax
from jax.experimental import pallas as pl
from jax.experimental.pallas import tpu as pltpu
from jax.sharding import PartitionSpec as P

F32 = jnp.float32
BF16 = jnp.bfloat16
TOK = 256
CH = 512
KC = 1024
HEADS = 16
HPC = 8
NS = HPC
NOPE = 128
ROPE = 64
QK = NOPE + ROPE
LAT = 512
MSG = TOK + ROPE // 2
NCHIP = 4
SEQ = CH * NCHIP
MESH = pl.DeviceIdType.MESH
A_COLS = pl.ds(0, NOPE)
B_COLS = pl.ds(NOPE, NOPE)


def nt(a, b):
    return lax.dot_general(a, b, (((1,), (1,)), ((), ())), preferred_element_type=F32)


def nn(a, b):
    return lax.dot_general(a, b, (((1,), (0,)), ((), ())), preferred_element_type=F32)


def tn(a, b):
    return lax.dot_general(a, b, (((0,), (0,)), ((), ())), preferred_element_type=F32)


def mul(i, n):
    return pl.multiple_of(i * n, n)


def attn_kernel(q_in, do_in, c_in, r_in, wk_in, wv_in,
                o_out, dq_out, dw_out, dlat_out, dr_out,
                do_raw, wk_raw, wv_raw, stage, do_snd,
                qt, do_ref, c_ref, rt, rn, wk, wv, o_ref, dq_ref, dw_ref, dwo, dcr, drr, msg,
                ct, kv, qn, dot_, s_buf, p_buf, rb1, rb2, rbd, rbr, rbx, rby, rbh,
                lsem, xs, xr, cs, crs, ws, wr, fs, fr, fl, d1s, d1r, d2s, d2r):
    scale = 1.0 / math.sqrt(QK)
    c2 = scale * math.log2(math.e)
    me = lax.axis_index("cp")
    core = lax.rem(me, 2)
    chip = lax.div(me, 2)
    x = lax.rem(chip, 2)
    y = lax.div(chip, 2)
    partner = me + 1 - 2 * core
    xn = me + 2 - 4 * x
    yn = me + 4 - 8 * y
    dn = xn + 4 - 8 * y

    def rcopy(src, dst, ss, rs, dev):
        return pltpu.make_async_remote_copy(src_ref=src, dst_ref=dst, send_sem=ss, recv_sem=rs,
                                            device_id=(dev,), device_id_type=MESH)

    my_rows = pl.ds(mul(me, TOK), TOK)
    own_rows = pl.ds(mul(core, TOK), TOK)
    oth_rows = pl.ds(mul(1 - core, TOK), TOK)
    mine = pl.ds(mul(core, HPC), HPC)

    other = pl.ds(mul(1 - core, HPC), HPC)

    local = [pltpu.make_async_copy(c_in, c_ref.at[my_rows], lsem.at[0]),
             pltpu.make_async_copy(r_in, rt.at[:, my_rows], lsem.at[1]),
             pltpu.make_async_copy(q_in.at[mine], qt.at[:, :, own_rows], lsem.at[2]),
             pltpu.make_async_copy(do_in, do_raw, lsem.at[3]),
             pltpu.make_async_copy(wk_in.at[:, mine], wk_raw, lsem.at[4]),
             pltpu.make_async_copy(wv_in.at[:, mine], wv_raw, lsem.at[5])]
    for cp in local:
        cp.start()

    bar = pltpu.get_barrier_semaphore()
    for peer in (partner, xn, yn, dn):
        pl.semaphore_signal(bar, inc=1, device_id=(peer,), device_id_type=MESH)
    pl.semaphore_wait(bar, 4)

    local[0].wait()
    local[1].wait()

    def latent_copies(i, src, dev):
        rows = pl.ds(mul(src, TOK), TOK)
        return (rcopy(c_ref.at[rows], c_ref.at[rows], cs.at[0, i], crs.at[0, i], dev),
                rcopy(rt.at[:, rows], rt.at[:, rows], cs.at[1, i], crs.at[1, i], dev))

    c_direct = [latent_copies(i, me, dev) for i, dev in enumerate((partner, xn, yn, dn))]
    for pair in c_direct:
        for cp in pair:
            cp.start()

    heads = [rcopy(q_in.at[other], qt.at[:, :, own_rows], xs.at[0], xr.at[0], partner),
             rcopy(do_snd, do_ref.at[:, own_rows], xs.at[1], xr.at[1], partner)]
    heads[0].start()
    local[3].wait()

    def pick(h, rows, stride):
        return stage[pl.ds(h, rows, stride=stride), :].astype(BF16)

    def widen(i, _):
        rows = pl.ds(mul(i, 256), 256)
        stage[rows, :] = do_raw[rows, :].astype(F32)
        return 0
    lax.fori_loop(0, TOK * HEADS // 256, widen, 0)
    is0 = core == 0
    for i in range(HPC):
        lo = pick(i, TOK, HEADS)
        hi = pick(i + HPC, TOK, HEADS)
        do_ref[i, own_rows, :] = jnp.where(is0, lo, hi)
        do_snd[i] = jnp.where(is0, hi, lo)
    heads[1].start()
    for t, (raw, out) in enumerate(((wk_raw, wk), (wv_raw, wv))):
        local[4 + t].wait()

        def body(i, _, raw=raw):
            ls = pl.ds(mul(i, 32), 32)
            stage[pl.ds(mul(i, 256), 256), :] = raw[ls].astype(F32).reshape(256, NOPE)
            return 0
        lax.fori_loop(0, LAT // 32, body, 0)
        for i in range(HPC):
            out[i] = pick(i, LAT, HPC)

    def zero_dc(j, _):
        rows = pl.ds(mul(j, KC), KC)
        dcr[rows, :] = jnp.zeros((KC, LAT), F32)
        drr[rows, :] = jnp.zeros((KC, ROPE), F32)
        return 0
    lax.fori_loop(0, y + 1, zero_dc, 0)
    local[2].wait()
    for cp in heads:
        cp.wait()
    for cp in c_direct[0]:
        cp.wait()

    def turn(j):
        rows = pl.ds(mul(j, KC), KC)
        ct[j] = c_ref[rows, :].T
        rn[rows, :] = rt[:, rows].T

    c_fwd = [None] + [latent_copies(3 + i, src, partner) for i, src in ((1, xn), (2, yn), (3, dn))]

    def wait_latents(which):
        for i in which:
            for cp in c_direct[i]:
                cp.wait()
            for cp in c_fwd[i]:
                cp.start()
        for i in which:
            for cp in c_fwd[i]:
                cp.wait()

    wait_latents((1,))
    turn(y)

    hx = pl.ds(mul(x, 256), 256)
    hx1 = pl.ds(mul(1 - x, 256), 256)
    hy = pl.ds(mul(y, 256), 256)
    hy1 = pl.ds(mul(1 - y, 256), 256)
    qa = pl.ds(pl.multiple_of(x * 256 + y * 128, 128), 128)
    qa1 = pl.ds(pl.multiple_of(x * 256 + (1 - y) * 128, 128), 128)
    qb = pl.ds(pl.multiple_of(y * 256 + x * 128, 128), 128)
    qb1 = pl.ds(pl.multiple_of(y * 256 + (1 - x) * 128, 128), 128)

    def w_copy(phase, s):
        par = lax.rem(s, 2)
        if phase == 1:
            pair = ((dw_ref.at[s, hx1, A_COLS], rb1.at[par, 0], xn), (dw_ref.at[s, hy1, B_COLS], rb1.at[par, 1], yn))
        elif phase == 2:
            pair = ((dw_ref.at[s, qa1, A_COLS], rb2.at[par, 0], yn), (dw_ref.at[s, qb1, B_COLS], rb2.at[par, 1], xn))
        elif phase == 3:
            pair = ((dwo.at[s, qa, A_COLS], dwo.at[s, qa, A_COLS], yn),
                    (dwo.at[s, qb, B_COLS], dwo.at[s, qb, B_COLS], xn))
        else:
            pair = ((dwo.at[s, hx, A_COLS], dwo.at[s, hx, A_COLS], xn),
                    (dwo.at[s, hy, B_COLS], dwo.at[s, hy, B_COLS], yn))
        return [rcopy(a, b, ws.at[phase - 1, par, i], wr.at[phase - 1, par, i], d)
                for i, (a, b, d) in enumerate(pair)]

    def w_start(phase, s):
        for cp in w_copy(phase, s):
            cp.start()

    def w_wait(phase, s):
        for cp in w_copy(phase, s):
            cp.wait()

    def w_final(s, late):
        slot = core * NS + s
        parts = ((hx1, A_COLS), (hy1, B_COLS)) if late else ((hx, A_COLS), (hy, B_COLS))
        return [rcopy(dwo.at[s, r, c], dw_out.at[slot, r, c], fs.at[s, 2 * late + i], fr.at[s, 2 * late + i], partner)
                for i, (r, c) in enumerate(parts)]

    def w_local(s):
        return pltpu.make_async_copy(dwo.at[s], dw_out.at[core * NS + s], fl.at[s])

    def stage2(s):
        par = lax.rem(s, 2)
        w_wait(1, s)
        dw_ref[s, hx, A_COLS] += rb1[par, 0]
        dw_ref[s, hy, B_COLS] += rb1[par, 1]
        w_start(2, s)

    def stage3(s):
        par = lax.rem(s, 2)
        w_wait(2, s)
        dwo[s, qa, A_COLS] = dw_ref[s, qa, A_COLS] + rb2[par, 0]
        dwo[s, qb, B_COLS] = dw_ref[s, qb, B_COLS] + rb2[par, 1]
        w_start(3, s)

    def stage4(s):
        w_wait(3, s)
        w_start(4, s)
        for cp in w_final(s, 0):
            cp.start()

    def stage5(s):
        w_wait(4, s)
        for cp in w_final(s, 1):
            cp.start()
        w_local(s).start()

    def d1_copies(j):
        rows = pl.ds(pl.multiple_of(j * CH + (1 - core) * TOK, TOK), TOK)
        return (rcopy(dcr.at[rows], rbd.at[j], d1s.at[0, j], d1r.at[0, j], partner),
                rcopy(drr.at[rows], rbr.at[j], d1s.at[1, j], d1r.at[1, j], partner))

    def step(s, _):
        dw_ref[s] = jnp.zeros((LAT, 2 * NOPE), F32)
        qn[...] = qt[s].T
        dot_[...] = do_ref[s].T
        w_s = jnp.concatenate([wk[s], wv[s]], axis=1)

        def phase1(j, masked):
            rows = pl.ds(mul(j, KC), KC)
            kvv = nn(c_ref[rows, :], w_s).astype(BF16)
            kv[rows, :] = kvv
            k_cat = jnp.concatenate([kvv[:, :NOPE], rn[rows, :]], axis=1)
            s2 = nn(k_cat, qt[s]) * c2
            if masked:
                ki = lax.broadcasted_iota(jnp.int32, (KC, CH), 0)
                qi = lax.broadcasted_iota(jnp.int32, (KC, CH), 1)
                s2 = jnp.where(ki - qi <= x * CH, s2, -1e30)
            s_buf[rows, :] = s2
            m = jnp.max(s2, axis=0, keepdims=True)
            return m, jnp.sum(jnp.exp2(s2 - m), axis=0, keepdims=True)

        stats = phase1(y, True)

        @pl.when(s == 0)
        def _():
            @pl.when(y == 1)
            def _():
                wait_latents((2, 3))
                turn(0)

        def more(j, st):
            m0, l0 = st
            m1, l1 = phase1(j, False)
            m = jnp.maximum(m0, m1)
            return m, l0 * jnp.exp2(m0 - m) + l1 * jnp.exp2(m1 - m)

        m, l = lax.fori_loop(0, y, more, stats)
        lse = m + jnp.log2(l)

        def phase2(j, acc):
            rows = pl.ds(mul(j, KC), KC)
            pb = jnp.exp2(s_buf[rows, :] - lse).astype(BF16)
            p_buf[rows, :] = pb
            return acc + tn(kv[rows, NOPE:], pb)

        ot = lax.fori_loop(0, y + 1, phase2, jnp.zeros((NOPE, CH), F32))
        delta = jnp.sum(ot * dot_[...].astype(F32), axis=0, keepdims=True)
        o_ref[s] = ot.T.astype(BF16)

        @pl.when(s > 1)
        def _():
            stage3(s - 2)

        def phase3(j, acc):
            rows = pl.ds(mul(j, KC), KC)
            k = kv[rows, :NOPE]
            v = kv[rows, NOPE:]
            pb = p_buf[rows, :]
            dp = nn(v, dot_[...])
            ds = (pb.astype(F32) * (dp - delta)).astype(BF16)
            dkr = nn(ds, qn[...]) * scale
            dv = nn(pb, do_ref[s])
            dkv = jnp.concatenate([dkr[:, :NOPE].astype(BF16), dv.astype(BF16)], axis=1)
            drr[rows, :] += dkr[:, NOPE:]
            dcr[rows, :] += nt(dkv, w_s)
            dw_ref[s] += nn(ct[j], dkv)
            out = (acc[0] + tn(k, ds), acc[1] + nn(rt[:, rows], ds))

            @pl.when(s == NS - 1)
            def _():
                for t in range(2):
                    for cp in d1_copies(2 * j + t):
                        cp.start()

            @pl.when(j == 0)
            def _():
                @pl.when(s > 0)
                def _():
                    stage2(s - 1)
            return out

        dqn, dqr = lax.fori_loop(0, y + 1, phase3, (jnp.zeros((NOPE, CH), F32), jnp.zeros((ROPE, CH), F32)))
        w_start(1, s)
        dq_ref[s, :NOPE] = (dqn * scale).astype(BF16)
        dq_ref[s, NOPE:] = (dqr * scale).astype(BF16)

        @pl.when(s > 1)
        def _():
            stage4(s - 2)

        @pl.when(s > 2)
        def _():
            stage5(s - 3)
        return 0

    lax.fori_loop(0, NS, step, 0)

    @pl.when(y == 0)
    def _():
        wait_latents((2, 3))

    outs = [pltpu.make_async_copy(o_ref.at[:, own_rows], o_out.at[mine], lsem.at[6]),
            pltpu.make_async_copy(dq_ref.at[:, :, own_rows], dq_out.at[mine], lsem.at[7]),
            rcopy(o_ref.at[:, oth_rows], o_out.at[mine], xs.at[2], xr.at[2], partner),
            rcopy(dq_ref.at[:, :, oth_rows], dq_out.at[mine], xs.at[3], xr.at[3], partner)]
    for cp in outs:
        cp.start()

    def join(j):
        for cp in d1_copies(j):
            cp.wait()
        rows = pl.ds(pl.multiple_of(j * CH + core * TOK, TOK), TOK)
        msg[j, :TOK] = dcr[rows, :] + rbd[j]
        drt = (drr[rows, :] + rbr[j]).T
        msg[j, TOK:] = jnp.concatenate([drt[:ROPE // 2], drt[ROPE // 2:]], axis=1)


    halves = (pl.ds(0, MSG // 2), pl.ds(MSG // 2, MSG // 2))

    def to_x(j):
        return [rcopy(msg.at[j, h], rbx.at[h], d2s.at[0, i], d2r.at[0, i], xn) for i, h in enumerate(halves)]

    def to_y(j):
        return [rcopy(msg.at[j, h], rby.at[h], d2s.at[1, i], d2r.at[1, i], yn) for i, h in enumerate(halves)]

    half_x = rcopy(msg.at[0, halves[0]], rbh, d2s.at[2, 0], d2r.at[2, 0], xn)
    half_y = rcopy(msg.at[0, halves[1]], rbh, d2s.at[2, 1], d2r.at[2, 0], yn)

    def on(k):
        return pl.when(chip == k)

    stage3(NS - 2)
    join(0)
    join(1)
    stage2(NS - 1)

    @on(3)
    def _():
        half_x.start()
        half_y.start()

    @on(2)
    def _():
        to_x(1)[0].start()
    stage5(NS - 3)
    stage4(NS - 2)
    stage3(NS - 1)

    @pl.when(y == 1)
    def _():
        join(2)

    @on(3)
    def _():
        to_x(2)[0].start()
        to_x(1)[0].wait_recv()
        msg[1, halves[0]] += rbx[halves[0]]
        to_y(1)[0].start()

    @on(2)
    def _():
        to_x(1)[1].start()
        to_y(0)[1].start()
        half_x.wait_recv()
        msg[0, halves[0]] += rbh[...]

    @on(1)
    def _():
        to_x(0)[0].start()
        half_y.wait_recv()
        msg[0, halves[1]] += rbh[...]
    stage4(NS - 1)

    @on(3)
    def _():
        to_x(2)[1].start()
        to_x(1)[1].wait_recv()
        msg[1, halves[1]] += rbx[halves[1]]
        to_y(1)[1].start()

    @on(2)
    def _():
        to_y(0)[0].start()

    @on(1)
    def _():
        to_x(0)[1].start()

    @pl.when(y == 1)
    def _():
        join(3)
    stage5(NS - 2)
    stage5(NS - 1)

    def all_of(copies, recv):
        for cp in copies:
            if recv:
                cp.wait_recv()
            else:
                cp.wait_send()

    @pl.when(chip != 3)
    def _():
        @pl.when(chip != 1)
        def _():
            all_of(to_x(0), True)
            msg[chip] += rbx[...]

        @pl.when(chip != 2)
        def _():
            all_of(to_y(0), True)
            msg[chip] += rby[...]

    dlat_out[...] = msg[chip, :TOK].astype(BF16)
    dr_out[:ROPE // 2] = msg[chip, TOK:, :TOK].astype(BF16)
    dr_out[ROPE // 2:] = msg[chip, TOK:, TOK:].astype(BF16)

    @pl.when(chip != 0)
    def _():
        all_of(to_x(0), False)

        @pl.when(chip != 1)
        def _():
            all_of(to_y(0), False)

    @pl.when(chip == 3)
    def _():
        all_of((half_x, half_y), False)
    for cp in outs:
        cp.wait()

    def drain(s, _):
        for cp in w_final(s, 0) + w_final(s, 1):
            cp.wait()
        w_local(s).wait()
        return 0
    lax.fori_loop(0, NS, drain, 0)


PARTS = 2


def layout_kernel(o_t, dw, dq_t, dc, dr, o_ref, dk_ref, dv_ref, dq_ref, dc_ref, dr_ref):
    def by_row(v):
        return jnp.swapaxes(v, 0, 1).reshape(v.shape[0] * v.shape[1], NOPE)

    dk_ref[...] = by_row(dw[:, :, :NOPE])
    dv_ref[...] = by_row(dw[:, :, NOPE:])
    o_ref[...] = by_row(o_t[...].astype(F32)).astype(BF16)
    dq_ref[...] = dq_t[...]
    dc_ref[...] = dc[...]
    dr_ref[...] = dr[...]


def to_output_layout(o_t, dw, dq_t, dc, dr):
    tok, lat = TOK // PARTS, LAT // PARTS
    passed = [pl.BlockSpec((HEADS // PARTS, QK, TOK), lambda i: (i, 0, 0)),
              pl.BlockSpec((tok, LAT), lambda i: (i, 0)),
              pl.BlockSpec((ROPE // PARTS, TOK), lambda i: (i, 0))]
    return pl.pallas_call(
        layout_kernel,
        grid=(PARTS,),
        out_shape=(jax.ShapeDtypeStruct((TOK * HEADS, NOPE), BF16),
                   jax.ShapeDtypeStruct((LAT * HEADS, NOPE), F32),
                   jax.ShapeDtypeStruct((LAT * HEADS, NOPE), F32),
                   jax.ShapeDtypeStruct(dq_t.shape, BF16),
                   jax.ShapeDtypeStruct(dc.shape, BF16),
                   jax.ShapeDtypeStruct(dr.shape, BF16)),
        in_specs=[pl.BlockSpec((HEADS, tok, NOPE), lambda i: (0, i, 0)),
                  pl.BlockSpec((HEADS, lat, 2 * NOPE), lambda i: (0, i, 0))] + passed,
        out_specs=[pl.BlockSpec((tok * HEADS, NOPE), lambda i: (i, 0)),
                   pl.BlockSpec((lat * HEADS, NOPE), lambda i: (i, 0)),
                   pl.BlockSpec((lat * HEADS, NOPE), lambda i: (i, 0))] + passed,
        compiler_params=pltpu.CompilerParams(vmem_limit_bytes=60 << 20),
    )(o_t, dw, dq_t, dc, dr)


def solution(mesh):
    seq_spec = P("cp")

    def local_step(queries, latent, key_rope, w_uk, w_uv, d_out):
        any_spec = pl.BlockSpec(memory_space=pl.ANY)
        vm_spec = pl.BlockSpec(memory_space=pltpu.VMEM)
        dma = pltpu.SemaphoreType.DMA
        vm = pltpu.VMEM
        o_t, dq_t, dw, d_latent, d_key_rope = pl.pallas_call(
            attn_kernel,
            out_shape=(jax.ShapeDtypeStruct((HEADS, TOK, NOPE), BF16),
                       jax.ShapeDtypeStruct((HEADS, QK, TOK), BF16),
                       jax.ShapeDtypeStruct((HEADS, LAT, 2 * NOPE), F32),
                       jax.ShapeDtypeStruct((TOK, LAT), BF16),
                       jax.ShapeDtypeStruct((ROPE, TOK), BF16)),
            in_specs=[any_spec] * 6,
            out_specs=[any_spec] * 3 + [vm_spec] * 2,
            scratch_shapes=[vm((TOK * HEADS, NOPE), BF16),
                            vm((LAT, HPC, NOPE), BF16), vm((LAT, HPC, NOPE), BF16),
                            vm((TOK * HEADS, NOPE), F32), vm((HPC, TOK, NOPE), BF16),
                            vm((HPC, QK, CH), BF16), vm((HPC, CH, NOPE), BF16),
                            vm((SEQ, LAT), BF16), vm((ROPE, SEQ), BF16), vm((SEQ, ROPE), BF16),
                            vm((HPC, LAT, NOPE), BF16), vm((HPC, LAT, NOPE), BF16),
                            vm((HPC, CH, NOPE), BF16), vm((HPC, QK, CH), BF16),
                            vm((NS, LAT, 2 * NOPE), F32), vm((NS, LAT, 2 * NOPE), F32),
                            vm((SEQ, LAT), F32), vm((SEQ, ROPE), F32), vm((NCHIP, MSG, LAT), F32),
                            vm((SEQ // KC, LAT, KC), BF16), vm((SEQ, 2 * NOPE), BF16),
                            vm((CH, QK), BF16), vm((NOPE, CH), BF16),
                            vm((SEQ, CH), F32), vm((SEQ, CH), BF16),
                            vm((2, 2, 256, NOPE), F32), vm((2, 2, 128, NOPE), F32),
                            vm((NCHIP, TOK, LAT), F32), vm((NCHIP, TOK, ROPE), F32),
                            vm((MSG, LAT), F32), vm((MSG, LAT), F32), vm((MSG // 2, LAT), F32),
                            dma((8,)), dma((4,)), dma((4,)), dma((2, 7)), dma((2, 7)),
                            dma((4, 2, 2)), dma((4, 2, 2)), dma((NS, 4)), dma((NS, 4)), dma((NS,)),
                            dma((2, NCHIP)), dma((2, NCHIP)), dma((3, 2)), dma((3, 2))],
            compiler_params=pltpu.CompilerParams(vmem_limit_bytes=63 << 20, collective_id=0, has_side_effects=True),
            cost_estimate=pl.CostEstimate(flops=30 * 10**9, bytes_accessed=20 << 20, transcendentals=10**7),
        )(jnp.transpose(queries, (1, 2, 0)), d_out.reshape(TOK * HEADS, NOPE), latent, key_rope.T, w_uk, w_uv)

        o, dk, dv, dq_t, d_latent, d_key_rope = to_output_layout(o_t, dw, dq_t, d_latent, d_key_rope)
        return (o.reshape(TOK, HEADS, NOPE), jnp.transpose(dq_t, (2, 0, 1)), d_latent, d_key_rope.T,
                dk.reshape(LAT, HEADS, NOPE), dv.reshape(LAT, HEADS, NOPE))

    return jax.shard_map(local_step, mesh=mesh,
                         in_specs=(seq_spec, seq_spec, seq_spec, P(), P(), seq_spec),
                         out_specs=(seq_spec, seq_spec, seq_spec, seq_spec, P(), P()),
                         check_vma=False)
```

```python
import math
import jax
import jax.numpy as jnp
from jax import lax
from jax.experimental import pallas as pl
from jax.experimental.pallas import tpu as pltpu
from jax.sharding import PartitionSpec as P

F32 = jnp.float32
BF16 = jnp.bfloat16
TOK = 256
CH = 512
KC = 1024
HEADS = 16
HPC = 8
NS = HPC
NOPE = 128
ROPE = 64
QK = NOPE + ROPE
LAT = 512
MSG = TOK + ROPE // 2
NCHIP = 4
SEQ = CH * NCHIP
MESH = pl.DeviceIdType.MESH
A_COLS = pl.ds(0, NOPE)
B_COLS = pl.ds(NOPE, NOPE)


def nt(a, b):
    return lax.dot_general(a, b, (((1,), (1,)), ((), ())), preferred_element_type=F32)


def nn(a, b):
    return lax.dot_general(a, b, (((1,), (0,)), ((), ())), preferred_element_type=F32)


def tn(a, b):
    return lax.dot_general(a, b, (((0,), (0,)), ((), ())), preferred_element_type=F32)


def mul(i, n):
    return pl.multiple_of(i * n, n)


def attn_kernel(q_in, do_in, c_in, r_in, wk_in, wv_in,
                o_out, dq_out, dw_out, dlat_out, dr_out,
                do_raw, wk_raw, wv_raw, stage, do_snd,
                qt, do_ref, c_ref, rt, rn, wk, wv, o_ref, dq_ref, dw_ref, dcr, drr, msg,
                ct, kv, qn, dot_, s_buf, p_buf, rb1, rb2, rbd, rbr, rbx, rby, rbh,
                lsem, xs, xr, cs, crs, ws, wr, fs, fr, d1s, d1r, d2s, d2r):
    scale = 1.0 / math.sqrt(QK)
    c2 = scale * math.log2(math.e)
    me = lax.axis_index("cp")
    core = lax.rem(me, 2)
    chip = lax.div(me, 2)
    x = lax.rem(chip, 2)
    y = lax.div(chip, 2)
    partner = me + 1 - 2 * core
    xn = me + 2 - 4 * x
    yn = me + 4 - 8 * y
    dn = xn + 4 - 8 * y

    def rcopy(src, dst, ss, rs, dev):
        return pltpu.make_async_remote_copy(src_ref=src, dst_ref=dst, send_sem=ss, recv_sem=rs,
                                            device_id=(dev,), device_id_type=MESH)

    my_rows = pl.ds(mul(me, TOK), TOK)
    own_rows = pl.ds(mul(core, TOK), TOK)
    oth_rows = pl.ds(mul(1 - core, TOK), TOK)
    mine = pl.ds(mul(core, HPC), HPC)

    other = pl.ds(mul(1 - core, HPC), HPC)

    local = [pltpu.make_async_copy(c_in, c_ref.at[my_rows], lsem.at[0]),
             pltpu.make_async_copy(r_in, rt.at[:, my_rows], lsem.at[1]),
             pltpu.make_async_copy(q_in.at[mine], qt.at[:, :, own_rows], lsem.at[2]),
             pltpu.make_async_copy(do_in, do_raw, lsem.at[3]),
             pltpu.make_async_copy(wk_in.at[:, mine], wk_raw, lsem.at[4]),
             pltpu.make_async_copy(wv_in.at[:, mine], wv_raw, lsem.at[5])]
    for cp in local:
        cp.start()

    bar = pltpu.get_barrier_semaphore()
    for peer in (partner, xn, yn, dn):
        pl.semaphore_signal(bar, inc=1, device_id=(peer,), device_id_type=MESH)
    pl.semaphore_wait(bar, 4)

    local[0].wait()
    local[1].wait()

    def latent_copies(i, src, dev):
        rows = pl.ds(mul(src, TOK), TOK)
        return (rcopy(c_ref.at[rows], c_ref.at[rows], cs.at[0, i], crs.at[0, i], dev),
                rcopy(rt.at[:, rows], rt.at[:, rows], cs.at[1, i], crs.at[1, i], dev))

    c_direct = [latent_copies(i, me, dev) for i, dev in enumerate((partner, xn, yn, dn))]
    for pair in c_direct:
        for cp in pair:
            cp.start()

    heads = [rcopy(q_in.at[other], qt.at[:, :, own_rows], xs.at[0], xr.at[0], partner),
             rcopy(do_snd, do_ref.at[:, own_rows], xs.at[1], xr.at[1], partner)]
    heads[0].start()
    local[3].wait()

    def pick(h, rows, stride):
        return stage[pl.ds(h, rows, stride=stride), :].astype(BF16)

    def widen(i, _):
        rows = pl.ds(mul(i, 256), 256)
        stage[rows, :] = do_raw[rows, :].astype(F32)
        return 0
    lax.fori_loop(0, TOK * HEADS // 256, widen, 0)
    is0 = core == 0
    for i in range(HPC):
        lo = pick(i, TOK, HEADS)
        hi = pick(i + HPC, TOK, HEADS)
        do_ref[i, own_rows, :] = jnp.where(is0, lo, hi)
        do_snd[i] = jnp.where(is0, hi, lo)
    heads[1].start()
    for t, (raw, out) in enumerate(((wk_raw, wk), (wv_raw, wv))):
        local[4 + t].wait()

        def body(i, _, raw=raw):
            ls = pl.ds(mul(i, 32), 32)
            stage[pl.ds(mul(i, 256), 256), :] = raw[ls].astype(F32).reshape(256, NOPE)
            return 0
        lax.fori_loop(0, LAT // 32, body, 0)
        for i in range(HPC):
            out[i] = pick(i, LAT, HPC)

    def zero_dc(j, _):
        rows = pl.ds(mul(j, KC), KC)
        dcr[rows, :] = jnp.zeros((KC, LAT), F32)
        drr[rows, :] = jnp.zeros((KC, ROPE), F32)
        return 0
    lax.fori_loop(0, y + 1, zero_dc, 0)
    local[2].wait()
    for cp in heads:
        cp.wait()
    for cp in c_direct[0]:
        cp.wait()

    def turn(j):
        rows = pl.ds(mul(j, KC), KC)
        ct[j] = c_ref[rows, :].T
        rn[rows, :] = rt[:, rows].T

    c_fwd = [None] + [latent_copies(3 + i, src, partner) for i, src in ((1, xn), (2, yn), (3, dn))]

    def wait_latents(which):
        for i in which:
            for cp in c_direct[i]:
                cp.wait()
            for cp in c_fwd[i]:
                cp.start()
        for i in which:
            for cp in c_fwd[i]:
                cp.wait()

    wait_latents((1,))
    turn(y)

    hx = pl.ds(mul(x, 256), 256)
    hx1 = pl.ds(mul(1 - x, 256), 256)
    hy = pl.ds(mul(y, 256), 256)
    hy1 = pl.ds(mul(1 - y, 256), 256)
    qa = pl.ds(pl.multiple_of(x * 256 + y * 128, 128), 128)
    qa1 = pl.ds(pl.multiple_of(x * 256 + (1 - y) * 128, 128), 128)
    qb = pl.ds(pl.multiple_of(y * 256 + x * 128, 128), 128)
    qb1 = pl.ds(pl.multiple_of(y * 256 + (1 - x) * 128, 128), 128)

    def w_copy(phase, s):
        par = lax.rem(s, 2)
        t = core * NS + s
        if phase == 1:
            pair = ((dw_ref.at[s, hx1, A_COLS], rb1.at[par, 0], xn), (dw_ref.at[s, hy1, B_COLS], rb1.at[par, 1], yn))
        elif phase == 2:
            pair = ((dw_ref.at[s, qa1, A_COLS], rb2.at[par, 0], yn), (dw_ref.at[s, qb1, B_COLS], rb2.at[par, 1], xn))
        elif phase == 3:
            pair = ((dw_out.at[t, qa, A_COLS], dw_out.at[t, qa, A_COLS], yn),
                    (dw_out.at[t, qb, B_COLS], dw_out.at[t, qb, B_COLS], xn))
        else:
            pair = ((dw_out.at[t, hx, A_COLS], dw_out.at[t, hx, A_COLS], xn),
                    (dw_out.at[t, hy, B_COLS], dw_out.at[t, hy, B_COLS], yn))
        return [rcopy(a, b, ws.at[phase - 1, par, i], wr.at[phase - 1, par, i], d)
                for i, (a, b, d) in enumerate(pair)]

    def w_start(phase, s):
        for cp in w_copy(phase, s):
            cp.start()

    def w_wait(phase, s):
        for cp in w_copy(phase, s):
            cp.wait()

    def w_final(s, late):
        t = core * NS + s
        parts = ((hx1, A_COLS), (hy1, B_COLS)) if late else ((hx, A_COLS), (hy, B_COLS))
        return [rcopy(dw_out.at[t, r, c], dw_out.at[t, r, c], fs.at[s, 2 * late + i], fr.at[s, 2 * late + i], partner)
                for i, (r, c) in enumerate(parts)]

    def stage2(s):
        par = lax.rem(s, 2)
        w_wait(1, s)
        dw_ref[s, hx, A_COLS] += rb1[par, 0]
        dw_ref[s, hy, B_COLS] += rb1[par, 1]
        w_start(2, s)

    def stage3(s):
        par = lax.rem(s, 2)
        w_wait(2, s)
        t = core * NS + s
        dw_out[t, qa, A_COLS] = dw_ref[s, qa, A_COLS] + rb2[par, 0]
        dw_out[t, qb, B_COLS] = dw_ref[s, qb, B_COLS] + rb2[par, 1]
        w_start(3, s)

    def stage4(s):
        w_wait(3, s)
        w_start(4, s)
        for cp in w_final(s, 0):
            cp.start()

    def stage5(s):
        w_wait(4, s)
        for cp in w_final(s, 1):
            cp.start()

    def d1_copies(j):
        rows = pl.ds(pl.multiple_of(j * CH + (1 - core) * TOK, TOK), TOK)
        return (rcopy(dcr.at[rows], rbd.at[j], d1s.at[0, j], d1r.at[0, j], partner),
                rcopy(drr.at[rows], rbr.at[j], d1s.at[1, j], d1r.at[1, j], partner))

    def step(s, _):
        dw_ref[s] = jnp.zeros((LAT, 2 * NOPE), F32)
        qn[...] = qt[s].T
        dot_[...] = do_ref[s].T
        w_s = jnp.concatenate([wk[s], wv[s]], axis=1)

        def phase1(j, masked):
            rows = pl.ds(mul(j, KC), KC)
            kvv = nn(c_ref[rows, :], w_s).astype(BF16)
            kv[rows, :] = kvv
            k_cat = jnp.concatenate([kvv[:, :NOPE], rn[rows, :]], axis=1)
            s2 = nn(k_cat, qt[s]) * c2
            if masked:
                ki = lax.broadcasted_iota(jnp.int32, (KC, CH), 0)
                qi = lax.broadcasted_iota(jnp.int32, (KC, CH), 1)
                s2 = jnp.where(ki - qi <= x * CH, s2, -1e30)
            s_buf[rows, :] = s2
            m = jnp.max(s2, axis=0, keepdims=True)
            return m, jnp.sum(jnp.exp2(s2 - m), axis=0, keepdims=True)

        stats = phase1(y, True)

        @pl.when(s == 0)
        def _():
            @pl.when(y == 1)
            def _():
                wait_latents((2, 3))
                turn(0)

        def more(j, st):
            m0, l0 = st
            m1, l1 = phase1(j, False)
            m = jnp.maximum(m0, m1)
            return m, l0 * jnp.exp2(m0 - m) + l1 * jnp.exp2(m1 - m)

        m, l = lax.fori_loop(0, y, more, stats)
        lse = m + jnp.log2(l)

        def phase2(j, acc):
            rows = pl.ds(mul(j, KC), KC)
            pb = jnp.exp2(s_buf[rows, :] - lse).astype(BF16)
            p_buf[rows, :] = pb
            return acc + tn(kv[rows, NOPE:], pb)

        ot = lax.fori_loop(0, y + 1, phase2, jnp.zeros((NOPE, CH), F32))
        delta = jnp.sum(ot * dot_[...].astype(F32), axis=0, keepdims=True)
        o_ref[s] = ot.T.astype(BF16)

        @pl.when(s > 1)
        def _():
            stage3(s - 2)

        def phase3(j, acc):
            rows = pl.ds(mul(j, KC), KC)
            k = kv[rows, :NOPE]
            v = kv[rows, NOPE:]
            pb = p_buf[rows, :]
            dp = nn(v, dot_[...])
            ds = (pb.astype(F32) * (dp - delta)).astype(BF16)
            dkr = nn(ds, qn[...]) * scale
            dv = nn(pb, do_ref[s])
            dkv = jnp.concatenate([dkr[:, :NOPE].astype(BF16), dv.astype(BF16)], axis=1)
            drr[rows, :] += dkr[:, NOPE:]
            dcr[rows, :] += nt(dkv, w_s)
            dw_ref[s] += nn(ct[j], dkv)
            out = (acc[0] + tn(k, ds), acc[1] + nn(rt[:, rows], ds))

            @pl.when(s == NS - 1)
            def _():
                for t in range(2):
                    for cp in d1_copies(2 * j + t):
                        cp.start()

            @pl.when(j == 0)
            def _():
                @pl.when(s > 0)
                def _():
                    stage2(s - 1)
            return out

        dqn, dqr = lax.fori_loop(0, y + 1, phase3, (jnp.zeros((NOPE, CH), F32), jnp.zeros((ROPE, CH), F32)))
        w_start(1, s)
        dq_ref[s, :NOPE] = (dqn * scale).astype(BF16)
        dq_ref[s, NOPE:] = (dqr * scale).astype(BF16)

        @pl.when(s > 1)
        def _():
            stage4(s - 2)

        @pl.when(s > 2)
        def _():
            stage5(s - 3)
        return 0

    lax.fori_loop(0, NS, step, 0)

    @pl.when(y == 0)
    def _():
        wait_latents((2, 3))

    outs = [rcopy(o_ref.at[:, oth_rows], o_out.at[mine], xs.at[2], xr.at[2], partner),
            rcopy(dq_ref.at[:, :, oth_rows], dq_out.at[mine], xs.at[3], xr.at[3], partner)]
    for cp in outs:
        cp.start()

    def join(j):
        for cp in d1_copies(j):
            cp.wait()
        rows = pl.ds(pl.multiple_of(j * CH + core * TOK, TOK), TOK)
        msg[j, :TOK] = dcr[rows, :] + rbd[j]
        drt = (drr[rows, :] + rbr[j]).T
        msg[j, TOK:] = jnp.concatenate([drt[:ROPE // 2], drt[ROPE // 2:]], axis=1)


    halves = (pl.ds(0, MSG // 2), pl.ds(MSG // 2, MSG // 2))

    def to_x(j):
        return [rcopy(msg.at[j, h], rbx.at[h], d2s.at[0, i], d2r.at[0, i], xn) for i, h in enumerate(halves)]

    def to_y(j):
        return [rcopy(msg.at[j, h], rby.at[h], d2s.at[1, i], d2r.at[1, i], yn) for i, h in enumerate(halves)]

    half_x = rcopy(msg.at[0, halves[0]], rbh, d2s.at[2, 0], d2r.at[2, 0], xn)
    half_y = rcopy(msg.at[0, halves[1]], rbh, d2s.at[2, 1], d2r.at[2, 0], yn)

    def on(k):
        return pl.when(chip == k)

    stage3(NS - 2)
    join(0)
    join(1)
    stage2(NS - 1)

    @on(3)
    def _():
        half_x.start()
        half_y.start()

    @on(2)
    def _():
        to_x(1)[0].start()
    stage5(NS - 3)
    stage4(NS - 2)
    stage3(NS - 1)

    @pl.when(y == 1)
    def _():
        join(2)

    @on(3)
    def _():
        to_x(2)[0].start()
        to_x(1)[0].wait_recv()
        msg[1, halves[0]] += rbx[halves[0]]
        to_y(1)[0].start()

    @on(2)
    def _():
        to_x(1)[1].start()
        to_y(0)[1].start()
        half_x.wait_recv()
        msg[0, halves[0]] += rbh[...]

    @on(1)
    def _():
        to_x(0)[0].start()
        half_y.wait_recv()
        msg[0, halves[1]] += rbh[...]
    stage4(NS - 1)

    @on(3)
    def _():
        to_x(2)[1].start()
        to_x(1)[1].wait_recv()
        msg[1, halves[1]] += rbx[halves[1]]
        to_y(1)[1].start()

    @on(2)
    def _():
        to_y(0)[0].start()

    @on(1)
    def _():
        to_x(0)[1].start()

    @pl.when(y == 1)
    def _():
        join(3)

    def keep(h, _):
        o_out[core * HPC + h] = o_ref[h, own_rows, :]
        dq_out[core * HPC + h] = dq_ref[h, :, own_rows]
        return 0
    lax.fori_loop(0, HPC, keep, 0)
    stage5(NS - 2)
    stage5(NS - 1)

    def all_of(copies, recv):
        for cp in copies:
            if recv:
                cp.wait_recv()
            else:
                cp.wait_send()

    @pl.when(chip != 3)
    def _():
        @pl.when(chip != 1)
        def _():
            all_of(to_x(0), True)
            msg[chip] += rbx[...]

        @pl.when(chip != 2)
        def _():
            all_of(to_y(0), True)
            msg[chip] += rby[...]

    dlat_out[...] = msg[chip, :TOK].astype(BF16)
    dr_out[:ROPE // 2] = msg[chip, TOK:, :TOK].astype(BF16)
    dr_out[ROPE // 2:] = msg[chip, TOK:, TOK:].astype(BF16)

    @pl.when(chip != 0)
    def _():
        all_of(to_x(0), False)

        @pl.when(chip != 1)
        def _():
            all_of(to_y(0), False)

    @pl.when(chip == 3)
    def _():
        all_of((half_x, half_y), False)
    for cp in outs:
        cp.wait()

    def drain(s, _):
        for cp in w_final(s, 0) + w_final(s, 1):
            cp.wait()
        return 0
    lax.fori_loop(0, NS, drain, 0)


PARTS = 8


def layout_kernel(dw, o_t, dq_t, dc, dr, o_out, dk_out, dv_out, dq_out, dc_out, dr_out,
                  o_stage, stage, osem, ssem):
    lat = LAT // PARTS
    stores = [pltpu.make_async_copy(a, b, osem.at[i])
              for i, (a, b) in enumerate(((o_stage, o_out), (dq_t, dq_out), (dc, dc_out), (dr, dr_out)))]

    def by_row(v):
        return jnp.swapaxes(v, 0, 1).reshape(v.shape[0] * v.shape[1], NOPE)

    def put(i):
        rows = pl.ds(i * lat * HEADS, lat * HEADS)
        return [pltpu.make_async_copy(stage.at[i % 2, a], out.at[rows], ssem.at[i % 2, a])
                for a, out in enumerate((dk_out, dv_out))]

    for i in range(PARTS):
        for a in range(2):
            if i > 1:
                put(i - 2)[a].wait()
            stage[i % 2, a] = by_row(dw[:, i * lat:(i + 1) * lat, a * NOPE:(a + 1) * NOPE])
            put(i)[a].start()
        if i == 0:
            for cp in stores[1:]:
                cp.start()
            o_stage[...] = by_row(o_t[...].astype(F32)).astype(BF16)
            stores[0].start()
    for i in (PARTS - 2, PARTS - 1):
        for cp in put(i):
            cp.wait()
    for cp in stores:
        cp.wait()


def to_output_layout(dw, o_t, dq_t, dc, dr):
    any_spec = pl.BlockSpec(memory_space=pl.ANY)
    dma = pltpu.SemaphoreType.DMA
    rows = LAT // PARTS * HEADS
    return pl.pallas_call(
        layout_kernel,
        out_shape=(jax.ShapeDtypeStruct((TOK * HEADS, NOPE), BF16),
                   jax.ShapeDtypeStruct((LAT * HEADS, NOPE), F32),
                   jax.ShapeDtypeStruct((LAT * HEADS, NOPE), F32),
                   jax.ShapeDtypeStruct(dq_t.shape, BF16),
                   jax.ShapeDtypeStruct(dc.shape, BF16),
                   jax.ShapeDtypeStruct(dr.shape, BF16)),
        in_specs=[pl.BlockSpec(memory_space=pltpu.VMEM)] * 5,
        out_specs=[any_spec] * 6,
        scratch_shapes=[pltpu.VMEM((TOK * HEADS, NOPE), BF16),
                        pltpu.VMEM((2, 2, rows, NOPE), F32),
                        dma((4,)), dma((2, 2))],
        compiler_params=pltpu.CompilerParams(vmem_limit_bytes=32 << 20),
    )(dw, o_t, dq_t, dc, dr)


def solution(mesh):
    seq_spec = P("cp")

    def local_step(queries, latent, key_rope, w_uk, w_uv, d_out):
        any_spec = pl.BlockSpec(memory_space=pl.ANY)
        vm_spec = pl.BlockSpec(memory_space=pltpu.VMEM)
        dma = pltpu.SemaphoreType.DMA
        vm = pltpu.VMEM
        o_t, dq_t, dw, d_latent, d_key_rope = pl.pallas_call(
            attn_kernel,
            out_shape=(vm((HEADS, TOK, NOPE), BF16), vm((HEADS, QK, TOK), BF16), vm((HEADS, LAT, 2 * NOPE), F32),
                       vm((TOK, LAT), BF16), vm((ROPE, TOK), BF16)),
            in_specs=[any_spec] * 6,
            out_specs=[vm_spec] * 5,
            scratch_shapes=[vm((TOK * HEADS, NOPE), BF16),
                            vm((LAT, HPC, NOPE), BF16), vm((LAT, HPC, NOPE), BF16),
                            vm((TOK * HEADS, NOPE), F32), vm((HPC, TOK, NOPE), BF16),
                            vm((HPC, QK, CH), BF16), vm((HPC, CH, NOPE), BF16),
                            vm((SEQ, LAT), BF16), vm((ROPE, SEQ), BF16), vm((SEQ, ROPE), BF16),
                            vm((HPC, LAT, NOPE), BF16), vm((HPC, LAT, NOPE), BF16),
                            vm((HPC, CH, NOPE), BF16), vm((HPC, QK, CH), BF16),
                            vm((NS, LAT, 2 * NOPE), F32),
                            vm((SEQ, LAT), F32), vm((SEQ, ROPE), F32), vm((NCHIP, MSG, LAT), F32),
                            vm((SEQ // KC, LAT, KC), BF16), vm((SEQ, 2 * NOPE), BF16),
                            vm((CH, QK), BF16), vm((NOPE, CH), BF16),
                            vm((SEQ, CH), F32), vm((SEQ, CH), BF16),
                            vm((2, 2, 256, NOPE), F32), vm((2, 2, 128, NOPE), F32),
                            vm((NCHIP, TOK, LAT), F32), vm((NCHIP, TOK, ROPE), F32),
                            vm((MSG, LAT), F32), vm((MSG, LAT), F32), vm((MSG // 2, LAT), F32),
                            dma((6,)), dma((4,)), dma((4,)), dma((2, 7)), dma((2, 7)),
                            dma((4, 2, 2)), dma((4, 2, 2)), dma((NS, 4)), dma((NS, 4)),
                            dma((2, NCHIP)), dma((2, NCHIP)), dma((3, 2)), dma((3, 2))],
            compiler_params=pltpu.CompilerParams(vmem_limit_bytes=50 << 20, collective_id=0, has_side_effects=True),
            cost_estimate=pl.CostEstimate(flops=30 * 10**9, bytes_accessed=20 << 20, transcendentals=10**7),
        )(jnp.transpose(queries, (1, 2, 0)), d_out.reshape(TOK * HEADS, NOPE), latent, key_rope.T, w_uk, w_uv)

        o, dk, dv, dq_t, d_latent, d_key_rope = to_output_layout(dw, o_t, dq_t, d_latent, d_key_rope)
        return (o.reshape(TOK, HEADS, NOPE), jnp.transpose(dq_t, (2, 0, 1)), d_latent, d_key_rope.T,
                dk.reshape(LAT, HEADS, NOPE), dv.reshape(LAT, HEADS, NOPE))

    return jax.shard_map(local_step, mesh=mesh,
                         in_specs=(seq_spec, seq_spec, seq_spec, P(), P(), seq_spec),
                         out_specs=(seq_spec, seq_spec, seq_spec, seq_spec, P(), P()),
                         check_vma=False)
```

```python
import functools
import math
import jax
import jax.numpy as jnp
from jax import lax
from jax.experimental import pallas as pl
from jax.experimental.pallas import tpu as pltpu
from jax.sharding import PartitionSpec as P

F32 = jnp.float32
BF16 = jnp.bfloat16
TOK = 256
CH = 512
KC = 1024
HALF = TOK // 2
SUB = 256
HEADS = 16
HPC = 8
NS = HPC
NOPE = 128
ROPE = 64
QK = NOPE + ROPE
LAT = 512
MSG = TOK + ROPE // 2
NCHIP = 4
SEQ = CH * NCHIP
MESH = pl.DeviceIdType.MESH


def nt(a, b):
    return lax.dot_general(a, b, (((1,), (1,)), ((), ())), preferred_element_type=F32)


def nn(a, b):
    return lax.dot_general(a, b, (((1,), (0,)), ((), ())), preferred_element_type=F32)


def tn(a, b):
    return lax.dot_general(a, b, (((0,), (0,)), ((), ())), preferred_element_type=F32)


def mul(i, n):
    return pl.multiple_of(i * n, n)


def attn_kernel(q_in, do_in, c_in, r_in, wk_in, wv_in,
                o_out, dq_out, dw_out, dlat_out, dr_out,
                do_raw, wk_raw, wv_raw, stage, do_snd,
                qt, do_ref, c_ref, rt, rn, wk, wv, o_ref, dq_ref, dw_ref, dcr, drr, msg,
                ct, kv, qn, dot_, s_buf, m_buf, p_buf, rb1, rb2, rbd, rbr, rbx, rby, rbh,
                lsem, xs, xr, cs, crs, ws, wr, ps, fs, fr, d1s, d1r, d2s, d2r):
    scale = 1.0 / math.sqrt(QK)
    c2 = scale * math.log2(math.e)
    me = lax.axis_index("cp")
    core = lax.rem(me, 2)
    chip = lax.div(me, 2)
    x = lax.rem(chip, 2)
    y = lax.div(chip, 2)
    partner = me + 1 - 2 * core
    xn = me + 2 - 4 * x
    yn = me + 4 - 8 * y
    dn = xn + 4 - 8 * y

    def rcopy(src, dst, ss, rs, dev):
        return pltpu.make_async_remote_copy(src_ref=src, dst_ref=dst, send_sem=ss, recv_sem=rs,
                                            device_id=(dev,), device_id_type=MESH)

    my_rows = pl.ds(mul(me, TOK), TOK)
    own_rows = pl.ds(mul(core, TOK), TOK)
    oth_rows = pl.ds(mul(1 - core, TOK), TOK)
    mine = pl.ds(mul(core, HPC), HPC)

    other = pl.ds(mul(1 - core, HPC), HPC)

    local = [pltpu.make_async_copy(c_in, c_ref.at[my_rows], lsem.at[0]),
             pltpu.make_async_copy(r_in, rt.at[:, my_rows], lsem.at[1]),
             pltpu.make_async_copy(q_in.at[mine], qt.at[:, :, own_rows], lsem.at[2]),
             pltpu.make_async_copy(do_in, do_raw, lsem.at[3]),
             pltpu.make_async_copy(wk_in.at[:, mine], wk_raw, lsem.at[4]),
             pltpu.make_async_copy(wv_in.at[:, mine], wv_raw, lsem.at[5])]
    for cp in local:
        cp.start()

    bar = pltpu.get_barrier_semaphore()
    for peer in (partner, xn, yn, dn):
        pl.semaphore_signal(bar, inc=1, device_id=(peer,), device_id_type=MESH)
    pl.semaphore_wait(bar, 4)

    local[0].wait()
    local[1].wait()

    def latent_copies(i, src, dev, recv=None):
        recv = i if recv is None else recv
        rows = pl.ds(mul(src, TOK), TOK)
        parts = [c_ref.at[pl.ds(pl.multiple_of(src * TOK + t * HALF, HALF), HALF)] for t in range(2)]
        parts.append(rt.at[:, rows])
        return [rcopy(ref, ref, cs.at[t, i], crs.at[t, recv], dev) for t, ref in enumerate(parts)]

    low = y == 0
    is0 = core == 0
    c_direct = [latent_copies(i, me, dev) for i, dev in enumerate((partner, xn, yn, dn))]
    c_relay = latent_copies(7, yn, xn, 3)
    for cp in c_direct[0] + c_direct[1]:
        cp.start()

    @pl.when(low)
    def _():
        for cp in c_direct[2]:
            cp.start()

        @pl.when(is0)
        def _():
            for cp in c_direct[3]:
                cp.start()

    heads = [rcopy(q_in.at[other], qt.at[:, :, own_rows], xs.at[0], xr.at[0], partner),
             rcopy(do_snd, do_ref.at[:, own_rows], xs.at[1], xr.at[1], partner)]
    heads[0].start()
    local[3].wait()

    def pick(h, rows, stride):
        return stage[pl.ds(h, rows, stride=stride), :].astype(BF16)

    def widen(i, _):
        rows = pl.ds(mul(i, 256), 256)
        stage[rows, :] = do_raw[rows, :].astype(F32)
        return 0
    lax.fori_loop(0, TOK * HEADS // 256, widen, 0)
    for i in range(HPC):
        lo = pick(i, TOK, HEADS)
        hi = pick(i + HPC, TOK, HEADS)
        do_ref[i, own_rows, :] = jnp.where(is0, lo, hi)
        do_snd[i] = jnp.where(is0, hi, lo)
    heads[1].start()
    for t, (raw, out) in enumerate(((wk_raw, wk), (wv_raw, wv))):
        local[4 + t].wait()

        def body(i, _, raw=raw):
            ls = pl.ds(mul(i, 32), 32)
            stage[pl.ds(mul(i, 256), 256), :] = raw[ls].astype(F32).reshape(256, NOPE)
            return 0
        lax.fori_loop(0, LAT // 32, body, 0)
        for i in range(HPC):
            out[i] = pick(i, LAT, HPC)

    def zero_dc(j, _):
        rows = pl.ds(mul(j, KC), KC)
        dcr[rows, :] = jnp.zeros((KC, LAT), F32)
        drr[rows, :] = jnp.zeros((KC, ROPE), F32)
        return 0
    lax.fori_loop(0, y + 1, zero_dc, 0)
    local[2].wait()
    for cp in heads:
        cp.wait()
    for cp in c_direct[0]:
        cp.wait()

    def turn(j):
        rows = pl.ds(mul(j, KC), KC)
        ct[j] = c_ref[rows, :].T
        rn[rows, :] = rt[:, rows].T

    c_fwd = [None] + [latent_copies(3 + i, src, partner) for i, src in ((1, xn), (2, yn), (3, dn))]

    high = y == 1
    for t in (0, 1, 2):
        c_direct[1][t].wait()
        c_fwd[1][t].start()

        @pl.when(high)
        def _(t=t):
            c_direct[2][t].wait_recv()

            @pl.when(core == 1)
            def _():
                c_relay[t].start()
            c_fwd[2][t].start()
    for cp in c_fwd[1]:
        cp.wait()
    turn(y)

    def wait_latents():
        for t in (0, 1, 2):
            c_direct[3][t].wait_recv()
            c_fwd[3][t].start()
        for cp in c_fwd[2] + c_fwd[3]:
            cp.wait()

        @pl.when(core == 1)
        def _():
            for cp in c_relay:
                cp.wait_send()

    hx = pl.ds(mul(x, 256), 256)
    hx1 = pl.ds(mul(1 - x, 256), 256)
    hy = pl.ds(mul(y, 256), 256)
    hy1 = pl.ds(mul(1 - y, 256), 256)
    qa = pl.ds(pl.multiple_of(x * 256 + y * 128, 128), 128)
    qa1 = pl.ds(pl.multiple_of(x * 256 + (1 - y) * 128, 128), 128)
    qb = pl.ds(pl.multiple_of(y * 256 + x * 128, 128), 128)
    qb1 = pl.ds(pl.multiple_of(y * 256 + (1 - x) * 128, 128), 128)

    def w_copy(phase, s):
        par = lax.rem(s, 2)
        t = core * NS + s
        if phase == 1:
            pair = ((dw_ref.at[s, 0, hx1], rb1.at[par, 0], xn), (dw_ref.at[s, 1, hy1], rb1.at[par, 1], yn))
        elif phase == 2:
            pair = ((dw_ref.at[s, 0, qa1], rb2.at[par, 0], yn), (dw_ref.at[s, 1, qb1], rb2.at[par, 1], xn))
        elif phase == 3:
            pair = ((dw_out.at[t, 0, qa], dw_out.at[t, 0, qa], yn),
                    (dw_out.at[t, 1, qb], dw_out.at[t, 1, qb], xn))
        else:
            pair = ((dw_out.at[t, 0, hx], dw_out.at[t, 0, hx], xn),
                    (dw_out.at[t, 1, hy], dw_out.at[t, 1, hy], yn))
        return [rcopy(a, b, ws.at[phase - 1, par, i], wr.at[phase - 1, par, i], d)
                for i, (a, b, d) in enumerate(pair)]

    def w_start(phase, s):
        for cp in w_copy(phase, s):
            cp.start()

    def w_wait(phase, s):
        for cp in w_copy(phase, s):
            cp.wait()

    def w_final(s, late):
        t = core * NS + s
        par = lax.rem(s, 2)
        parts = (hx1, hy1) if late else (hx, hy)
        return [rcopy(dw_out.at[t, i, r], dw_out.at[t, i, r], fs.at[par, 2 * late + i], fr.at[par, 2 * late + i],
                      partner) for i, r in enumerate(parts)]

    def hand_over(s, late):
        def wait_last():
            for cp in w_final(s - 1, late):
                cp.wait()
        if isinstance(s, int):
            wait_last()
        else:
            pl.when(s > 0)(wait_last)
        for cp in w_final(s, late):
            cp.start()

    def stage2(s):
        par = lax.rem(s, 2)
        w_wait(1, s)
        dw_ref[s, 0, hx] += rb1[par, 0]
        dw_ref[s, 1, hy] += rb1[par, 1]
        w_start(2, s)

    def stage3(s):
        par = lax.rem(s, 2)
        w_wait(2, s)
        t = core * NS + s
        dw_out[t, 0, qa] = dw_ref[s, 0, qa] + rb2[par, 0]
        dw_out[t, 1, qb] = dw_ref[s, 1, qb] + rb2[par, 1]
        w_start(3, s)

    def stage4(s):
        w_wait(3, s)
        w_start(4, s)
        hand_over(s, 0)

    def stage5(s):
        w_wait(4, s)
        hand_over(s, 1)

    def last4(s):
        w_wait(3, s)
        to_a, to_b = w_copy(4, s)

        @pl.when(low)
        def _():
            to_a.start()

        @pl.when(chip != 3)
        def _():
            to_b.start()
        hand_over(s, 0)

    def w_pass(s):
        par = lax.rem(s, 2)
        t = core * NS + s
        pair = ((dw_out.at[t, 0, hx1], yn), (dw_out.at[t, 1, hy1], xn))
        return [rcopy(ref, ref, ps.at[par, i], wr.at[3, par, i], dev) for i, (ref, dev) in enumerate(pair)]

    def last5a(s):
        w_copy(4, s)[0].wait_recv()

        @pl.when(low)
        def _():
            w_pass(s)[0].start()

    def last5b(s):
        w_copy(4, s)[1].wait_recv()

        @pl.when(chip == 0)
        def _():
            w_pass(s)[1].start()
        hand_over(s, 1)

    def last_sent(s):
        @pl.when(low)
        def _():
            w_copy(4, s)[0].wait_send()
            w_pass(s)[0].wait_send()

        @pl.when(chip != 3)
        def _():
            w_copy(4, s)[1].wait_send()

        @pl.when(chip == 0)
        def _():
            w_pass(s)[1].wait_send()

    def d1_copies(j):
        rows = pl.ds(pl.multiple_of(j * CH + (1 - core) * TOK, TOK), TOK)
        return (rcopy(dcr.at[rows], rbd.at[j], d1s.at[0, j], d1r.at[0, j], partner),
                rcopy(drr.at[rows], rbr.at[j], d1s.at[1, j], d1r.at[1, j], partner))

    def step(s, _):
        dw_ref[s] = jnp.zeros((2, LAT, NOPE), F32)
        qn[...] = qt[s].T
        dot_[...] = do_ref[s].T
        w_s = jnp.concatenate([wk[s], wv[s]], axis=1)

        def phase1(j, masked):
            ms, ls = [], []
            for t in range(KC // SUB):
                rows = pl.ds(pl.multiple_of(j * KC + t * SUB, SUB), SUB)
                kvv = nn(c_ref[rows, :], w_s).astype(BF16)
                kv[rows, :] = kvv
                k_cat = jnp.concatenate([kvv[:, :NOPE], rn[rows, :]], axis=1)
                s2 = nn(k_cat, qt[s]) * c2
                if masked:
                    ki = lax.broadcasted_iota(jnp.int32, (SUB, CH), 0)
                    qi = lax.broadcasted_iota(jnp.int32, (SUB, CH), 1)
                    s2 = jnp.where(ki - qi <= x * CH - t * SUB, s2, -1e30 * math.log2(math.e))
                m = jnp.max(s2, axis=0, keepdims=True)
                e = jnp.exp2(s2 - m)
                s_buf[rows, :] = e
                m_buf[j * (KC // SUB) + t] = m
                ms.append(m)
                ls.append(jnp.sum(e, axis=0, keepdims=True))
            top = functools.reduce(jnp.maximum, ms)
            return top, sum(l * jnp.exp2(m - top) for m, l in zip(ms, ls))

        stats = phase1(y, True)

        @pl.when(s > 1)
        def _():
            stage3(s - 2)

        @pl.when(s == 0)
        def _():
            @pl.when(high)
            def _():
                wait_latents()
                turn(0)

        def more(j, st):
            m0, l0 = st
            m1, l1 = phase1(j, False)
            m = jnp.maximum(m0, m1)
            return m, l0 * jnp.exp2(m0 - m) + l1 * jnp.exp2(m1 - m)

        m, l = lax.fori_loop(0, y, more, stats)
        lse = m + jnp.log2(l)

        def phase2(j, acc):
            rows = pl.ds(mul(j, KC), KC)
            parts = []
            for t in range(KC // SUB):
                sub = pl.ds(pl.multiple_of(j * KC + t * SUB, SUB), SUB)
                fac = jnp.exp2(m_buf[j * (KC // SUB) + t] - lse)
                parts.append((s_buf[sub, :] * fac).astype(BF16))
                p_buf[sub, :] = parts[-1]
            return acc + tn(kv[rows, NOPE:], jnp.concatenate(parts, axis=0))

        ot = lax.fori_loop(0, y + 1, phase2, jnp.zeros((NOPE, CH), F32))
        delta = jnp.sum(ot * dot_[...].astype(F32), axis=0, keepdims=True)
        o_ref[s] = ot.T.astype(BF16)

        def phase3(j, acc):
            rows = pl.ds(mul(j, KC), KC)
            k = kv[rows, :NOPE]
            v = kv[rows, NOPE:]
            pb = p_buf[rows, :]
            dp = nn(v, dot_[...])
            ds = (pb.astype(F32) * (dp - delta)).astype(BF16)
            dkr = nn(ds, qn[...]) * scale
            dv = nn(pb, do_ref[s])
            dkv = jnp.concatenate([dkr[:, :NOPE].astype(BF16), dv.astype(BF16)], axis=1)
            drr[rows, :] += dkr[:, NOPE:]
            dcr[rows, :] += nt(dkv, w_s)
            dw = nn(ct[j], dkv)
            dw_ref[s, 0] += dw[:, :NOPE]
            dw_ref[s, 1] += dw[:, NOPE:]
            out = (acc[0] + tn(k, ds), acc[1] + nn(rt[:, rows], ds))

            @pl.when(s == NS - 1)
            def _():
                for t in range(2):
                    for cp in d1_copies(2 * j + t):
                        cp.start()

            @pl.when(j == 0)
            def _():
                @pl.when(s > 0)
                def _():
                    stage2(s - 1)

                @pl.when(s > 1)
                def _():
                    stage4(s - 2)
            return out

        dqn, dqr = lax.fori_loop(0, y + 1, phase3, (jnp.zeros((NOPE, CH), F32), jnp.zeros((ROPE, CH), F32)))
        w_start(1, s)
        dq_ref[s, :NOPE] = (dqn * scale).astype(BF16)
        dq_ref[s, NOPE:] = (dqr * scale).astype(BF16)

        @pl.when(s > 2)
        def _():
            stage5(s - 3)
        return 0

    lax.fori_loop(0, NS, step, 0)

    @pl.when(low)
    def _():
        for cp in c_direct[2]:
            cp.wait_send()

        @pl.when(is0)
        def _():
            for cp in c_direct[3]:
                cp.wait_send()

    outs = [rcopy(o_ref.at[:, oth_rows], o_out.at[mine], xs.at[2], xr.at[2], partner),
            rcopy(dq_ref.at[:, :, oth_rows], dq_out.at[mine], xs.at[3], xr.at[3], partner)]
    for cp in outs:
        cp.start()

    def join(j):
        for cp in d1_copies(j):
            cp.wait()
        rows = pl.ds(pl.multiple_of(j * CH + core * TOK, TOK), TOK)
        msg[j, :TOK] = dcr[rows, :] + rbd[j]
        drt = (drr[rows, :] + rbr[j]).T
        msg[j, TOK:] = jnp.concatenate([drt[:ROPE // 2], drt[ROPE // 2:]], axis=1)


    quarters = [pl.ds(i * (MSG // 4), MSG // 4) for i in range(4)]

    def to_x(j):
        return [rcopy(msg.at[j, h], rbx.at[h], d2s.at[0, i], d2r.at[0, i], xn) for i, h in enumerate(quarters)]

    def to_y(j):
        return [rcopy(msg.at[j, h], rby.at[h], d2s.at[1, i], d2r.at[1, i], yn) for i, h in enumerate(quarters)]

    half_x = [rcopy(msg.at[0, quarters[i]], rbh.at[i], d2s.at[2, i], d2r.at[2, i], xn) for i in (0, 1)]
    half_y = [rcopy(msg.at[0, quarters[2 + i]], rbh.at[i], d2s.at[2, 2 + i], d2r.at[2, i], yn) for i in (0, 1)]

    def start(copies):
        for cp in copies:
            cp.start()

    def on(k):
        return pl.when(chip == k)

    def add_and_pass(i):
        to_x(1)[i].wait_recv()
        msg[1, quarters[i]] += rbx[quarters[i]]
        to_y(1)[i].start()

    stage3(NS - 2)
    join(0)
    join(1)
    stage2(NS - 1)

    @on(3)
    def _():
        start((half_x[0], half_y[0]))

    @on(2)
    def _():
        to_x(1)[0].start()
    stage5(NS - 3)
    last4(NS - 2)
    stage3(NS - 1)

    @pl.when(high)
    def _():
        join(2)

    @on(3)
    def _():
        start((half_x[1], half_y[1], to_x(2)[0]))
        add_and_pass(0)
        add_and_pass(1)
        to_x(2)[1].start()

    @on(2)
    def _():
        start(to_x(1)[1:])
        start(to_y(0)[2:])

    @on(1)
    def _():
        start(to_x(0)[:2])

    @pl.when(low)
    def _():
        last5a(NS - 2)

    @on(0)
    def _():
        last5b(NS - 2)
    last4(NS - 1)

    @on(3)
    def _():
        start(to_x(2)[2:])
        add_and_pass(2)
        add_and_pass(3)

    @on(2)
    def _():
        for i in (0, 1):
            half_x[i].wait_recv()
            msg[0, quarters[i]] += rbh[i]
            to_y(0)[i].start()

    @on(1)
    def _():
        for i in (0, 1):
            half_y[i].wait_recv()
            msg[0, quarters[2 + i]] += rbh[i]
            to_x(0)[2 + i].start()

    @pl.when(high)
    def _():
        join(3)

    def keep(h, _):
        o_out[core * HPC + h] = o_ref[h, own_rows, :]
        dq_out[core * HPC + h] = dq_ref[h, :, own_rows]
        return 0
    lax.fori_loop(0, HPC, keep, 0)

    @pl.when(high)
    def _():
        last5a(NS - 2)

    @pl.when(chip != 0)
    def _():
        last5b(NS - 2)
    last5a(NS - 1)
    last5b(NS - 1)
    last_sent(NS - 2)
    last_sent(NS - 1)

    def all_of(copies, recv):
        for cp in copies:
            if recv:
                cp.wait_recv()
            else:
                cp.wait_send()

    @pl.when(chip != 3)
    def _():
        @pl.when(chip != 1)
        def _():
            all_of(to_x(0), True)
            msg[chip] += rbx[...]

        @pl.when(chip != 2)
        def _():
            all_of(to_y(0), True)
            msg[chip] += rby[...]

    dlat_out[...] = msg[chip, :TOK].astype(BF16)
    dr_out[:ROPE // 2] = msg[chip, TOK:, :TOK].astype(BF16)
    dr_out[ROPE // 2:] = msg[chip, TOK:, TOK:].astype(BF16)

    @pl.when(chip != 0)
    def _():
        all_of(to_x(0), False)

        @pl.when(chip != 1)
        def _():
            all_of(to_y(0), False)

    @pl.when(chip == 3)
    def _():
        all_of(half_x + half_y, False)
    for cp in outs:
        cp.wait()

    for cp in w_final(NS - 1, 0) + w_final(NS - 1, 1):
        cp.wait()


PARTS = 4


def layout_kernel(dw, o_t, dq_t, dc, dr, o_out, dk_out, dv_out, dq_out, dc_out, dr_out,
                  o_stage, stage, osem, ssem):
    lat = LAT // PARTS
    stores = [pltpu.make_async_copy(a, b, osem.at[i])
              for i, (a, b) in enumerate(((o_stage, o_out), (dq_t, dq_out), (dc, dc_out), (dr, dr_out)))]

    def by_row(v):
        return jnp.swapaxes(v, 0, 1).reshape(v.shape[0] * v.shape[1], NOPE)

    def put(i):
        rows = pl.ds(i * lat * HEADS, lat * HEADS)
        return [pltpu.make_async_copy(stage.at[i % 2, a], out.at[rows], ssem.at[i % 2, a])
                for a, out in enumerate((dk_out, dv_out))]

    for i in range(PARTS):
        for a in range(2):
            if i > 1:
                put(i - 2)[a].wait()
            stage[i % 2, a] = by_row(dw[:, a, i * lat:(i + 1) * lat])
            put(i)[a].start()
        if i == 0:
            for cp in stores[1:]:
                cp.start()
            o_stage[...] = by_row(o_t[...].astype(F32)).astype(BF16)
            stores[0].start()
    for i in (PARTS - 2, PARTS - 1):
        for cp in put(i):
            cp.wait()
    for cp in stores:
        cp.wait()


def to_output_layout(dw, o_t, dq_t, dc, dr):
    any_spec = pl.BlockSpec(memory_space=pl.ANY)
    dma = pltpu.SemaphoreType.DMA
    rows = LAT // PARTS * HEADS
    return pl.pallas_call(
        layout_kernel,
        out_shape=(jax.ShapeDtypeStruct((TOK * HEADS, NOPE), BF16),
                   jax.ShapeDtypeStruct((LAT * HEADS, NOPE), F32),
                   jax.ShapeDtypeStruct((LAT * HEADS, NOPE), F32),
                   jax.ShapeDtypeStruct(dq_t.shape, BF16),
                   jax.ShapeDtypeStruct(dc.shape, BF16),
                   jax.ShapeDtypeStruct(dr.shape, BF16)),
        in_specs=[pl.BlockSpec(memory_space=pltpu.VMEM)] * 5,
        out_specs=[any_spec] * 6,
        scratch_shapes=[pltpu.VMEM((TOK * HEADS, NOPE), BF16),
                        pltpu.VMEM((2, 2, rows, NOPE), F32),
                        dma((4,)), dma((2, 2))],
        compiler_params=pltpu.CompilerParams(vmem_limit_bytes=32 << 20),
    )(dw, o_t, dq_t, dc, dr)


def solution(mesh):
    seq_spec = P("cp")

    def local_step(queries, latent, key_rope, w_uk, w_uv, d_out):
        any_spec = pl.BlockSpec(memory_space=pl.ANY)
        vm_spec = pl.BlockSpec(memory_space=pltpu.VMEM)
        dma = pltpu.SemaphoreType.DMA
        vm = pltpu.VMEM
        o_t, dq_t, dw, d_latent, d_key_rope = pl.pallas_call(
            attn_kernel,
            out_shape=(vm((HEADS, TOK, NOPE), BF16), vm((HEADS, QK, TOK), BF16), vm((HEADS, 2, LAT, NOPE), F32),
                       vm((TOK, LAT), BF16), vm((ROPE, TOK), BF16)),
            in_specs=[any_spec] * 6,
            out_specs=[vm_spec] * 5,
            scratch_shapes=[vm((TOK * HEADS, NOPE), BF16),
                            vm((LAT, HPC, NOPE), BF16), vm((LAT, HPC, NOPE), BF16),
                            vm((TOK * HEADS, NOPE), F32), vm((HPC, TOK, NOPE), BF16),
                            vm((HPC, QK, CH), BF16), vm((HPC, CH, NOPE), BF16),
                            vm((SEQ, LAT), BF16), vm((ROPE, SEQ), BF16), vm((SEQ, ROPE), BF16),
                            vm((HPC, LAT, NOPE), BF16), vm((HPC, LAT, NOPE), BF16),
                            vm((HPC, CH, NOPE), BF16), vm((HPC, QK, CH), BF16),
                            vm((NS, 2, LAT, NOPE), F32),
                            vm((SEQ, LAT), F32), vm((SEQ, ROPE), F32), vm((NCHIP, MSG, LAT), F32),
                            vm((SEQ // KC, LAT, KC), BF16), vm((SEQ, 2 * NOPE), BF16),
                            vm((CH, QK), BF16), vm((NOPE, CH), BF16),
                            vm((SEQ, CH), F32), vm((SEQ // SUB, 1, CH), F32), vm((SEQ, CH), BF16),
                            vm((2, 2, 256, NOPE), F32), vm((2, 2, 128, NOPE), F32),
                            vm((NCHIP, TOK, LAT), F32), vm((NCHIP, TOK, ROPE), F32),
                            vm((MSG, LAT), F32), vm((MSG, LAT), F32), vm((2, MSG // 4, LAT), F32),
                            dma((6,)), dma((4,)), dma((4,)), dma((3, 8)), dma((3, 7)),
                            dma((4, 2, 2)), dma((4, 2, 2)), dma((2, 2)), dma((2, 4)), dma((2, 4)),
                            dma((2, NCHIP)), dma((2, NCHIP)), dma((3, 4)), dma((3, 4))],
            compiler_params=pltpu.CompilerParams(vmem_limit_bytes=50 << 20, collective_id=0, has_side_effects=True),
            cost_estimate=pl.CostEstimate(flops=30 * 10**9, bytes_accessed=20 << 20, transcendentals=10**7),
        )(jnp.transpose(queries, (1, 2, 0)), d_out.reshape(TOK * HEADS, NOPE), latent, key_rope.T, w_uk, w_uv)

        o, dk, dv, dq_t, d_latent, d_key_rope = to_output_layout(dw, o_t, dq_t, d_latent, d_key_rope)
        return (o.reshape(TOK, HEADS, NOPE), jnp.transpose(dq_t, (2, 0, 1)), d_latent, d_key_rope.T,
                dk.reshape(LAT, HEADS, NOPE), dv.reshape(LAT, HEADS, NOPE))

    return jax.shard_map(local_step, mesh=mesh,
                         in_specs=(seq_spec, seq_spec, seq_spec, P(), P(), seq_spec),
                         out_specs=(seq_spec, seq_spec, seq_spec, seq_spec, P(), P()),
                         check_vma=False)
```

```python
import functools
import math
import jax
import jax.numpy as jnp
from jax import lax
from jax.experimental import pallas as pl
from jax.experimental.pallas import tpu as pltpu
from jax.sharding import PartitionSpec as P

F32 = jnp.float32
BF16 = jnp.bfloat16
TOK = 256
CH = 512
KC = 1024
HALF = TOK // 2
SUB = 256
HEADS = 16
HPC = 8
NS = HPC
NOPE = 128
ROPE = 64
QK = NOPE + ROPE
LAT = 512
PACK = ROPE // 2
NCHIP = 4
SEQ = CH * NCHIP
MESH = pl.DeviceIdType.MESH


def nt(a, b):
    return lax.dot_general(a, b, (((1,), (1,)), ((), ())), preferred_element_type=F32)


def nn(a, b):
    return lax.dot_general(a, b, (((1,), (0,)), ((), ())), preferred_element_type=F32)


def tn(a, b):
    return lax.dot_general(a, b, (((0,), (0,)), ((), ())), preferred_element_type=F32)


def mul(i, n):
    return pl.multiple_of(i * n, n)


def attn_kernel(q_in, do_in, c_in, r_in, wk_in, wv_in,
                o_out, dq_out, dw_out, dlat_out, dr_out,
                do_raw, wk_raw, wv_raw, stage, do_snd,
                qt, do_ref, c_ref, rt, rn, wk, wv, o_ref, dq_ref, dw_ref, dcr, drr, msg, msr, mrb,
                ct, kv, qn, dot_, s_buf, m_buf, p_buf, rb1, rb2, rbd, rbr, rbx, rby, rbh, rbxr, rbyr,
                lsem, xs, xr, cs, crs, ws, wr, ps, fs, fr):
    scale = 1.0 / math.sqrt(QK)
    c2 = scale * math.log2(math.e)
    me = lax.axis_index("cp")
    core = lax.rem(me, 2)
    chip = lax.div(me, 2)
    x = lax.rem(chip, 2)
    y = lax.div(chip, 2)
    partner = me + 1 - 2 * core
    xn = me + 2 - 4 * x
    yn = me + 4 - 8 * y
    dn = xn + 4 - 8 * y

    def rcopy(src, dst, ss, rs, dev):
        return pltpu.make_async_remote_copy(src_ref=src, dst_ref=dst, send_sem=ss, recv_sem=rs,
                                            device_id=(dev,), device_id_type=MESH)

    my_rows = pl.ds(mul(me, TOK), TOK)
    own_rows = pl.ds(mul(core, TOK), TOK)
    oth_rows = pl.ds(mul(1 - core, TOK), TOK)
    mine = pl.ds(mul(core, HPC), HPC)

    other = pl.ds(mul(1 - core, HPC), HPC)

    local = [pltpu.make_async_copy(c_in, c_ref.at[my_rows], lsem.at[0]),
             pltpu.make_async_copy(r_in, rt.at[:, my_rows], lsem.at[1]),
             pltpu.make_async_copy(q_in.at[mine], qt.at[:, :, own_rows], lsem.at[2]),
             pltpu.make_async_copy(do_in, do_raw, lsem.at[3]),
             pltpu.make_async_copy(wk_in.at[:, mine], wk_raw, lsem.at[4]),
             pltpu.make_async_copy(wv_in.at[:, mine], wv_raw, lsem.at[5])]
    for cp in local:
        cp.start()

    bar = pltpu.get_barrier_semaphore()
    for peer in (partner, xn, yn, dn):
        pl.semaphore_signal(bar, inc=1, device_id=(peer,), device_id_type=MESH)
    pl.semaphore_wait(bar, 4)

    local[0].wait()
    local[1].wait()

    def latent_copies(i, src, dev, recv=None):
        recv = i if recv is None else recv
        rows = pl.ds(mul(src, TOK), TOK)
        parts = [c_ref.at[pl.ds(pl.multiple_of(src * TOK + t * HALF, HALF), HALF)] for t in range(2)]
        parts.append(rt.at[:, rows])
        return [rcopy(ref, ref, cs.at[t, i], crs.at[t, recv], dev) for t, ref in enumerate(parts)]

    low = y == 0
    is0 = core == 0
    c_direct = [latent_copies(i, me, dev) for i, dev in enumerate((partner, xn, yn, dn))]
    c_relay = latent_copies(7, yn, xn, 3)
    for cp in c_direct[0] + c_direct[1]:
        cp.start()

    @pl.when(low)
    def _():
        for cp in c_direct[2]:
            cp.start()

        @pl.when(is0)
        def _():
            for cp in c_direct[3]:
                cp.start()

    heads = [rcopy(q_in.at[other], qt.at[:, :, own_rows], xs.at[0], xr.at[0], partner),
             rcopy(do_snd, do_ref.at[:, own_rows], xs.at[1], xr.at[1], partner)]
    heads[0].start()
    local[3].wait()

    def pick(h, rows, stride):
        return stage[pl.ds(h, rows, stride=stride), :].astype(BF16)

    def widen(i, _):
        rows = pl.ds(mul(i, 256), 256)
        stage[rows, :] = do_raw[rows, :].astype(F32)
        return 0
    lax.fori_loop(0, TOK * HEADS // 256, widen, 0)
    for i in range(HPC):
        lo = pick(i, TOK, HEADS)
        hi = pick(i + HPC, TOK, HEADS)
        do_ref[i, own_rows, :] = jnp.where(is0, lo, hi)
        do_snd[i] = jnp.where(is0, hi, lo)
    heads[1].start()
    for t, (raw, out) in enumerate(((wk_raw, wk), (wv_raw, wv))):
        local[4 + t].wait()

        def body(i, _, raw=raw):
            ls = pl.ds(mul(i, 32), 32)
            stage[pl.ds(mul(i, 256), 256), :] = raw[ls].astype(F32).reshape(256, NOPE)
            return 0
        lax.fori_loop(0, LAT // 32, body, 0)
        for i in range(HPC):
            out[i] = pick(i, LAT, HPC)

    def zero_dc(j, _):
        rows = pl.ds(mul(j, KC), KC)
        dcr[rows, :] = jnp.zeros((KC, LAT), F32)
        drr[rows, :] = jnp.zeros((KC, ROPE), F32)
        return 0
    lax.fori_loop(0, y + 1, zero_dc, 0)
    local[2].wait()
    for cp in heads:
        cp.wait()
    for cp in c_direct[0]:
        cp.wait()

    def turn(j):
        rows = pl.ds(mul(j, KC), KC)
        ct[j] = c_ref[rows, :].T
        rn[rows, :] = rt[:, rows].T

    c_fwd = [None] + [latent_copies(3 + i, src, partner) for i, src in ((1, xn), (2, yn), (3, dn))]

    high = y == 1
    for t in (0, 1, 2):
        c_direct[1][t].wait()
        c_fwd[1][t].start()

        @pl.when(high)
        def _(t=t):
            c_direct[2][t].wait_recv()

            @pl.when(core == 1)
            def _():
                c_relay[t].start()
            c_fwd[2][t].start()
    for cp in c_fwd[1]:
        cp.wait()
    turn(y)

    def wait_latents():
        for t in (0, 1, 2):
            c_direct[3][t].wait_recv()
            c_fwd[3][t].start()
        for cp in c_fwd[2] + c_fwd[3]:
            cp.wait()

        @pl.when(core == 1)
        def _():
            for cp in c_relay:
                cp.wait_send()

    hx = pl.ds(mul(x, 256), 256)
    hx1 = pl.ds(mul(1 - x, 256), 256)
    hy = pl.ds(mul(y, 256), 256)
    hy1 = pl.ds(mul(1 - y, 256), 256)
    qa = pl.ds(pl.multiple_of(x * 256 + y * 128, 128), 128)
    qa1 = pl.ds(pl.multiple_of(x * 256 + (1 - y) * 128, 128), 128)
    qb = pl.ds(pl.multiple_of(y * 256 + x * 128, 128), 128)
    qb1 = pl.ds(pl.multiple_of(y * 256 + (1 - x) * 128, 128), 128)

    def w_copy(phase, s):
        par = lax.rem(s, 2)
        t = core * NS + s
        if phase == 1:
            pair = ((dw_ref.at[s, 0, hx1], rb1.at[par, 0], xn), (dw_ref.at[s, 1, hy1], rb1.at[par, 1], yn))
        elif phase == 2:
            pair = ((dw_ref.at[s, 0, qa1], rb2.at[par, 0], yn), (dw_ref.at[s, 1, qb1], rb2.at[par, 1], xn))
        elif phase == 3:
            pair = ((dw_out.at[t, 0, qa], dw_out.at[t, 0, qa], yn),
                    (dw_out.at[t, 1, qb], dw_out.at[t, 1, qb], xn))
        else:
            pair = ((dw_out.at[t, 0, hx], dw_out.at[t, 0, hx], xn),
                    (dw_out.at[t, 1, hy], dw_out.at[t, 1, hy], yn))
        return [rcopy(a, b, ws.at[phase - 1, par, i], wr.at[phase - 1, par, i], d)
                for i, (a, b, d) in enumerate(pair)]

    def w_start(phase, s):
        for cp in w_copy(phase, s):
            cp.start()

    def w_wait(phase, s):
        for cp in w_copy(phase, s):
            cp.wait()

    def w_final(s, late):
        t = core * NS + s
        par = lax.rem(s, 2)
        parts = (hx1, hy1) if late else (hx, hy)
        return [rcopy(dw_out.at[t, i, r], dw_out.at[t, i, r], fs.at[par, 2 * late + i], fr.at[par, 2 * late + i],
                      partner) for i, r in enumerate(parts)]

    def hand_over(s, late):
        def wait_last():
            for cp in w_final(s - 1, late):
                cp.wait()
        if isinstance(s, int):
            wait_last()
        else:
            pl.when(s > 0)(wait_last)
        for cp in w_final(s, late):
            cp.start()

    def stage2(s):
        par = lax.rem(s, 2)
        w_wait(1, s)
        dw_ref[s, 0, hx] += rb1[par, 0]
        dw_ref[s, 1, hy] += rb1[par, 1]
        w_start(2, s)

    def stage3(s):
        par = lax.rem(s, 2)
        w_wait(2, s)
        t = core * NS + s
        dw_out[t, 0, qa] = dw_ref[s, 0, qa] + rb2[par, 0]
        dw_out[t, 1, qb] = dw_ref[s, 1, qb] + rb2[par, 1]
        w_start(3, s)

    def stage4(s):
        w_wait(3, s)
        w_start(4, s)
        hand_over(s, 0)

    def stage5(s):
        w_wait(4, s)
        hand_over(s, 1)

    def last4(s):
        w_wait(3, s)
        to_a, to_b = w_copy(4, s)

        @pl.when(low)
        def _():
            to_a.start()

        @pl.when(chip != 3)
        def _():
            to_b.start()
        hand_over(s, 0)

    def w_pass(s):
        par = lax.rem(s, 2)
        t = core * NS + s
        pair = ((dw_out.at[t, 0, hx1], yn), (dw_out.at[t, 1, hy1], xn))
        return [rcopy(ref, ref, ps.at[par, i], wr.at[3, par, i], dev) for i, (ref, dev) in enumerate(pair)]

    def last5a(s):
        w_copy(4, s)[0].wait_recv()

        @pl.when(low)
        def _():
            w_pass(s)[0].start()

    def last5b(s):
        w_copy(4, s)[1].wait_recv()

        @pl.when(chip == 0)
        def _():
            w_pass(s)[1].start()
        hand_over(s, 1)

    def last_sent(s):
        @pl.when(low)
        def _():
            w_copy(4, s)[0].wait_send()
            w_pass(s)[0].wait_send()

        @pl.when(chip != 3)
        def _():
            w_copy(4, s)[1].wait_send()

        @pl.when(chip == 0)
        def _():
            w_pass(s)[1].wait_send()

    def d1_copies(j):
        rows = pl.ds(pl.multiple_of(j * CH + (1 - core) * TOK, TOK), TOK)
        return (rcopy(dcr.at[rows], rbd.at[j], cs.at[0, j], crs.at[0, j], partner),
                rcopy(drr.at[rows], rbr.at[j], cs.at[1, j], crs.at[1, j], partner))

    def step(s, _):
        dw_ref[s] = jnp.zeros((2, LAT, NOPE), F32)
        qn[...] = qt[s].T
        dot_[...] = do_ref[s].T
        w_s = jnp.concatenate([wk[s], wv[s]], axis=1)

        def phase1(j, masked):
            ms, ls = [], []
            for t in range(KC // SUB):
                rows = pl.ds(pl.multiple_of(j * KC + t * SUB, SUB), SUB)
                kvv = nn(c_ref[rows, :], w_s).astype(BF16)
                kv[rows, :] = kvv
                k_cat = jnp.concatenate([kvv[:, :NOPE], rn[rows, :]], axis=1)
                s2 = nn(k_cat, qt[s]) * c2
                if masked:
                    ki = lax.broadcasted_iota(jnp.int32, (SUB, CH), 0)
                    qi = lax.broadcasted_iota(jnp.int32, (SUB, CH), 1)
                    s2 = jnp.where(ki - qi <= x * CH - t * SUB, s2, -1e30 * math.log2(math.e))
                m = jnp.max(s2, axis=0, keepdims=True)
                e = jnp.exp2(s2 - m)
                s_buf[rows, :] = e
                m_buf[j * (KC // SUB) + t] = m
                ms.append(m)
                ls.append(jnp.sum(e, axis=0, keepdims=True))
            top = functools.reduce(jnp.maximum, ms)
            return top, sum(l * jnp.exp2(m - top) for m, l in zip(ms, ls))

        stats = phase1(y, True)

        @pl.when(s > 1)
        def _():
            stage3(s - 2)

        @pl.when(s == 0)
        def _():
            @pl.when(high)
            def _():
                wait_latents()
                turn(0)

            @pl.when(low)
            def _():
                for cp in c_direct[2]:
                    cp.wait_send()

                @pl.when(is0)
                def _():
                    for cp in c_direct[3]:
                        cp.wait_send()

        def more(j, st):
            m0, l0 = st
            m1, l1 = phase1(j, False)
            m = jnp.maximum(m0, m1)
            return m, l0 * jnp.exp2(m0 - m) + l1 * jnp.exp2(m1 - m)

        m, l = lax.fori_loop(0, y, more, stats)
        lse = m + jnp.log2(l)

        def phase2(j, acc):
            rows = pl.ds(mul(j, KC), KC)
            parts = []
            for t in range(KC // SUB):
                sub = pl.ds(pl.multiple_of(j * KC + t * SUB, SUB), SUB)
                fac = jnp.exp2(m_buf[j * (KC // SUB) + t] - lse)
                parts.append((s_buf[sub, :] * fac).astype(BF16))
                p_buf[sub, :] = parts[-1]
            return acc + tn(kv[rows, NOPE:], jnp.concatenate(parts, axis=0))

        ot = lax.fori_loop(0, y + 1, phase2, jnp.zeros((NOPE, CH), F32))
        delta = jnp.sum(ot * dot_[...].astype(F32), axis=0, keepdims=True)
        o_ref[s] = ot.T.astype(BF16)

        def phase3(j, acc):
            rows = pl.ds(mul(j, KC), KC)
            k = kv[rows, :NOPE]
            v = kv[rows, NOPE:]
            pb = p_buf[rows, :]
            dp = nn(v, dot_[...])
            ds = (pb.astype(F32) * (dp - delta)).astype(BF16)
            dkr = nn(ds, qn[...]) * scale
            dv = nn(pb, do_ref[s])
            dkv = jnp.concatenate([dkr[:, :NOPE].astype(BF16), dv.astype(BF16)], axis=1)
            drr[rows, :] += dkr[:, NOPE:]
            dcr[rows, :] += nt(dkv, w_s)
            dw = nn(ct[j], dkv)
            dw_ref[s, 0] += dw[:, :NOPE]
            dw_ref[s, 1] += dw[:, NOPE:]
            out = (acc[0] + tn(k, ds), acc[1] + nn(rt[:, rows], ds))

            @pl.when(s == NS - 1)
            def _():
                for t in range(2):
                    for cp in d1_copies(2 * j + t):
                        cp.start()

            @pl.when(j == 0)
            def _():
                @pl.when(s > 0)
                def _():
                    stage2(s - 1)
            return out

        dqn, dqr = lax.fori_loop(0, y + 1, phase3, (jnp.zeros((NOPE, CH), F32), jnp.zeros((ROPE, CH), F32)))
        w_start(1, s)
        dq_ref[s, :NOPE] = (dqn * scale).astype(BF16)
        dq_ref[s, NOPE:] = (dqr * scale).astype(BF16)

        @pl.when(s > 1)
        def _():
            stage4(s - 2)

        @pl.when(s > 2)
        def _():
            stage5(s - 3)
        return 0

    lax.fori_loop(0, NS, step, 0)

    outs = [rcopy(o_ref.at[:, oth_rows], o_out.at[mine], xs.at[2], xr.at[2], partner),
            rcopy(dq_ref.at[:, :, oth_rows], dq_out.at[mine], xs.at[3], xr.at[3], partner)]
    for cp in outs:
        cp.start()

    def join(j):
        for cp in d1_copies(j):
            cp.wait()
        rows = pl.ds(pl.multiple_of(j * CH + core * TOK, TOK), TOK)
        msg[j] = dcr[rows, :] + rbd[j]
        drt = (drr[rows, :] + rbr[j]).T
        msr[j] = jnp.concatenate([drt[:PACK], drt[PACK:]], axis=1)
        mrb[j] = msr[j].astype(BF16)


    quarters = [pl.ds(i * (TOK // 4), TOK // 4) for i in range(4)]

    def slot(kind, i):
        if kind == 2:
            return 2, i
        return (kind, 4 + i) if i < 4 else (2, 5 + kind)

    def to_x(j):
        return ([rcopy(msg.at[j, h], rbx.at[h], cs.at[slot(0, i)], crs.at[slot(0, i)], xn) for i, h in enumerate(quarters)]
                + [rcopy(mrb.at[j], rbxr, cs.at[slot(0, 4)], crs.at[slot(0, 4)], xn)])

    def to_y(j):
        return ([rcopy(msg.at[j, h], rby.at[h], cs.at[slot(1, i)], crs.at[slot(1, i)], yn) for i, h in enumerate(quarters)]
                + [rcopy(mrb.at[j], rbyr, cs.at[slot(1, 4)], crs.at[slot(1, 4)], yn)])

    half_x = [rcopy(msg.at[0, quarters[i]], rbh.at[i], cs.at[slot(2, i)], crs.at[slot(2, i)], xn) for i in (0, 1)]
    half_y = [rcopy(msg.at[0, quarters[2 + i]], rbh.at[i], cs.at[slot(2, 2 + i)], crs.at[slot(2, i)], yn) for i in (0, 1)]
    half_y.append(rcopy(mrb.at[0], rbxr, cs.at[slot(2, 4)], crs.at[slot(2, 4)], yn))

    def start(copies):
        for cp in copies:
            cp.start()

    def on(k):
        return pl.when(chip == k)

    def add_and_pass(i):
        to_x(1)[i].wait_recv()
        msg[1, quarters[i]] += rbx[quarters[i]]
        to_y(1)[i].start()

    def add_dr(j, buf):
        msr[j] += buf[...].astype(F32)
        mrb[j] = msr[j].astype(BF16)

    stage3(NS - 2)
    join(0)
    join(1)
    stage2(NS - 1)

    stage5(NS - 3)
    last4(NS - 2)
    stage3(NS - 1)

    @on(3)
    def _():
        start((half_x[0], half_y[0]))

    @on(2)
    def _():
        to_x(1)[0].start()

    @pl.when(high)
    def _():
        join(2)

    @on(3)
    def _():
        start((half_x[1], half_y[1], half_y[2], to_x(2)[0]))
        add_and_pass(0)
        add_and_pass(1)
        to_x(2)[1].start()

    @on(2)
    def _():
        start(to_x(1)[1:])
        start(to_y(0)[2:])

    @on(1)
    def _():
        start(to_x(0)[:2])

    @pl.when(low)
    def _():
        last5a(NS - 2)

    @on(0)
    def _():
        last5b(NS - 2)
    last4(NS - 1)

    @on(3)
    def _():
        start(to_x(2)[2:])
        add_and_pass(2)
        add_and_pass(3)
        to_x(1)[4].wait_recv()
        add_dr(1, rbxr)
        to_y(1)[4].start()

    @on(2)
    def _():
        for i in (0, 1):
            half_x[i].wait_recv()
            msg[0, quarters[i]] += rbh[i]
            to_y(0)[i].start()

    @on(1)
    def _():
        for i in (0, 1):
            half_y[i].wait_recv()
            msg[0, quarters[2 + i]] += rbh[i]
            to_x(0)[2 + i].start()
        half_y[2].wait_recv()
        add_dr(0, rbxr)
        to_x(0)[4].start()

    @pl.when(high)
    def _():
        join(3)

    def keep(h, _):
        o_out[core * HPC + h] = o_ref[h, own_rows, :]
        dq_out[core * HPC + h] = dq_ref[h, :, own_rows]
        return 0
    lax.fori_loop(0, HPC, keep, 0)

    @pl.when(high)
    def _():
        last5a(NS - 2)

    @pl.when(chip != 0)
    def _():
        last5b(NS - 2)
    last5a(NS - 1)
    last5b(NS - 1)
    last_sent(NS - 2)
    last_sent(NS - 1)

    def all_of(copies, recv):
        for cp in copies:
            if recv:
                cp.wait_recv()
            else:
                cp.wait_send()

    @pl.when(chip != 3)
    def _():
        @pl.when(chip != 1)
        def _():
            all_of(to_x(0), True)
            msg[chip] += rbx[...]
            add_dr(chip, rbxr)

        @pl.when(chip != 2)
        def _():
            all_of(to_y(0), True)
            msg[chip] += rby[...]
            add_dr(chip, rbyr)

    dlat_out[...] = msg[chip].astype(BF16)
    dr_out[:PACK] = msr[chip, :, :TOK].astype(BF16)
    dr_out[PACK:] = msr[chip, :, TOK:].astype(BF16)

    @pl.when(chip != 0)
    def _():
        all_of(to_x(0), False)

        @pl.when(chip != 1)
        def _():
            all_of(to_y(0), False)

    @pl.when(chip == 3)
    def _():
        all_of(half_x + half_y, False)
    for cp in outs:
        cp.wait()

    for cp in w_final(NS - 1, 0) + w_final(NS - 1, 1):
        cp.wait()


PARTS = 4


def layout_kernel(dw, o_t, dq_t, dc, dr, o_out, dk_out, dv_out, dq_out, dc_out, dr_out,
                  o_stage, stage, osem, ssem):
    lat = LAT // PARTS
    stores = [pltpu.make_async_copy(a, b, osem.at[i])
              for i, (a, b) in enumerate(((o_stage, o_out), (dq_t, dq_out), (dc, dc_out), (dr, dr_out)))]

    def by_row(v):
        return jnp.swapaxes(v, 0, 1).reshape(v.shape[0] * v.shape[1], NOPE)

    def put(i):
        rows = pl.ds(i * lat * HEADS, lat * HEADS)
        return [pltpu.make_async_copy(stage.at[i % 2, a], out.at[rows], ssem.at[i % 2, a])
                for a, out in enumerate((dk_out, dv_out))]

    for i in range(PARTS):
        for a in range(2):
            if i > 1:
                put(i - 2)[a].wait()
            stage[i % 2, a] = by_row(dw[:, a, i * lat:(i + 1) * lat])
            put(i)[a].start()
        if i == 0:
            for cp in stores[1:]:
                cp.start()
            o_stage[...] = by_row(o_t[...].astype(F32)).astype(BF16)
            stores[0].start()
    for i in (PARTS - 2, PARTS - 1):
        for cp in put(i):
            cp.wait()
    for cp in stores:
        cp.wait()


def to_output_layout(dw, o_t, dq_t, dc, dr):
    any_spec = pl.BlockSpec(memory_space=pl.ANY)
    dma = pltpu.SemaphoreType.DMA
    rows = LAT // PARTS * HEADS
    return pl.pallas_call(
        layout_kernel,
        out_shape=(jax.ShapeDtypeStruct((TOK * HEADS, NOPE), BF16),
                   jax.ShapeDtypeStruct((LAT * HEADS, NOPE), F32),
                   jax.ShapeDtypeStruct((LAT * HEADS, NOPE), F32),
                   jax.ShapeDtypeStruct(dq_t.shape, BF16),
                   jax.ShapeDtypeStruct(dc.shape, BF16),
                   jax.ShapeDtypeStruct(dr.shape, BF16)),
        in_specs=[pl.BlockSpec(memory_space=pltpu.VMEM)] * 5,
        out_specs=[any_spec] * 6,
        scratch_shapes=[pltpu.VMEM((TOK * HEADS, NOPE), BF16),
                        pltpu.VMEM((2, 2, rows, NOPE), F32),
                        dma((4,)), dma((2, 2))],
        compiler_params=pltpu.CompilerParams(vmem_limit_bytes=32 << 20),
    )(dw, o_t, dq_t, dc, dr)


def solution(mesh):
    seq_spec = P("cp")

    def local_step(queries, latent, key_rope, w_uk, w_uv, d_out):
        any_spec = pl.BlockSpec(memory_space=pl.ANY)
        vm_spec = pl.BlockSpec(memory_space=pltpu.VMEM)
        dma = pltpu.SemaphoreType.DMA
        vm = pltpu.VMEM
        o_t, dq_t, dw, d_latent, d_key_rope = pl.pallas_call(
            attn_kernel,
            out_shape=(vm((HEADS, TOK, NOPE), BF16), vm((HEADS, QK, TOK), BF16), vm((HEADS, 2, LAT, NOPE), F32),
                       vm((TOK, LAT), BF16), vm((ROPE, TOK), BF16)),
            in_specs=[any_spec] * 6,
            out_specs=[vm_spec] * 5,
            scratch_shapes=[vm((TOK * HEADS, NOPE), BF16),
                            vm((LAT, HPC, NOPE), BF16), vm((LAT, HPC, NOPE), BF16),
                            vm((TOK * HEADS, NOPE), F32), vm((HPC, TOK, NOPE), BF16),
                            vm((HPC, QK, CH), BF16), vm((HPC, CH, NOPE), BF16),
                            vm((SEQ, LAT), BF16), vm((ROPE, SEQ), BF16), vm((SEQ, ROPE), BF16),
                            vm((HPC, LAT, NOPE), BF16), vm((HPC, LAT, NOPE), BF16),
                            vm((HPC, CH, NOPE), BF16), vm((HPC, QK, CH), BF16),
                            vm((NS, 2, LAT, NOPE), F32),
                            vm((SEQ, LAT), F32), vm((SEQ, ROPE), F32), vm((NCHIP, TOK, LAT), F32), vm((NCHIP, PACK, LAT), F32), vm((NCHIP, PACK, LAT), BF16),
                            vm((SEQ // KC, LAT, KC), BF16), vm((SEQ, 2 * NOPE), BF16),
                            vm((CH, QK), BF16), vm((NOPE, CH), BF16),
                            vm((SEQ, CH), F32), vm((SEQ // SUB, 1, CH), F32), vm((SEQ, CH), BF16),
                            vm((2, 2, 256, NOPE), F32), vm((2, 2, 128, NOPE), F32),
                            vm((NCHIP, TOK, LAT), F32), vm((NCHIP, TOK, ROPE), F32),
                            vm((TOK, LAT), F32), vm((TOK, LAT), F32), vm((2, TOK // 4, LAT), F32),
                            vm((PACK, LAT), BF16), vm((PACK, LAT), BF16),
                            dma((6,)), dma((4,)), dma((4,)), dma((3, 8)), dma((3, 8)),
                            dma((4, 2, 2)), dma((4, 2, 2)), dma((2, 2)), dma((2, 4)), dma((2, 4))],
            compiler_params=pltpu.CompilerParams(vmem_limit_bytes=50 << 20, collective_id=0, has_side_effects=True),
            cost_estimate=pl.CostEstimate(flops=30 * 10**9, bytes_accessed=20 << 20, transcendentals=10**7),
        )(jnp.transpose(queries, (1, 2, 0)), d_out.reshape(TOK * HEADS, NOPE), latent, key_rope.T, w_uk, w_uv)

        o, dk, dv, dq_t, d_latent, d_key_rope = to_output_layout(dw, o_t, dq_t, d_latent, d_key_rope)
        return (o.reshape(TOK, HEADS, NOPE), jnp.transpose(dq_t, (2, 0, 1)), d_latent, d_key_rope.T,
                dk.reshape(LAT, HEADS, NOPE), dv.reshape(LAT, HEADS, NOPE))

    return jax.shard_map(local_step, mesh=mesh,
                         in_specs=(seq_spec, seq_spec, seq_spec, P(), P(), seq_spec),
                         out_specs=(seq_spec, seq_spec, seq_spec, seq_spec, P(), P()),
                         check_vma=False)
```

```python
import functools
import math
import jax
import jax.numpy as jnp
from jax import lax
from jax.experimental import pallas as pl
from jax.experimental.pallas import tpu as pltpu
from jax.sharding import PartitionSpec as P

F32 = jnp.float32
BF16 = jnp.bfloat16
TOK = 256
CH = 512
KC = 1024
HALF = TOK // 2
SUB = 256
HEADS = 16
HPC = 8
NS = HPC
NOPE = 128
ROPE = 64
QK = NOPE + ROPE
LAT = 512
PACK = ROPE // 2
NCHIP = 4
SEQ = CH * NCHIP
MESH = pl.DeviceIdType.MESH


def nt(a, b):
    return lax.dot_general(a, b, (((1,), (1,)), ((), ())), preferred_element_type=F32)


def nn(a, b):
    return lax.dot_general(a, b, (((1,), (0,)), ((), ())), preferred_element_type=F32)


def tn(a, b):
    return lax.dot_general(a, b, (((0,), (0,)), ((), ())), preferred_element_type=F32)


def mul(i, n):
    return pl.multiple_of(i * n, n)


def attn_kernel(q_in, do_in, c_in, r_in, wk_in, wv_in,
                o_out, dq_out, dw_out, dlat_out, dr_out,
                do_raw, wk_raw, wv_raw, stage, do_snd,
                qt, do_ref, c_ref, rt, rn, wk, wv, o_ref, dq_ref, dw_ref, dcr, drr, msg, msr, mrb,
                ct, kv, qn, dot_, s_buf, m_buf, p_buf, rb1, rb2, rbd, rbr, rbx, rby, rbh, rbxr, rbyr,
                lsem, xs, xr, cs, crs, ws, wr, ps, fs, fr):
    scale = 1.0 / math.sqrt(QK)
    c2 = scale * math.log2(math.e)
    me = lax.axis_index("cp")
    core = lax.rem(me, 2)
    chip = lax.div(me, 2)
    x = lax.rem(chip, 2)
    y = lax.div(chip, 2)
    partner = me + 1 - 2 * core
    xn = me + 2 - 4 * x
    yn = me + 4 - 8 * y
    dn = xn + 4 - 8 * y

    def rcopy(src, dst, ss, rs, dev):
        return pltpu.make_async_remote_copy(src_ref=src, dst_ref=dst, send_sem=ss, recv_sem=rs,
                                            device_id=(dev,), device_id_type=MESH)

    my_rows = pl.ds(mul(me, TOK), TOK)
    own_rows = pl.ds(mul(core, TOK), TOK)
    oth_rows = pl.ds(mul(1 - core, TOK), TOK)
    mine = pl.ds(mul(core, HPC), HPC)

    other = pl.ds(mul(1 - core, HPC), HPC)

    local = [pltpu.make_async_copy(c_in, c_ref.at[my_rows], lsem.at[0]),
             pltpu.make_async_copy(r_in, rt.at[:, my_rows], lsem.at[1]),
             pltpu.make_async_copy(q_in.at[mine], qt.at[:, :, own_rows], lsem.at[2]),
             pltpu.make_async_copy(do_in, do_raw, lsem.at[3]),
             pltpu.make_async_copy(wk_in.at[:, mine], wk_raw, lsem.at[4]),
             pltpu.make_async_copy(wv_in.at[:, mine], wv_raw, lsem.at[5])]
    for cp in local:
        cp.start()

    bar = pltpu.get_barrier_semaphore()
    for peer in (partner, xn, yn, dn):
        pl.semaphore_signal(bar, inc=1, device_id=(peer,), device_id_type=MESH)
    pl.semaphore_wait(bar, 4)

    local[0].wait()
    local[1].wait()

    def latent_copies(i, src, dev, recv=None):
        recv = i if recv is None else recv
        rows = pl.ds(mul(src, TOK), TOK)
        parts = [c_ref.at[pl.ds(pl.multiple_of(src * TOK + t * HALF, HALF), HALF)] for t in range(2)]
        parts.append(rt.at[:, rows])
        return [rcopy(ref, ref, cs.at[t, i], crs.at[t, recv], dev) for t, ref in enumerate(parts)]

    low = y == 0
    is0 = core == 0
    c_direct = [latent_copies(i, me, dev) for i, dev in enumerate((partner, xn, yn, dn))]
    c_relay = latent_copies(7, yn, xn, 3)
    for cp in c_direct[0] + c_direct[1]:
        cp.start()

    @pl.when(low)
    def _():
        for cp in c_direct[2]:
            cp.start()

        @pl.when(is0)
        def _():
            for cp in c_direct[3]:
                cp.start()

    heads = [rcopy(q_in.at[other], qt.at[:, :, own_rows], xs.at[0], xr.at[0], partner),
             rcopy(do_snd, do_ref.at[:, own_rows], xs.at[1], xr.at[1], partner)]
    heads[0].start()
    local[3].wait()

    def pick(h, rows, stride):
        return stage[pl.ds(h, rows, stride=stride), :].astype(BF16)

    def widen(i, _):
        rows = pl.ds(mul(i, 256), 256)
        stage[rows, :] = do_raw[rows, :].astype(F32)
        return 0
    lax.fori_loop(0, TOK * HEADS // 256, widen, 0)
    for i in range(HPC):
        lo = pick(i, TOK, HEADS)
        hi = pick(i + HPC, TOK, HEADS)
        do_ref[i, own_rows, :] = jnp.where(is0, lo, hi)
        do_snd[i] = jnp.where(is0, hi, lo)
    heads[1].start()
    for t, (raw, out) in enumerate(((wk_raw, wk), (wv_raw, wv))):
        local[4 + t].wait()

        def body(i, _, raw=raw):
            ls = pl.ds(mul(i, 32), 32)
            stage[pl.ds(mul(i, 256), 256), :] = raw[ls].astype(F32).reshape(256, NOPE)
            return 0
        lax.fori_loop(0, LAT // 32, body, 0)
        for i in range(HPC):
            out[i] = pick(i, LAT, HPC)

    def zero_dc(j, _):
        rows = pl.ds(mul(j, KC), KC)
        dcr[rows, :] = jnp.zeros((KC, LAT), F32)
        drr[rows, :] = jnp.zeros((KC, ROPE), F32)
        return 0
    lax.fori_loop(0, y + 1, zero_dc, 0)
    local[2].wait()
    for cp in heads:
        cp.wait()
    for cp in c_direct[0]:
        cp.wait()

    def turn(j):
        rows = pl.ds(mul(j, KC), KC)
        ct[j] = c_ref[rows, :].T
        rn[rows, :] = rt[:, rows].T

    c_fwd = [None] + [latent_copies(3 + i, src, partner) for i, src in ((1, xn), (2, yn), (3, dn))]

    high = y == 1
    for t in (0, 1, 2):
        c_direct[1][t].wait()
        c_fwd[1][t].start()

        @pl.when(high)
        def _(t=t):
            c_direct[2][t].wait_recv()

            @pl.when(core == 1)
            def _():
                c_relay[t].start()
            c_fwd[2][t].start()
    for cp in c_fwd[1]:
        cp.wait()
    turn(y)

    def wait_latents():
        for t in (0, 1, 2):
            c_direct[3][t].wait_recv()
            c_fwd[3][t].start()
        for cp in c_fwd[2] + c_fwd[3]:
            cp.wait()

        @pl.when(core == 1)
        def _():
            for cp in c_relay:
                cp.wait_send()

    hx = pl.ds(mul(x, 256), 256)
    hx1 = pl.ds(mul(1 - x, 256), 256)
    hy = pl.ds(mul(y, 256), 256)
    hy1 = pl.ds(mul(1 - y, 256), 256)
    qa = pl.ds(pl.multiple_of(x * 256 + y * 128, 128), 128)
    qa1 = pl.ds(pl.multiple_of(x * 256 + (1 - y) * 128, 128), 128)
    qb = pl.ds(pl.multiple_of(y * 256 + x * 128, 128), 128)
    qb1 = pl.ds(pl.multiple_of(y * 256 + (1 - x) * 128, 128), 128)

    def w_copy(phase, s):
        par = lax.rem(s, 2)
        t = core * NS + s
        if phase == 1:
            pair = ((dw_ref.at[s, 0, hx1], rb1.at[par, 0], xn), (dw_ref.at[s, 1, hy1], rb1.at[par, 1], yn))
        elif phase == 2:
            pair = ((dw_ref.at[s, 0, qa1], rb2.at[par, 0], yn), (dw_ref.at[s, 1, qb1], rb2.at[par, 1], xn))
        elif phase == 3:
            pair = ((dw_out.at[t, 0, qa], dw_out.at[t, 0, qa], yn),
                    (dw_out.at[t, 1, qb], dw_out.at[t, 1, qb], xn))
        else:
            pair = ((dw_out.at[t, 0, hx], dw_out.at[t, 0, hx], xn),
                    (dw_out.at[t, 1, hy], dw_out.at[t, 1, hy], yn))
        return [rcopy(a, b, ws.at[phase - 1, par, i], wr.at[phase - 1, par, i], d)
                for i, (a, b, d) in enumerate(pair)]

    def w_start(phase, s):
        for cp in w_copy(phase, s):
            cp.start()

    def w_wait(phase, s):
        for cp in w_copy(phase, s):
            cp.wait()

    def w_final(s, late):
        t = core * NS + s
        par = lax.rem(s, 2)
        parts = (hx1, hy1) if late else (hx, hy)
        return [rcopy(dw_out.at[t, i, r], dw_out.at[t, i, r], fs.at[par, 2 * late + i], fr.at[par, 2 * late + i],
                      partner) for i, r in enumerate(parts)]

    def hand_over(s, late):
        def wait_last():
            for cp in w_final(s - 1, late):
                cp.wait()
        if isinstance(s, int):
            wait_last()
        else:
            pl.when(s > 0)(wait_last)
        for cp in w_final(s, late):
            cp.start()

    def stage2(s):
        par = lax.rem(s, 2)
        w_wait(1, s)
        dw_ref[s, 0, hx] += rb1[par, 0]
        dw_ref[s, 1, hy] += rb1[par, 1]
        w_start(2, s)

    def stage3(s):
        par = lax.rem(s, 2)
        w_wait(2, s)
        t = core * NS + s
        dw_out[t, 0, qa] = dw_ref[s, 0, qa] + rb2[par, 0]
        dw_out[t, 1, qb] = dw_ref[s, 1, qb] + rb2[par, 1]
        w_start(3, s)

    def stage4(s):
        w_wait(3, s)
        w_start(4, s)
        hand_over(s, 0)

    def stage5(s):
        w_wait(4, s)
        hand_over(s, 1)

    def last4(s):
        w_wait(3, s)
        to_a, to_b = w_copy(4, s)

        @pl.when(low)
        def _():
            to_a.start()

        @pl.when(chip != 3)
        def _():
            to_b.start()
        hand_over(s, 0)

    def w_pass(s):
        par = lax.rem(s, 2)
        t = core * NS + s
        pair = ((dw_out.at[t, 0, hx1], yn), (dw_out.at[t, 1, hy1], xn))
        return [rcopy(ref, ref, ps.at[par, i], wr.at[3, par, i], dev) for i, (ref, dev) in enumerate(pair)]

    def last5a(s):
        w_copy(4, s)[0].wait_recv()

        @pl.when(low)
        def _():
            w_pass(s)[0].start()

    def last5b(s):
        w_copy(4, s)[1].wait_recv()

        @pl.when(chip == 0)
        def _():
            w_pass(s)[1].start()
        hand_over(s, 1)

    def last_sent(s):
        @pl.when(low)
        def _():
            w_copy(4, s)[0].wait_send()
            w_pass(s)[0].wait_send()

        @pl.when(chip != 3)
        def _():
            w_copy(4, s)[1].wait_send()

        @pl.when(chip == 0)
        def _():
            w_pass(s)[1].wait_send()

    def d1_copies(j):
        rows = pl.ds(pl.multiple_of(j * CH + (1 - core) * TOK, TOK), TOK)
        return (rcopy(dcr.at[rows], rbd.at[j], cs.at[0, j], crs.at[0, j], partner),
                rcopy(drr.at[rows], rbr.at[j], cs.at[1, j], crs.at[1, j], partner))

    def step(s, _):
        dw_ref[s] = jnp.zeros((2, LAT, NOPE), F32)
        qn[...] = qt[s].T
        dot_[...] = do_ref[s].T
        w_s = jnp.concatenate([wk[s], wv[s]], axis=1)

        def phase1(j, masked):
            ms, ls = [], []
            for t in range(KC // SUB):
                rows = pl.ds(pl.multiple_of(j * KC + t * SUB, SUB), SUB)
                kvv = nn(c_ref[rows, :], w_s).astype(BF16)
                kv[rows, :] = kvv
                k_cat = jnp.concatenate([kvv[:, :NOPE], rn[rows, :]], axis=1)
                s2 = nn(k_cat, qt[s]) * c2
                if masked:
                    ki = lax.broadcasted_iota(jnp.int32, (SUB, CH), 0)
                    qi = lax.broadcasted_iota(jnp.int32, (SUB, CH), 1)
                    s2 = jnp.where(ki - qi <= x * CH - t * SUB, s2, -1e30 * math.log2(math.e))
                m = jnp.max(s2, axis=0, keepdims=True)
                e = jnp.exp2(s2 - m)
                s_buf[rows, :] = e
                m_buf[j * (KC // SUB) + t] = m
                ms.append(m)
                ls.append(jnp.sum(e, axis=0, keepdims=True))
            top = functools.reduce(jnp.maximum, ms)
            return top, sum(l * jnp.exp2(m - top) for m, l in zip(ms, ls))

        stats = phase1(y, True)

        @pl.when(s > 1)
        def _():
            stage3(s - 2)

        @pl.when(s == 0)
        def _():
            @pl.when(high)
            def _():
                wait_latents()
                turn(0)

            @pl.when(low)
            def _():
                for cp in c_direct[2]:
                    cp.wait_send()

                @pl.when(is0)
                def _():
                    for cp in c_direct[3]:
                        cp.wait_send()

        def more(j, st):
            m0, l0 = st
            m1, l1 = phase1(j, False)
            m = jnp.maximum(m0, m1)
            return m, l0 * jnp.exp2(m0 - m) + l1 * jnp.exp2(m1 - m)

        top, l = lax.fori_loop(0, y, more, stats)
        inv = 1.0 / l

        def phase2(j, acc):
            rows = pl.ds(mul(j, KC), KC)
            parts = []
            for t in range(KC // SUB):
                sub = pl.ds(pl.multiple_of(j * KC + t * SUB, SUB), SUB)
                fac = jnp.exp2(m_buf[j * (KC // SUB) + t] - top) * inv
                parts.append((s_buf[sub, :] * fac).astype(BF16))
                p_buf[sub, :] = parts[-1]
            return acc + tn(kv[rows, NOPE:], jnp.concatenate(parts, axis=0))

        ot = lax.fori_loop(0, y + 1, phase2, jnp.zeros((NOPE, CH), F32))
        delta = jnp.sum(ot * dot_[...].astype(F32), axis=0, keepdims=True)
        o_ref[s] = ot.T.astype(BF16)

        def phase3(j, acc):
            rows = pl.ds(mul(j, KC), KC)
            k = kv[rows, :NOPE]
            v = kv[rows, NOPE:]
            pb = p_buf[rows, :]
            dp = nn(v, dot_[...])
            ds = (pb.astype(F32) * (dp - delta)).astype(BF16)
            dkr = nn(ds, qn[...]) * scale
            dv = nn(pb, do_ref[s])
            dkv = jnp.concatenate([dkr[:, :NOPE].astype(BF16), dv.astype(BF16)], axis=1)
            drr[rows, :] += dkr[:, NOPE:]
            dcr[rows, :] += nt(dkv, w_s)
            dw = nn(ct[j], dkv)
            dw_ref[s, 0] += dw[:, :NOPE]
            dw_ref[s, 1] += dw[:, NOPE:]
            out = (acc[0] + tn(k, ds), acc[1] + nn(rt[:, rows], ds))

            @pl.when(s == NS - 1)
            def _():
                for t in range(2):
                    for cp in d1_copies(2 * j + t):
                        cp.start()

            @pl.when(j == 0)
            def _():
                @pl.when(s > 0)
                def _():
                    stage2(s - 1)
            return out

        dqn, dqr = lax.fori_loop(0, y + 1, phase3, (jnp.zeros((NOPE, CH), F32), jnp.zeros((ROPE, CH), F32)))
        w_start(1, s)
        dq_ref[s, :NOPE] = (dqn * scale).astype(BF16)
        dq_ref[s, NOPE:] = (dqr * scale).astype(BF16)

        @pl.when(s > 1)
        def _():
            stage4(s - 2)

        @pl.when(s > 2)
        def _():
            stage5(s - 3)
        return 0

    lax.fori_loop(0, NS, step, 0)

    outs = [rcopy(o_ref.at[:, oth_rows], o_out.at[mine], xs.at[2], xr.at[2], partner),
            rcopy(dq_ref.at[:, :, oth_rows], dq_out.at[mine], xs.at[3], xr.at[3], partner)]
    for cp in outs:
        cp.start()

    def join(j):
        for cp in d1_copies(j):
            cp.wait()
        rows = pl.ds(pl.multiple_of(j * CH + core * TOK, TOK), TOK)
        msg[j] = dcr[rows, :] + rbd[j]
        drt = (drr[rows, :] + rbr[j]).T
        msr[j] = jnp.concatenate([drt[:PACK], drt[PACK:]], axis=1)
        mrb[j] = msr[j].astype(BF16)


    quarters = [pl.ds(i * (TOK // 4), TOK // 4) for i in range(4)]

    def slot(kind, i):
        if kind == 2:
            return 2, i
        return (kind, 4 + i) if i < 4 else (2, 5 + kind)

    def to_x(j):
        return ([rcopy(msg.at[j, h], rbx.at[h], cs.at[slot(0, i)], crs.at[slot(0, i)], xn) for i, h in enumerate(quarters)]
                + [rcopy(mrb.at[j], rbxr, cs.at[slot(0, 4)], crs.at[slot(0, 4)], xn)])

    def to_y(j):
        return ([rcopy(msg.at[j, h], rby.at[h], cs.at[slot(1, i)], crs.at[slot(1, i)], yn) for i, h in enumerate(quarters)]
                + [rcopy(mrb.at[j], rbyr, cs.at[slot(1, 4)], crs.at[slot(1, 4)], yn)])

    half_x = [rcopy(msg.at[0, quarters[i]], rbh.at[i], cs.at[slot(2, i)], crs.at[slot(2, i)], xn) for i in (0, 1)]
    half_y = [rcopy(msg.at[0, quarters[2 + i]], rbh.at[i], cs.at[slot(2, 2 + i)], crs.at[slot(2, i)], yn) for i in (0, 1)]
    half_y.append(rcopy(mrb.at[0], rbxr, cs.at[slot(2, 4)], crs.at[slot(2, 4)], yn))

    def start(copies):
        for cp in copies:
            cp.start()

    def on(k):
        return pl.when(chip == k)

    def add_and_pass(i):
        to_x(1)[i].wait_recv()
        msg[1, quarters[i]] += rbx[quarters[i]]
        to_y(1)[i].start()

    def add_dr(j, buf):
        msr[j] += buf[...].astype(F32)
        mrb[j] = msr[j].astype(BF16)

    stage3(NS - 2)
    join(0)
    join(1)
    stage2(NS - 1)

    stage5(NS - 3)
    last4(NS - 2)
    stage3(NS - 1)

    @on(3)
    def _():
        start((half_x[0], half_y[0]))

    @on(2)
    def _():
        to_x(1)[0].start()

    @pl.when(high)
    def _():
        join(2)

    @on(3)
    def _():
        start((half_x[1], half_y[1], half_y[2], to_x(2)[0]))
        add_and_pass(0)
        add_and_pass(1)
        to_x(2)[1].start()

    @on(2)
    def _():
        start(to_x(1)[1:])
        start(to_y(0)[2:])

    @on(1)
    def _():
        start(to_x(0)[:2])

    @pl.when(low)
    def _():
        last5a(NS - 2)

    @on(0)
    def _():
        last5b(NS - 2)
    last4(NS - 1)

    @on(3)
    def _():
        start(to_x(2)[2:])
        add_and_pass(2)
        add_and_pass(3)
        to_x(1)[4].wait_recv()
        add_dr(1, rbxr)
        to_y(1)[4].start()

    @on(2)
    def _():
        for i in (0, 1):
            half_x[i].wait_recv()
            msg[0, quarters[i]] += rbh[i]
            to_y(0)[i].start()

    @on(1)
    def _():
        for i in (0, 1):
            half_y[i].wait_recv()
            msg[0, quarters[2 + i]] += rbh[i]
            to_x(0)[2 + i].start()
        half_y[2].wait_recv()
        add_dr(0, rbxr)
        to_x(0)[4].start()

    @pl.when(high)
    def _():
        join(3)

    def keep(h, _):
        o_out[core * HPC + h] = o_ref[h, own_rows, :]
        dq_out[core * HPC + h] = dq_ref[h, :, own_rows]
        return 0
    lax.fori_loop(0, HPC, keep, 0)

    @pl.when(high)
    def _():
        last5a(NS - 2)

    @pl.when(chip != 0)
    def _():
        last5b(NS - 2)
    last5a(NS - 1)
    last5b(NS - 1)
    last_sent(NS - 2)
    last_sent(NS - 1)

    def all_of(copies, recv):
        for cp in copies:
            if recv:
                cp.wait_recv()
            else:
                cp.wait_send()

    @pl.when(chip != 3)
    def _():
        @pl.when(chip != 1)
        def _():
            all_of(to_x(0), True)
            msg[chip] += rbx[...]
            add_dr(chip, rbxr)

        @pl.when(chip != 2)
        def _():
            all_of(to_y(0), True)
            msg[chip] += rby[...]
            add_dr(chip, rbyr)

    dlat_out[...] = msg[chip].astype(BF16)
    dr_out[:PACK] = msr[chip, :, :TOK].astype(BF16)
    dr_out[PACK:] = msr[chip, :, TOK:].astype(BF16)

    @pl.when(chip != 0)
    def _():
        all_of(to_x(0), False)

        @pl.when(chip != 1)
        def _():
            all_of(to_y(0), False)

    @pl.when(chip == 3)
    def _():
        all_of(half_x + half_y, False)
    for cp in outs:
        cp.wait()

    for cp in w_final(NS - 1, 0) + w_final(NS - 1, 1):
        cp.wait()


PARTS = 4


def layout_kernel(dw, o_t, dq_t, dc, dr, o_out, dk_out, dv_out, dq_out, dc_out, dr_out,
                  o_stage, stage, osem, ssem):
    lat = LAT // PARTS
    stores = [pltpu.make_async_copy(a, b, osem.at[i])
              for i, (a, b) in enumerate(((o_stage, o_out), (dq_t, dq_out), (dc, dc_out), (dr, dr_out)))]

    def by_row(v):
        return jnp.swapaxes(v, 0, 1).reshape(v.shape[0] * v.shape[1], NOPE)

    def put(i):
        rows = pl.ds(i * lat * HEADS, lat * HEADS)
        return [pltpu.make_async_copy(stage.at[i % 2, a], out.at[rows], ssem.at[i % 2, a])
                for a, out in enumerate((dk_out, dv_out))]

    for i in range(PARTS):
        for a in range(2):
            if i > 1:
                put(i - 2)[a].wait()
            stage[i % 2, a] = by_row(dw[:, a, i * lat:(i + 1) * lat])
            put(i)[a].start()
        if i == 0:
            for cp in stores[1:]:
                cp.start()
            o_stage[...] = by_row(o_t[...].astype(F32)).astype(BF16)
            stores[0].start()
    for i in (PARTS - 2, PARTS - 1):
        for cp in put(i):
            cp.wait()
    for cp in stores:
        cp.wait()


def to_output_layout(dw, o_t, dq_t, dc, dr):
    any_spec = pl.BlockSpec(memory_space=pl.ANY)
    dma = pltpu.SemaphoreType.DMA
    rows = LAT // PARTS * HEADS
    return pl.pallas_call(
        layout_kernel,
        out_shape=(jax.ShapeDtypeStruct((TOK * HEADS, NOPE), BF16),
                   jax.ShapeDtypeStruct((LAT * HEADS, NOPE), F32),
                   jax.ShapeDtypeStruct((LAT * HEADS, NOPE), F32),
                   jax.ShapeDtypeStruct(dq_t.shape, BF16),
                   jax.ShapeDtypeStruct(dc.shape, BF16),
                   jax.ShapeDtypeStruct(dr.shape, BF16)),
        in_specs=[pl.BlockSpec(memory_space=pltpu.VMEM)] * 5,
        out_specs=[any_spec] * 6,
        scratch_shapes=[pltpu.VMEM((TOK * HEADS, NOPE), BF16),
                        pltpu.VMEM((2, 2, rows, NOPE), F32),
                        dma((4,)), dma((2, 2))],
        compiler_params=pltpu.CompilerParams(vmem_limit_bytes=32 << 20),
    )(dw, o_t, dq_t, dc, dr)


def solution(mesh):
    seq_spec = P("cp")

    def local_step(queries, latent, key_rope, w_uk, w_uv, d_out):
        any_spec = pl.BlockSpec(memory_space=pl.ANY)
        vm_spec = pl.BlockSpec(memory_space=pltpu.VMEM)
        dma = pltpu.SemaphoreType.DMA
        vm = pltpu.VMEM
        o_t, dq_t, dw, d_latent, d_key_rope = pl.pallas_call(
            attn_kernel,
            out_shape=(vm((HEADS, TOK, NOPE), BF16), vm((HEADS, QK, TOK), BF16), vm((HEADS, 2, LAT, NOPE), F32),
                       vm((TOK, LAT), BF16), vm((ROPE, TOK), BF16)),
            in_specs=[any_spec] * 6,
            out_specs=[vm_spec] * 5,
            scratch_shapes=[vm((TOK * HEADS, NOPE), BF16),
                            vm((LAT, HPC, NOPE), BF16), vm((LAT, HPC, NOPE), BF16),
                            vm((TOK * HEADS, NOPE), F32), vm((HPC, TOK, NOPE), BF16),
                            vm((HPC, QK, CH), BF16), vm((HPC, CH, NOPE), BF16),
                            vm((SEQ, LAT), BF16), vm((ROPE, SEQ), BF16), vm((SEQ, ROPE), BF16),
                            vm((HPC, LAT, NOPE), BF16), vm((HPC, LAT, NOPE), BF16),
                            vm((HPC, CH, NOPE), BF16), vm((HPC, QK, CH), BF16),
                            vm((NS, 2, LAT, NOPE), F32),
                            vm((SEQ, LAT), F32), vm((SEQ, ROPE), F32), vm((NCHIP, TOK, LAT), F32), vm((NCHIP, PACK, LAT), F32), vm((NCHIP, PACK, LAT), BF16),
                            vm((SEQ // KC, LAT, KC), BF16), vm((SEQ, 2 * NOPE), BF16),
                            vm((CH, QK), BF16), vm((NOPE, CH), BF16),
                            vm((SEQ, CH), F32), vm((SEQ // SUB, 1, CH), F32), vm((SEQ, CH), BF16),
                            vm((2, 2, 256, NOPE), F32), vm((2, 2, 128, NOPE), F32),
                            vm((NCHIP, TOK, LAT), F32), vm((NCHIP, TOK, ROPE), F32),
                            vm((TOK, LAT), F32), vm((TOK, LAT), F32), vm((2, TOK // 4, LAT), F32),
                            vm((PACK, LAT), BF16), vm((PACK, LAT), BF16),
                            dma((6,)), dma((4,)), dma((4,)), dma((3, 8)), dma((3, 8)),
                            dma((4, 2, 2)), dma((4, 2, 2)), dma((2, 2)), dma((2, 4)), dma((2, 4))],
            compiler_params=pltpu.CompilerParams(vmem_limit_bytes=50 << 20, collective_id=0, has_side_effects=True),
            cost_estimate=pl.CostEstimate(flops=30 * 10**9, bytes_accessed=20 << 20, transcendentals=10**7),
        )(jnp.transpose(queries, (1, 2, 0)), d_out.reshape(TOK * HEADS, NOPE), latent, key_rope.T, w_uk, w_uv)

        o, dk, dv, dq_t, d_latent, d_key_rope = to_output_layout(dw, o_t, dq_t, d_latent, d_key_rope)
        return (o.reshape(TOK, HEADS, NOPE), jnp.transpose(dq_t, (2, 0, 1)), d_latent, d_key_rope.T,
                dk.reshape(LAT, HEADS, NOPE), dv.reshape(LAT, HEADS, NOPE))

    return jax.shard_map(local_step, mesh=mesh,
                         in_specs=(seq_spec, seq_spec, seq_spec, P(), P(), seq_spec),
                         out_specs=(seq_spec, seq_spec, seq_spec, seq_spec, P(), P()),
                         check_vma=False)
```

```python
import functools
import math
import jax
import jax.numpy as jnp
from jax import lax
from jax.experimental import pallas as pl
from jax.experimental.pallas import tpu as pltpu
from jax.sharding import PartitionSpec as P

F32 = jnp.float32
BF16 = jnp.bfloat16
TOK = 256
CH = 512
KC = 1024
HALF = TOK // 2
SUB = 256
HEADS = 16
HPC = 8
NS = HPC
NOPE = 128
ROPE = 64
QK = NOPE + ROPE
LAT = 512
PACK = ROPE // 2
NCHIP = 4
SEQ = CH * NCHIP
MESH = pl.DeviceIdType.MESH


def nt(a, b):
    return lax.dot_general(a, b, (((1,), (1,)), ((), ())), preferred_element_type=F32)


def nn(a, b):
    return lax.dot_general(a, b, (((1,), (0,)), ((), ())), preferred_element_type=F32)


def tn(a, b):
    return lax.dot_general(a, b, (((0,), (0,)), ((), ())), preferred_element_type=F32)


def mul(i, n):
    return pl.multiple_of(i * n, n)


def attn_kernel(q_in, do_in, c_in, r_in, wk_in, wv_in,
                o_out, dq_out, dw_out, dlat_out, dr_out,
                do_raw, wk_raw, wv_raw, stage, do_snd,
                qt, do_ref, c_ref, rt, rn, wk, wv, o_ref, dq_ref, dw_ref, dcr, drr, msg, msr, mrb,
                ct, kv, qn, dot_, s_buf, m_buf, p_buf, rb1, rb2, rbd, rbr, rbx, rby, rbh, rbxr, rbyr,
                lsem, xs, xr, cs, crs, ws, wr, ps, fs, fr):
    scale = 1.0 / math.sqrt(QK)
    c2 = scale * math.log2(math.e)
    me = lax.axis_index("cp")
    core = lax.rem(me, 2)
    chip = lax.div(me, 2)
    x = lax.rem(chip, 2)
    y = lax.div(chip, 2)
    partner = me + 1 - 2 * core
    xn = me + 2 - 4 * x
    yn = me + 4 - 8 * y
    dn = xn + 4 - 8 * y

    def rcopy(src, dst, ss, rs, dev):
        return pltpu.make_async_remote_copy(src_ref=src, dst_ref=dst, send_sem=ss, recv_sem=rs,
                                            device_id=(dev,), device_id_type=MESH)

    my_rows = pl.ds(mul(me, TOK), TOK)
    own_rows = pl.ds(mul(core, TOK), TOK)
    oth_rows = pl.ds(mul(1 - core, TOK), TOK)
    mine = pl.ds(mul(core, HPC), HPC)

    other = pl.ds(mul(1 - core, HPC), HPC)

    local = [pltpu.make_async_copy(c_in, c_ref.at[my_rows], lsem.at[0]),
             pltpu.make_async_copy(r_in, rt.at[:, my_rows], lsem.at[1]),
             pltpu.make_async_copy(q_in.at[mine], qt.at[:, :, own_rows], lsem.at[2]),
             pltpu.make_async_copy(do_in, do_raw, lsem.at[3]),
             pltpu.make_async_copy(wk_in.at[:, mine], wk_raw, lsem.at[4]),
             pltpu.make_async_copy(wv_in.at[:, mine], wv_raw, lsem.at[5])]
    for cp in local:
        cp.start()

    bar = pltpu.get_barrier_semaphore()
    for peer in (partner, xn, yn, dn):
        pl.semaphore_signal(bar, inc=1, device_id=(peer,), device_id_type=MESH)
    pl.semaphore_wait(bar, 4)

    local[0].wait()
    local[1].wait()

    def latent_copies(i, src, dev, recv=None):
        recv = i if recv is None else recv
        rows = pl.ds(mul(src, TOK), TOK)
        parts = [c_ref.at[pl.ds(pl.multiple_of(src * TOK + t * HALF, HALF), HALF)] for t in range(2)]
        parts.append(rt.at[:, rows])
        return [rcopy(ref, ref, cs.at[t, i], crs.at[t, recv], dev) for t, ref in enumerate(parts)]

    low = y == 0
    is0 = core == 0
    c_direct = [latent_copies(i, me, dev) for i, dev in enumerate((partner, xn, yn, dn))]
    c_relay = latent_copies(7, yn, xn, 3)
    for cp in c_direct[0] + c_direct[1]:
        cp.start()

    @pl.when(low)
    def _():
        for cp in c_direct[2]:
            cp.start()

        @pl.when(is0)
        def _():
            for cp in c_direct[3]:
                cp.start()

    heads = [rcopy(q_in.at[other], qt.at[:, :, own_rows], xs.at[0], xr.at[0], partner),
             rcopy(do_snd, do_ref.at[:, own_rows], xs.at[1], xr.at[1], partner)]
    heads[0].start()
    local[3].wait()

    def pick(h, rows, stride):
        return stage[pl.ds(h, rows, stride=stride), :].astype(BF16)

    def widen(i, _):
        rows = pl.ds(mul(i, 256), 256)
        stage[rows, :] = do_raw[rows, :].astype(F32)
        return 0
    lax.fori_loop(0, TOK * HEADS // 256, widen, 0)
    for i in range(HPC):
        lo = pick(i, TOK, HEADS)
        hi = pick(i + HPC, TOK, HEADS)
        do_ref[i, own_rows, :] = jnp.where(is0, lo, hi)
        do_snd[i] = jnp.where(is0, hi, lo)
    heads[1].start()
    for t, (raw, out) in enumerate(((wk_raw, wk), (wv_raw, wv))):
        local[4 + t].wait()

        def body(i, _, raw=raw):
            ls = pl.ds(mul(i, 32), 32)
            stage[pl.ds(mul(i, 256), 256), :] = raw[ls].astype(F32).reshape(256, NOPE)
            return 0
        lax.fori_loop(0, LAT // 32, body, 0)
        for i in range(HPC):
            out[i] = pick(i, LAT, HPC)

    def zero_dc(j, _):
        rows = pl.ds(mul(j, KC), KC)
        dcr[rows, :] = jnp.zeros((KC, LAT), F32)
        drr[rows, :] = jnp.zeros((KC, ROPE), F32)
        return 0
    lax.fori_loop(0, y + 1, zero_dc, 0)
    local[2].wait()
    for cp in heads:
        cp.wait()
    for cp in c_direct[0]:
        cp.wait()

    def turn(j):
        rows = pl.ds(mul(j, KC), KC)
        ct[j] = c_ref[rows, :].T
        rn[rows, :] = rt[:, rows].T

    c_fwd = [None] + [latent_copies(3 + i, src, partner) for i, src in ((1, xn), (2, yn), (3, dn))]

    high = y == 1
    for t in (0, 1, 2):
        c_direct[1][t].wait()
        c_fwd[1][t].start()

        @pl.when(high)
        def _(t=t):
            c_direct[2][t].wait_recv()

            @pl.when(core == 1)
            def _():
                c_relay[t].start()
            c_fwd[2][t].start()
    for cp in c_fwd[1]:
        cp.wait()
    turn(y)

    def wait_latents():
        for t in (0, 1, 2):
            c_direct[3][t].wait_recv()
            c_fwd[3][t].start()
        for cp in c_fwd[2] + c_fwd[3]:
            cp.wait()

        @pl.when(core == 1)
        def _():
            for cp in c_relay:
                cp.wait_send()

    hx = pl.ds(mul(x, 256), 256)
    hx1 = pl.ds(mul(1 - x, 256), 256)
    hy = pl.ds(mul(y, 256), 256)
    hy1 = pl.ds(mul(1 - y, 256), 256)
    qa = pl.ds(pl.multiple_of(x * 256 + y * 128, 128), 128)
    qa1 = pl.ds(pl.multiple_of(x * 256 + (1 - y) * 128, 128), 128)
    qb = pl.ds(pl.multiple_of(y * 256 + x * 128, 128), 128)
    qb1 = pl.ds(pl.multiple_of(y * 256 + (1 - x) * 128, 128), 128)

    def w_copy(phase, s):
        par = lax.rem(s, 2)
        t = core * NS + s
        if phase == 1:
            pair = ((dw_ref.at[s, 0, hx1], rb1.at[par, 0], xn), (dw_ref.at[s, 1, hy1], rb1.at[par, 1], yn))
        elif phase == 2:
            pair = ((dw_ref.at[s, 0, qa1], rb2.at[par, 0], yn), (dw_ref.at[s, 1, qb1], rb2.at[par, 1], xn))
        elif phase == 3:
            pair = ((dw_out.at[t, 0, qa], dw_out.at[t, 0, qa], yn),
                    (dw_out.at[t, 1, qb], dw_out.at[t, 1, qb], xn))
        else:
            pair = ((dw_out.at[t, 0, hx], dw_out.at[t, 0, hx], xn),
                    (dw_out.at[t, 1, hy], dw_out.at[t, 1, hy], yn))
        return [rcopy(a, b, ws.at[phase - 1, par, i], wr.at[phase - 1, par, i], d)
                for i, (a, b, d) in enumerate(pair)]

    def w_start(phase, s):
        for cp in w_copy(phase, s):
            cp.start()

    def w_wait(phase, s):
        for cp in w_copy(phase, s):
            cp.wait()

    def w_final(s, late):
        t = core * NS + s
        par = lax.rem(s, 2)
        parts = (hx1, hy1) if late else (hx, hy)
        return [rcopy(dw_out.at[t, i, r], dw_out.at[t, i, r], fs.at[par, 2 * late + i], fr.at[par, 2 * late + i],
                      partner) for i, r in enumerate(parts)]

    def hand_over(s, late):
        def wait_last():
            for cp in w_final(s - 1, late):
                cp.wait()
        if isinstance(s, int):
            wait_last()
        else:
            pl.when(s > 0)(wait_last)
        for cp in w_final(s, late):
            cp.start()

    def stage2(s):
        par = lax.rem(s, 2)
        w_wait(1, s)
        dw_ref[s, 0, hx] += rb1[par, 0]
        dw_ref[s, 1, hy] += rb1[par, 1]
        w_start(2, s)

    def stage3(s):
        par = lax.rem(s, 2)
        w_wait(2, s)
        t = core * NS + s
        dw_out[t, 0, qa] = dw_ref[s, 0, qa] + rb2[par, 0]
        dw_out[t, 1, qb] = dw_ref[s, 1, qb] + rb2[par, 1]
        w_start(3, s)

    def stage4(s):
        w_wait(3, s)
        w_start(4, s)
        hand_over(s, 0)

    def stage5(s):
        w_wait(4, s)
        hand_over(s, 1)

    def last4(s):
        w_wait(3, s)
        to_a, to_b = w_copy(4, s)

        @pl.when(low)
        def _():
            to_a.start()

        @pl.when(chip != 3)
        def _():
            to_b.start()
        hand_over(s, 0)

    def w_pass(s):
        par = lax.rem(s, 2)
        t = core * NS + s
        pair = ((dw_out.at[t, 0, hx1], yn), (dw_out.at[t, 1, hy1], xn))
        return [rcopy(ref, ref, ps.at[par, i], wr.at[3, par, i], dev) for i, (ref, dev) in enumerate(pair)]

    def last5a(s):
        w_copy(4, s)[0].wait_recv()

        @pl.when(low)
        def _():
            w_pass(s)[0].start()

    def last5b(s):
        w_copy(4, s)[1].wait_recv()

        @pl.when(chip == 0)
        def _():
            w_pass(s)[1].start()
        hand_over(s, 1)

    def last_sent(s):
        @pl.when(low)
        def _():
            w_copy(4, s)[0].wait_send()
            w_pass(s)[0].wait_send()

        @pl.when(chip != 3)
        def _():
            w_copy(4, s)[1].wait_send()

        @pl.when(chip == 0)
        def _():
            w_pass(s)[1].wait_send()

    def d1_copies(j):
        rows = pl.ds(pl.multiple_of(j * CH + (1 - core) * TOK, TOK), TOK)
        return (rcopy(dcr.at[rows], rbd.at[j], cs.at[0, j], crs.at[0, j], partner),
                rcopy(drr.at[rows], rbr.at[j], cs.at[1, j], crs.at[1, j], partner))

    def step(s, _):
        dw_ref[s] = jnp.zeros((2, LAT, NOPE), F32)
        qn[...] = qt[s].T
        dot_[...] = do_ref[s].T
        w_s = jnp.concatenate([wk[s], wv[s]], axis=1)

        def phase1(j, masked):
            ms, ls = [], []
            for t in range(KC // SUB):
                rows = pl.ds(pl.multiple_of(j * KC + t * SUB, SUB), SUB)
                kvv = nn(c_ref[rows, :], w_s).astype(BF16)
                kv[rows, :] = kvv
                k_cat = jnp.concatenate([kvv[:, :NOPE], rn[rows, :]], axis=1)
                s2 = nn(k_cat, qt[s]) * c2
                if masked:
                    ki = lax.broadcasted_iota(jnp.int32, (SUB, CH), 0)
                    qi = lax.broadcasted_iota(jnp.int32, (SUB, CH), 1)
                    s2 = jnp.where(ki - qi <= x * CH - t * SUB, s2, -1e30 * math.log2(math.e))
                m = jnp.max(s2, axis=0, keepdims=True)
                e = jnp.exp2(s2 - m)
                s_buf[rows, :] = e
                m_buf[j * (KC // SUB) + t] = m
                ms.append(m)
                ls.append(jnp.sum(e, axis=0, keepdims=True))
            top = functools.reduce(jnp.maximum, ms)
            return top, sum(l * jnp.exp2(m - top) for m, l in zip(ms, ls))

        stats = phase1(y, True)

        @pl.when(s > 3)
        def _():
            stage5(s - 4)

        @pl.when(s > 1)
        def _():
            stage3(s - 2)

        @pl.when(s == 0)
        def _():
            @pl.when(high)
            def _():
                wait_latents()
                turn(0)

            @pl.when(low)
            def _():
                for cp in c_direct[2]:
                    cp.wait_send()

                @pl.when(is0)
                def _():
                    for cp in c_direct[3]:
                        cp.wait_send()

        def more(j, st):
            m0, l0 = st
            m1, l1 = phase1(j, False)
            m = jnp.maximum(m0, m1)
            return m, l0 * jnp.exp2(m0 - m) + l1 * jnp.exp2(m1 - m)

        top, l = lax.fori_loop(0, y, more, stats)
        inv = 1.0 / l

        def phase2(j, acc):
            rows = pl.ds(mul(j, KC), KC)
            parts = []
            for t in range(KC // SUB):
                sub = pl.ds(pl.multiple_of(j * KC + t * SUB, SUB), SUB)
                fac = jnp.exp2(m_buf[j * (KC // SUB) + t] - top) * inv
                parts.append((s_buf[sub, :] * fac).astype(BF16))
                p_buf[sub, :] = parts[-1]
            return acc + tn(kv[rows, NOPE:], jnp.concatenate(parts, axis=0))

        ot = lax.fori_loop(0, y + 1, phase2, jnp.zeros((NOPE, CH), F32))
        delta = jnp.sum(ot * dot_[...].astype(F32), axis=0, keepdims=True)
        o_ref[s] = ot.T.astype(BF16)

        def phase3(j, acc):
            rows = pl.ds(mul(j, KC), KC)
            k = kv[rows, :NOPE]
            v = kv[rows, NOPE:]
            pb = p_buf[rows, :]
            dp = nn(v, dot_[...])
            ds = (pb.astype(F32) * (dp - delta)).astype(BF16)
            dkr = nn(ds, qn[...]) * scale
            dv = nn(pb, do_ref[s])
            dkv = jnp.concatenate([dkr[:, :NOPE].astype(BF16), dv.astype(BF16)], axis=1)
            drr[rows, :] += dkr[:, NOPE:]
            dcr[rows, :] += nt(dkv, w_s)
            dw = nn(ct[j], dkv)
            dw_ref[s, 0] += dw[:, :NOPE]
            dw_ref[s, 1] += dw[:, NOPE:]
            out = (acc[0] + tn(k, ds), acc[1] + nn(rt[:, rows], ds))

            @pl.when(s == NS - 1)
            def _():
                for t in range(2):
                    for cp in d1_copies(2 * j + t):
                        cp.start()

            @pl.when(j == 0)
            def _():
                @pl.when(s > 0)
                def _():
                    stage2(s - 1)
            return out

        dqn, dqr = lax.fori_loop(0, y + 1, phase3, (jnp.zeros((NOPE, CH), F32), jnp.zeros((ROPE, CH), F32)))
        w_start(1, s)
        dq_ref[s, :NOPE] = (dqn * scale).astype(BF16)
        dq_ref[s, NOPE:] = (dqr * scale).astype(BF16)

        @pl.when(s > 1)
        def _():
            stage4(s - 2)
        return 0

    lax.fori_loop(0, NS, step, 0)

    outs = [rcopy(o_ref.at[:, oth_rows], o_out.at[mine], xs.at[0], xr.at[0], partner),
            rcopy(dq_ref.at[:, :, oth_rows], dq_out.at[mine], xs.at[1], xr.at[1], partner)]
    for cp in outs:
        cp.start()

    def join(j):
        for cp in d1_copies(j):
            cp.wait()
        rows = pl.ds(pl.multiple_of(j * CH + core * TOK, TOK), TOK)
        msg[j] = dcr[rows, :] + rbd[j]
        drt = (drr[rows, :] + rbr[j]).T
        msr[j] = jnp.concatenate([drt[:PACK], drt[PACK:]], axis=1)
        mrb[j] = msr[j].astype(BF16)


    quarters = [pl.ds(i * (TOK // 4), TOK // 4) for i in range(4)]

    def slot(kind, i):
        if kind == 2:
            return 2, i
        return (kind, 4 + i) if i < 4 else (2, 5 + kind)

    def to_x(j):
        return ([rcopy(msg.at[j, h], rbx.at[h], cs.at[slot(0, i)], crs.at[slot(0, i)], xn) for i, h in enumerate(quarters)]
                + [rcopy(mrb.at[j], rbxr, cs.at[slot(0, 4)], crs.at[slot(0, 4)], xn)])

    def to_y(j):
        return ([rcopy(msg.at[j, h], rby.at[h], cs.at[slot(1, i)], crs.at[slot(1, i)], yn) for i, h in enumerate(quarters)]
                + [rcopy(mrb.at[j], rbyr, cs.at[slot(1, 4)], crs.at[slot(1, 4)], yn)])

    half_x = [rcopy(msg.at[0, quarters[i]], rbh.at[i], cs.at[slot(2, i)], crs.at[slot(2, i)], xn) for i in (0, 1)]
    half_y = [rcopy(msg.at[0, quarters[2 + i]], rbh.at[i], cs.at[slot(2, 2 + i)], crs.at[slot(2, i)], yn) for i in (0, 1)]
    half_y.append(rcopy(mrb.at[0], rbxr, cs.at[slot(2, 4)], crs.at[slot(2, 4)], yn))

    def start(copies):
        for cp in copies:
            cp.start()

    def on(k):
        return pl.when(chip == k)

    def add_and_pass(i):
        to_x(1)[i].wait_recv()
        msg[1, quarters[i]] += rbx[quarters[i]]
        to_y(1)[i].start()

    def add_dr(j, buf):
        msr[j] += buf[...].astype(F32)
        mrb[j] = msr[j].astype(BF16)

    stage5(NS - 4)
    stage3(NS - 2)
    join(0)
    join(1)
    stage2(NS - 1)

    stage5(NS - 3)
    last4(NS - 2)
    stage3(NS - 1)

    @on(3)
    def _():
        start((half_x[0], half_y[0]))

    @on(2)
    def _():
        to_x(1)[0].start()

    @pl.when(high)
    def _():
        join(2)

    @on(3)
    def _():
        start((half_x[1], half_y[1], half_y[2], to_x(2)[0]))
        add_and_pass(0)
        add_and_pass(1)
        to_x(2)[1].start()

    @on(2)
    def _():
        start(to_x(1)[1:])
        start(to_y(0)[2:])

    @on(1)
    def _():
        start(to_x(0)[:2])

    @pl.when(low)
    def _():
        last5a(NS - 2)

    @on(0)
    def _():
        last5b(NS - 2)
    last4(NS - 1)

    @on(3)
    def _():
        start(to_x(2)[2:])
        add_and_pass(2)
        add_and_pass(3)
        to_x(1)[4].wait_recv()
        add_dr(1, rbxr)
        to_y(1)[4].start()

    @on(2)
    def _():
        for i in (0, 1):
            half_x[i].wait_recv()
            msg[0, quarters[i]] += rbh[i]
            to_y(0)[i].start()

    @on(1)
    def _():
        for i in (0, 1):
            half_y[i].wait_recv()
            msg[0, quarters[2 + i]] += rbh[i]
            to_x(0)[2 + i].start()
        half_y[2].wait_recv()
        add_dr(0, rbxr)
        to_x(0)[4].start()

    @pl.when(high)
    def _():
        join(3)

    def keep(h, _):
        o_out[core * HPC + h] = o_ref[h, own_rows, :]
        dq_out[core * HPC + h] = dq_ref[h, :, own_rows]
        return 0
    lax.fori_loop(0, HPC, keep, 0)

    @pl.when(high)
    def _():
        last5a(NS - 2)

    @pl.when(chip != 0)
    def _():
        last5b(NS - 2)
    last5a(NS - 1)
    last5b(NS - 1)
    last_sent(NS - 2)
    last_sent(NS - 1)

    def all_of(copies, recv):
        for cp in copies:
            if recv:
                cp.wait_recv()
            else:
                cp.wait_send()

    @pl.when(chip != 3)
    def _():
        @pl.when(chip != 1)
        def _():
            all_of(to_x(0), True)
            msg[chip] += rbx[...]
            add_dr(chip, rbxr)

        @pl.when(chip != 2)
        def _():
            all_of(to_y(0), True)
            msg[chip] += rby[...]
            add_dr(chip, rbyr)

    dlat_out[...] = msg[chip].astype(BF16)
    dr_out[:PACK] = msr[chip, :, :TOK].astype(BF16)
    dr_out[PACK:] = msr[chip, :, TOK:].astype(BF16)

    @pl.when(chip != 0)
    def _():
        all_of(to_x(0), False)

        @pl.when(chip != 1)
        def _():
            all_of(to_y(0), False)

    @pl.when(chip == 3)
    def _():
        all_of(half_x + half_y, False)
    for cp in outs:
        cp.wait()

    for cp in w_final(NS - 1, 0) + w_final(NS - 1, 1):
        cp.wait()


PARTS = 4


def layout_kernel(dw, o_t, dq_t, dc, dr, o_out, dk_out, dv_out, dq_out, dc_out, dr_out,
                  o_stage, stage, osem, ssem):
    lat = LAT // PARTS
    stores = [pltpu.make_async_copy(a, b, osem.at[i])
              for i, (a, b) in enumerate(((o_stage, o_out), (dq_t, dq_out), (dc, dc_out), (dr, dr_out)))]

    def by_row(v):
        return jnp.swapaxes(v, 0, 1).reshape(v.shape[0] * v.shape[1], NOPE)

    def put(i):
        rows = pl.ds(i * lat * HEADS, lat * HEADS)
        return [pltpu.make_async_copy(stage.at[i % 2, a], out.at[rows], ssem.at[i % 2, a])
                for a, out in enumerate((dk_out, dv_out))]

    for i in range(PARTS):
        for a in range(2):
            if i > 1:
                put(i - 2)[a].wait()
            stage[i % 2, a] = by_row(dw[:, a, i * lat:(i + 1) * lat])
            put(i)[a].start()
        if i == 0:
            for cp in stores[1:]:
                cp.start()
            o_stage[...] = by_row(o_t[...].astype(F32)).astype(BF16)
            stores[0].start()
    for i in (PARTS - 2, PARTS - 1):
        for cp in put(i):
            cp.wait()
    for cp in stores:
        cp.wait()


def to_output_layout(dw, o_t, dq_t, dc, dr):
    any_spec = pl.BlockSpec(memory_space=pl.ANY)
    dma = pltpu.SemaphoreType.DMA
    rows = LAT // PARTS * HEADS
    return pl.pallas_call(
        layout_kernel,
        out_shape=(jax.ShapeDtypeStruct((TOK * HEADS, NOPE), BF16),
                   jax.ShapeDtypeStruct((LAT * HEADS, NOPE), F32),
                   jax.ShapeDtypeStruct((LAT * HEADS, NOPE), F32),
                   jax.ShapeDtypeStruct(dq_t.shape, BF16),
                   jax.ShapeDtypeStruct(dc.shape, BF16),
                   jax.ShapeDtypeStruct(dr.shape, BF16)),
        in_specs=[pl.BlockSpec(memory_space=pltpu.VMEM)] * 5,
        out_specs=[any_spec] * 6,
        scratch_shapes=[pltpu.VMEM((TOK * HEADS, NOPE), BF16),
                        pltpu.VMEM((2, 2, rows, NOPE), F32),
                        dma((4,)), dma((2, 2))],
        compiler_params=pltpu.CompilerParams(vmem_limit_bytes=32 << 20),
    )(dw, o_t, dq_t, dc, dr)


def solution(mesh):
    seq_spec = P("cp")

    def local_step(queries, latent, key_rope, w_uk, w_uv, d_out):
        any_spec = pl.BlockSpec(memory_space=pl.ANY)
        vm_spec = pl.BlockSpec(memory_space=pltpu.VMEM)
        dma = pltpu.SemaphoreType.DMA
        vm = pltpu.VMEM
        o_t, dq_t, dw, d_latent, d_key_rope = pl.pallas_call(
            attn_kernel,
            out_shape=(vm((HEADS, TOK, NOPE), BF16), vm((HEADS, QK, TOK), BF16), vm((HEADS, 2, LAT, NOPE), F32),
                       vm((TOK, LAT), BF16), vm((ROPE, TOK), BF16)),
            in_specs=[any_spec] * 6,
            out_specs=[vm_spec] * 5,
            scratch_shapes=[vm((TOK * HEADS, NOPE), BF16),
                            vm((LAT, HPC, NOPE), BF16), vm((LAT, HPC, NOPE), BF16),
                            vm((TOK * HEADS, NOPE), F32), vm((HPC, TOK, NOPE), BF16),
                            vm((HPC, QK, CH), BF16), vm((HPC, CH, NOPE), BF16),
                            vm((SEQ, LAT), BF16), vm((ROPE, SEQ), BF16), vm((SEQ, ROPE), BF16),
                            vm((HPC, LAT, NOPE), BF16), vm((HPC, LAT, NOPE), BF16),
                            vm((HPC, CH, NOPE), BF16), vm((HPC, QK, CH), BF16),
                            vm((NS, 2, LAT, NOPE), F32),
                            vm((SEQ, LAT), F32), vm((SEQ, ROPE), F32), vm((NCHIP, TOK, LAT), F32), vm((NCHIP, PACK, LAT), F32), vm((NCHIP, PACK, LAT), BF16),
                            vm((SEQ // KC, LAT, KC), BF16), vm((SEQ, 2 * NOPE), BF16),
                            vm((CH, QK), BF16), vm((NOPE, CH), BF16),
                            vm((SEQ, CH), F32), vm((SEQ // SUB, 1, CH), F32), vm((SEQ, CH), BF16),
                            vm((2, 2, 256, NOPE), F32), vm((2, 2, 128, NOPE), F32),
                            vm((NCHIP, TOK, LAT), F32), vm((NCHIP, TOK, ROPE), F32),
                            vm((TOK, LAT), F32), vm((TOK, LAT), F32), vm((2, TOK // 4, LAT), F32),
                            vm((PACK, LAT), BF16), vm((PACK, LAT), BF16),
                            dma((6,)), dma((2,)), dma((2,)), dma((3, 8)), dma((3, 8)),
                            dma((4, 2, 2)), dma((4, 2, 2)), dma((2, 2)), dma((2, 4)), dma((2, 4))],
            compiler_params=pltpu.CompilerParams(vmem_limit_bytes=50 << 20, collective_id=0, has_side_effects=True),
            cost_estimate=pl.CostEstimate(flops=30 * 10**9, bytes_accessed=20 << 20, transcendentals=10**7),
        )(jnp.transpose(queries, (1, 2, 0)), d_out.reshape(TOK * HEADS, NOPE), latent, key_rope.T, w_uk, w_uv)

        o, dk, dv, dq_t, d_latent, d_key_rope = to_output_layout(dw, o_t, dq_t, d_latent, d_key_rope)
        return (o.reshape(TOK, HEADS, NOPE), jnp.transpose(dq_t, (2, 0, 1)), d_latent, d_key_rope.T,
                dk.reshape(LAT, HEADS, NOPE), dv.reshape(LAT, HEADS, NOPE))

    return jax.shard_map(local_step, mesh=mesh,
                         in_specs=(seq_spec, seq_spec, seq_spec, P(), P(), seq_spec),
                         out_specs=(seq_spec, seq_spec, seq_spec, seq_spec, P(), P()),
                         check_vma=False)
```
